128 devices in a mesh: scene: 16 (over y, z), image: 8 (over x, core).
Axes of the slice: x: 4, y: 4, z: 4, core: 2. Of those that a mesh axis runs over, the one named last changes fastest.
Arguments:
- jacobian: bfloat16 [1024, 256, 1152], P(('scene', 'image')), may hold values from -0.1875 to 0.1875
- splat_ids: int32 [1024, 128], P(('scene', 'image')), may hold values from 0 to 16383, as said below
- pix_residual: bfloat16 [1024, 256], P(('scene', 'image')), may hold values from -6 to 6
- live_blocks: int32 [128], replicated, may hold values from 1 to 8, as said below
- proj_jac: bfloat16 [9, 59, 16384], P(None, None, 'scene'), may hold values from -0.75 to 0.75
- damping: float32 [59, 16384], P(None, 'scene'), may hold values from 0.1 to 1
- precond: float32 [59, 16384], P(None, 'scene'), may hold values from 0.3 to 9
Outputs:
- solution: float32 [59, 16384], P(None, 'scene')
- residual: float32 [59, 16384], P(None, 'scene')
The draws below stay inside these ranges and needn't reach their ends.
Inputs may be any that keep to these rules, and one draw needn't show every extreme that they name: live_blocks[d] counts the blocks in use on device d = scene index * 8 + image index; they are its slots 0 to live_blocks[d] - 1; some device uses all 8 while the device whose index differs from it in the lowest bit uses at most half of them. `splat_ids`: splat s of every block names a Gaussian of scene index s // 8, that is an id from that index times 1024 to the next such multiple.
All inputs are finite; a program needn't handle non-finite values.
Results may differ from the reference program's by a relative error of at most 0.0051.
Values may be sent and summed in bfloat16 or wider, within the bound.
No kernel may reach another device: no remote copies, remote signals or barrier semaphores. Data moves between devices by JAX's collectives and lax.ppermute only.
A program may use at most 64 MiB of HBM per device.

```python
import math
import jax
import jax.numpy as jnp
from jax import lax

PAR = 59
PROJ = 9
PIX = 256
SPL = 128
ITERS = 2
G_DEV = 1024
BLK_DEV = 8
G = 16384
BLOCKS = 1024
N_SCENE = 16
DEVICES = 128


def draw_live_blocks(key, part):
    first_key, second_key, third_key = jax.random.split(key, 3)
    lower_counts = jax.random.randint(first_key, (DEVICES,), 1, BLK_DEV // 2 + 1)
    heavy_mask = jax.random.randint(second_key, (DEVICES,), 0, 4) == 0
    counts = jnp.where(heavy_mask, BLK_DEV, lower_counts)
    chosen_device = jax.random.randint(third_key, (), 0, DEVICES)
    partner_device = jnp.bitwise_xor(chosen_device, 1)
    counts = counts.at[chosen_device].set(BLK_DEV)
    counts = counts.at[partner_device].set(lower_counts[partner_device])
    return counts.astype(jnp.int32)


def draw_splat_ids(key, part):
    owner_width = SPL // N_SCENE
    owners = jnp.arange(SPL, dtype=jnp.int32) // owner_width
    local_ids = jax.random.randint(key, (BLOCKS, SPL), 0, G_DEV)
    return (owners[None, :] * G_DEV + local_ids).astype(jnp.int32)


def draw_precond(key, part):
    ramp = 1.0 + 2.0 * jnp.arange(G, dtype=jnp.float32) / max(G - 1, 1)
    values = jnp.exp(jax.random.uniform(key, (PAR, G), jnp.float32, math.log(0.3), math.log(3.0)))
    return values * ramp[None, :]


def shard_levels(stream_key, extent, cuts, smallest, top_value):
    def one(dim, parts):
        draws = jax.random.uniform(jax.random.fold_in(jax.random.fold_in(stream_key, 6), dim), (parts,), jnp.float32, smallest / len(cuts), top_value / len(cuts))
        return jnp.repeat(jnp.exp(draws), extent[dim] // parts).reshape((-1,) + (1,) * (len(extent) - dim - 1))

    level = one(*cuts[0])
    for cut in cuts[1:]:
        level = level * one(*cut)
    return level


def centred(rng, extent, scale, bound, cuts=(), kind=jnp.bfloat16):
    values = scale * jax.random.normal(rng, extent, jnp.float32)
    if cuts:
        values = values * shard_levels(rng, extent, cuts, -0.22, 0.18)
    return jnp.clip(values, -bound, bound).astype(kind)


def setup_inputs(seed: int = 0) -> dict:
    splits = jax.random.split(jax.random.key(seed), 8)
    return {
        "jacobian": centred(splits[0], (BLOCKS, PIX, PROJ * SPL), (PROJ * SPL) ** -0.5, 0.1875, ((0, 128),)),
        "splat_ids": draw_splat_ids(jax.random.fold_in(splits[7], 71), 0),
        "pix_residual": centred(splits[2], (BLOCKS, PIX), 1.0, 6.0, ((0, 128),)),
        "live_blocks": draw_live_blocks(jax.random.fold_in(splits[7], 71), 0),
        "proj_jac": centred(splits[4], (PROJ, PAR, G), PAR ** -0.5, 0.75, ((2, 16),)),
        "damping": jnp.clip(jnp.exp(math.log(1.0) - 2.3025851 * jax.random.uniform(splits[5], (PAR, G), jnp.float32) ** shard_levels(splits[5], (PAR, G), ((1, 16),), -0.2, 0.2)), 0.1, 1.0),
        "precond": draw_precond(jax.random.fold_in(splits[7], 71), 0),
    }


def project(proj_jac, field):
    return jnp.einsum("kag,ag->kg", proj_jac.astype(jnp.float32), field, precision=lax.Precision.HIGHEST).astype(jnp.bfloat16)


def lift(proj_jac, weights):
    return jnp.einsum("kag,kg->ag", proj_jac.astype(jnp.float32), weights, precision=lax.Precision.HIGHEST)


def reference(jacobian, splat_ids, pix_residual, live_blocks, proj_jac, damping, precond):
    n_proj = proj_jac.shape[0]
    n_gauss = damping.shape[1]
    positions = jnp.arange(jacobian.shape[0], dtype=jnp.int32)
    active = (positions % BLK_DEV < live_blocks[positions // BLK_DEV]).astype(jnp.float32)

    def back_project(vectors):
        def advance(summed, pieces):
            jac_block, chosen, pixels, weight = pieces
            if vectors is None:
                signal = pixels
            else:
                picked = vectors[:, chosen].reshape(-1)
                signal = jnp.dot(jac_block, picked, preferred_element_type=jnp.float32).astype(jnp.bfloat16)
            returned = jnp.dot(signal, jac_block, preferred_element_type=jnp.float32) * weight
            return summed.at[:, chosen].add(returned.reshape(n_proj, -1)), None

        start = jnp.zeros((n_proj, n_gauss), jnp.float32)
        summed, _ = lax.scan(advance, start, (jacobian, splat_ids, pix_residual, active))
        return summed

    def operator(direction):
        return lift(proj_jac, back_project(project(proj_jac, direction))) + damping * direction

    residual = -lift(proj_jac, back_project(None))
    solution = jnp.zeros_like(residual)
    precon_res = precond * residual
    direction = precon_res
    rz_now = jnp.sum(residual * precon_res)
    for iteration in range(ITERS):
        image = operator(direction)
        alpha = rz_now / jnp.sum(direction * image)
        solution = solution + alpha * direction
        residual = residual - alpha * image
        precon_res = precond * residual
        rz_next = jnp.sum(residual * precon_res)
        direction = precon_res + (rz_next / rz_now) * direction
        rz_now = rz_next
    return solution, residual
```

```python
import jax
import jax.numpy as jnp
from jax import lax
from jax.experimental import pallas as pl
from jax.experimental.pallas import tpu as pltpu
from jax.sharding import Mesh
from jax.sharding import PartitionSpec as P

F32 = jnp.float32
BF16 = jnp.bfloat16
LANES = 128
ROWS = 16
VMEM = pl.BlockSpec(memory_space=pltpu.VMEM)
SMEM = pl.BlockSpec(memory_space=pltpu.SMEM)
ANY = pl.BlockSpec(memory_space=pl.ANY)
NT = (((1,), (1,)), ((), ()))


def call(kernel, out, in_specs, scratch=(), flops=1 << 20):
    return pl.pallas_call(
        kernel,
        out_shape=out,
        in_specs=in_specs,
        out_specs=jax.tree.map(lambda _: VMEM, out),
        scratch_shapes=scratch,
        compiler_params=pltpu.CompilerParams(vmem_limit_bytes=24 << 20),
        cost_estimate=pl.CostEstimate(flops=flops, bytes_accessed=1 << 20, transcendentals=0),
    )


def f32(*shape):
    return jax.ShapeDtypeStruct(shape, F32)


def j_copies(jac, jbuf, sem):
    return [pltpu.make_async_copy(jac.at[b], jbuf.at[b], sem.at[b]) for b in range(jac.shape[0])]


def pack_return(acc, ids, scalars, stage, out):
    n_blk = acc.shape[0]
    n_proj = acc.shape[1] // LANES
    stage[...] = jnp.zeros_like(stage)
    for k in range(n_proj):
        stage[pl.ds(k, n_blk, stride=ROWS), :] = acc[:, k * LANES : (k + 1) * LANES]
    stage[pl.ds(n_proj, n_blk, stride=ROWS), :] = ids.astype(F32)
    for i, value in enumerate(scalars):
        stage[n_proj + 1 + i : n_proj + 2 + i, :] = jnp.full((1, LANES), value, F32)
    turned = stage[...].T.reshape(out.shape[0], *out.shape[2:])
    for x in range(out.shape[1]):
        out[:, x] = turned


def rhs_kernel(live, jac, pix, ids, out, jbuf, stage, sem):
    copies = j_copies(jac, jbuf, sem)
    for copy in copies:
        copy.start()
    n_blk, n_pix = pix.shape
    row = lax.broadcasted_iota(jnp.int32, (n_blk, n_pix), 0)
    values = jnp.where(row < live[0], pix[...].astype(F32), 0.0)
    acc = jnp.zeros((n_blk, jac.shape[2]), F32)
    for b, copy in enumerate(copies):
        copy.wait()
        signal = jnp.where(row == b, values, 0.0).astype(BF16)
        acc += jnp.dot(signal, jbuf[b], preferred_element_type=F32)
    pack_return(acc, ids[...], (), stage, out)


def block_pass(picks, live, copies, jbuf, n_pix):
    n_blk = picks.shape[0]
    row = lax.broadcasted_iota(jnp.int32, (n_blk, n_pix), 0)
    chosen = picks.astype(BF16)
    acc = jnp.zeros(picks.shape, F32)
    for b, copy in enumerate(copies):
        copy.wait()
        image = lax.dot_general(chosen, jbuf[b], NT, preferred_element_type=F32)
        keep = (row == b) & (row < live)
        signal = jnp.where(keep, image, 0.0).astype(BF16)
        acc += jnp.dot(signal, jbuf[b], preferred_element_type=F32)
    return acc


def unpack_picks(recv, turned, n_blk, n_proj):
    turned[...] = recv[...].reshape(LANES, LANES).T
    return jnp.concatenate(
        [turned[pl.ds(k, n_blk, stride=ROWS), :] for k in range(n_proj)], axis=1
    )


def total_of(row, copies):
    return jnp.sum(row) * (1.0 / copies)


def first_kernel(live, jac, ids, recv, out, picks_out, jbuf, turned, stage, sem):
    copies = j_copies(jac, jbuf, sem)
    for copy in copies:
        copy.start()
    n_blk = ids.shape[0]
    n_proj = jac.shape[2] // LANES
    picks = unpack_picks(recv, turned, n_blk, n_proj)
    picks_out[...] = picks
    acc = block_pass(picks, live[0], copies, jbuf, jac.shape[1])
    pack_return(acc, ids[...], (), stage, out)


def second_kernel(
    live, jac, ids, recv, picks_in, res, dirn, image, precond, damping,
    out, res_out, dir_out, alpha_out, jbuf, turned, stage, sem,
):
    copies = j_copies(jac, jbuf, sem)
    for copy in copies:
        copy.start()
    n_blk = ids.shape[0]
    n_proj = jac.shape[2] // LANES
    fresh = unpack_picks(recv, turned, n_blk, n_proj)
    per = recv.shape[1]
    rz = total_of(turned[n_proj + 1 : n_proj + 2, :], per)
    curve = total_of(turned[n_proj + 2 : n_proj + 3, :], per)
    square = total_of(turned[n_proj + 3 : n_proj + 4, :], per)
    alpha = jnp.full((1, LANES), rz, F32) / jnp.full((1, LANES), curve, F32)
    after = rz - 2.0 * alpha * curve + alpha * alpha * square
    beta = after / jnp.full((1, LANES), rz, F32)
    alpha_out[...] = jnp.broadcast_to(alpha, alpha_out.shape)
    pieces = []
    for k in range(n_proj):
        cols = slice(k * LANES, (k + 1) * LANES)
        pieces.append((1.0 + beta) * picks_in[:, cols] - alpha * fresh[:, cols])
    picks = jnp.concatenate(pieces, axis=1)
    n_par, width = res.shape
    damped = jnp.zeros((n_par, LANES), F32)
    rz_next = jnp.zeros((n_par, LANES), F32)
    for h in range(width // LANES):
        cols = slice(h * LANES, (h + 1) * LANES)
        new_res = res[:, cols] - alpha * image[:, cols]
        precon = precond[:, cols] * new_res
        new_dir = precon + beta * dirn[:, cols]
        res_out[:, cols] = new_res
        dir_out[:, cols] = new_dir
        damped += damping[:, cols] * new_dir * new_dir
        rz_next += new_res * precon
    acc = block_pass(picks, live[0], copies, jbuf, jac.shape[1])
    scalars = (jnp.sum(picks * acc), jnp.sum(damped), jnp.sum(rz_next))
    pack_return(acc, ids[...], scalars, stage, out)


def sum_kernel(own_x, recv, out, ids_out, turned, left, right):
    n_x = recv.shape[1]
    n_blk = LANES // ROWS
    n_proj = 9
    sub = lax.broadcasted_iota(jnp.int32, (n_blk, LANES), 0)
    deep = lax.broadcasted_iota(jnp.int32, (LANES, LANES), 0)
    half = n_proj * 8
    for x in range(n_x):
        turned[x] = recv[:, x].reshape(LANES, LANES).T
        for b in range(n_blk):
            at = (x * n_blk + b) * LANES
            cols = slice(at, at + LANES)
            base = b * ROWS
            ids = turned[x, base + n_proj : base + n_proj + 1, :].astype(jnp.int32)
            high = jnp.broadcast_to(ids >> 7, (8, LANES)) == sub
            low = jnp.broadcast_to(ids & 127, (LANES, LANES)) == deep
            spread = jnp.concatenate(
                [
                    jnp.where(
                        high,
                        jnp.broadcast_to(turned[x, base + k : base + k + 1, :], (8, LANES)),
                        0.0,
                    )
                    for k in range(n_proj)
                ],
                axis=0,
            )
            coarse = spread.astype(BF16)
            left[0:half, cols] = coarse
            left[80 : 80 + half, cols] = (spread - coarse.astype(F32)).astype(BF16)
            right[:, cols] = jnp.where(low, 1.0, 0.0).astype(BF16)
    summed = lax.dot_general(left[...], right[...], NT, preferred_element_type=F32)
    out[0:half, :] = summed[0:half] + summed[80 : 80 + half]
    per = recv.shape[2]
    mixed = jnp.zeros((1, LANES), F32)
    for x in range(n_x):
        mixed += turned[x, n_proj + 1 : n_proj + 2, :]
    out[half : half + 1, :] = jnp.full((1, LANES), total_of(mixed, per), F32)
    for i in (1, 2):
        line = turned[0, n_proj + 1 + i : n_proj + 2 + i, :]
        out[half + i : half + i + 1, :] = jnp.full((1, LANES), total_of(line, per), F32)
    out[half + 3 : half + 8, :] = jnp.zeros((5, LANES), F32)
    ids_out[...] = turned[own_x[0], pl.ds(n_proj, n_blk, stride=ROWS), :].astype(jnp.int32)


def lifted(proj, weights, h):
    cols = slice(h * LANES, (h + 1) * LANES)
    n_proj, n_par, _ = proj.shape
    acc = jnp.zeros((n_par, LANES), F32)
    for k in range(n_proj):
        line = weights[k * 8 + h : k * 8 + h + 1, :]
        acc += proj[k, :, cols].astype(F32) * jnp.broadcast_to(line, (n_par, LANES))
    return acc


def projected(proj, field, h, table):
    cols = slice(h * LANES, (h + 1) * LANES)
    for k in range(proj.shape[0]):
        table[k : k + 1, cols] = jnp.sum(
            proj[k, :, cols].astype(F32) * field, axis=0, keepdims=True
        )


def lane_pick(table, low):
    return jnp.take_along_axis(table, low, axis=1, mode="promise_in_bounds")


def send_picks(table, ids, scalars, stage, out):
    n_blk = ids.shape[0]
    n_chunk = table.shape[1] // LANES
    stage[...] = jnp.zeros_like(stage)
    index = ids[...]
    low = index & 127
    high = index >> 7
    for b in range(n_blk):
        low_b = jnp.broadcast_to(low[b : b + 1, :], (8, LANES))
        high_b = jnp.broadcast_to(high[b : b + 1, :], (8, LANES))
        got = jnp.zeros((8, LANES), F32)
        for h in range(n_chunk):
            piece = lane_pick(table[0:8, h * LANES : (h + 1) * LANES], low_b)
            got = jnp.where(high_b == h, piece, got)
        stage[b * ROWS : b * ROWS + 8, :] = got
    got = jnp.zeros((n_blk, LANES), F32)
    for h in range(n_chunk):
        line = jnp.broadcast_to(table[8:9, h * LANES : (h + 1) * LANES], (n_blk, LANES))
        got = jnp.where(high == h, lane_pick(line, low), got)
    stage[pl.ds(8, n_blk, stride=ROWS), :] = got
    for i, value in enumerate(scalars):
        stage[10 + i : 11 + i, :] = jnp.full((1, LANES), value, F32)
    out[...] = stage[...].T.reshape(out.shape)


def start_kernel(own, partner, proj, precond, ids, out, res_out, dir_out, weights, table, stage):
    weights[...] = own[...] + partner[...]
    n_par, width = precond.shape
    for h in range(width // LANES):
        cols = slice(h * LANES, (h + 1) * LANES)
        res = -lifted(proj, weights, h)
        dirn = precond[:, cols] * res
        res_out[:, cols] = res
        dir_out[:, cols] = dirn
        projected(proj, dirn, h, table)
    send_picks(table, ids, (), stage, out)


def step_kernel(
    own, partner, proj, precond, damping, ids, res, dirn, out, image_out, weights, table, stage
):
    weights[...] = own[...] + partner[...]
    n_par, width = precond.shape
    rz = jnp.zeros((n_par, LANES), F32)
    curve = jnp.zeros((n_par, LANES), F32)
    square = jnp.zeros((n_par, LANES), F32)
    for h in range(width // LANES):
        cols = slice(h * LANES, (h + 1) * LANES)
        image = lifted(proj, weights, h) + damping[:, cols] * dirn[:, cols]
        image_out[:, cols] = image
        scaled = precond[:, cols] * image
        projected(proj, scaled, h, table)
        rz += res[:, cols] * dirn[:, cols]
        curve += dirn[:, cols] * image
        square += scaled * image
    send_picks(table, ids, (jnp.sum(rz), jnp.sum(curve), jnp.sum(square)), stage, out)


def last_kernel(
    own, partner, proj, damping, alpha_in, first_dir, res, dirn, sol_out, res_out, weights
):
    weights[...] = own[...] + partner[...]
    rows = proj.shape[0] * 8
    curve = weights[rows : rows + 1, :] + own[rows + 1 : rows + 2, :]
    alpha = own[rows + 2 : rows + 3, :] / curve
    alpha_first = alpha_in[0:1, :]
    for h in range(damping.shape[1] // LANES):
        cols = slice(h * LANES, (h + 1) * LANES)
        image = lifted(proj, weights, h) + damping[:, cols] * dirn[:, cols]
        sol_out[:, cols] = alpha_first * first_dir[:, cols] + alpha * dirn[:, cols]
        res_out[:, cols] = res[:, cols] - alpha * image


def local(jacobian, splat_ids, pix_residual, live_blocks, proj_jac, damping, precond):
    n_blk, n_pix, n_col = jacobian.shape
    n_par, g_dev = damping.shape
    n_scene, n_x, n_core = lax.axis_size("scene"), lax.axis_size("x"), lax.axis_size("core")
    position = (lax.axis_index("scene") * n_x + lax.axis_index("x")) * n_core + lax.axis_index(
        "core"
    )
    live = lax.dynamic_slice(live_blocks, (position,), (1,))
    own_x = lax.axis_index("x").astype(jnp.int32).reshape(1)
    ids = splat_ids & (g_dev - 1)

    per = LANES // n_scene
    msg = f32(n_scene, per, LANES)
    wide = f32(n_scene, n_x, per, LANES)
    sums = f32(80, LANES)
    state = f32(n_par, g_dev)
    square = pltpu.VMEM((LANES, LANES), F32)
    jbuf = pltpu.VMEM((n_blk, n_pix, n_col), BF16)
    sems = pltpu.SemaphoreType.DMA((n_blk,))
    weights = pltpu.VMEM((80, LANES), F32)
    table = pltpu.VMEM((16, g_dev), F32)

    def to_owners(message):
        flat = message.reshape(n_scene * n_x, per, LANES)
        got = lax.all_to_all(flat, ("scene", "x"), 0, 0, tiled=True)
        own, index = call(
            sum_kernel,
            (sums, jax.ShapeDtypeStruct((n_blk, LANES), jnp.int32)),
            [SMEM, VMEM],
            [
                pltpu.VMEM((n_x, LANES, LANES), F32),
                pltpu.VMEM((160, n_x * n_blk * LANES), BF16),
                pltpu.VMEM((LANES, n_x * n_blk * LANES), BF16),
            ],
        )(own_x, got.reshape(n_scene, n_x, per, LANES))
        partner = lax.ppermute(own, "core", [(0, 1), (1, 0)])
        return own, partner, index

    def to_blocks(message):
        return lax.all_to_all(message, "scene", 0, 0, tiled=True)

    message = call(rhs_kernel, wide, [SMEM, ANY, VMEM, VMEM], [jbuf, square, sems])(
        live, jacobian, pix_residual, ids
    )
    own, partner, index = to_owners(message)
    message, res, first_dir = call(
        start_kernel, (msg, state, state), [VMEM] * 5, [weights, table, square]
    )(own, partner, proj_jac, precond, index)
    arrived = to_blocks(message)
    message, picks = call(
        first_kernel,
        (wide, f32(n_blk, n_col)),
        [SMEM, ANY, VMEM, VMEM],
        [jbuf, square, square, sems],
    )(live, jacobian, ids, arrived)
    own, partner, index = to_owners(message)
    message, image = call(step_kernel, (msg, state), [VMEM] * 8, [weights, table, square])(
        own, partner, proj_jac, precond, damping, index, res, first_dir
    )
    arrived = to_blocks(message)
    message, res, second_dir, alpha = call(
        second_kernel,
        (wide, state, state, f32(8, LANES)),
        [SMEM, ANY] + [VMEM] * 8,
        [jbuf, square, square, sems],
    )(live, jacobian, ids, arrived, picks, res, first_dir, image, precond, damping)
    own, partner, index = to_owners(message)
    return call(last_kernel, (state, state), [VMEM] * 8, [weights])(
        own, partner, proj_jac, damping, alpha, first_dir, res, second_dir
    )


def solution(mesh):
    scene = mesh.shape["scene"]
    finer = Mesh(mesh.devices.reshape(scene, -1, 2), ("scene", "x", "core"))
    everywhere = ("scene", "x", "core")
    in_specs = (
        P(everywhere, None, None),
        P(everywhere, None),
        P(everywhere, None),
        P(),
        P(None, None, "scene"),
        P(None, "scene"),
        P(None, "scene"),
    )
    out_specs = (P(None, "scene"), P(None, "scene"))
    return jax.shard_map(local, mesh=finer, in_specs=in_specs, out_specs=out_specs, check_vma=False)
```

```python
import jax
import jax.numpy as jnp
from jax import lax
from jax.experimental import pallas as pl
from jax.experimental.pallas import tpu as pltpu
from jax.sharding import Mesh
from jax.sharding import PartitionSpec as P

F32 = jnp.float32
BF16 = jnp.bfloat16
LANES = 128
ROWS = 16
VMEM = pl.BlockSpec(memory_space=pltpu.VMEM)
HBM = pl.BlockSpec(memory_space=pltpu.HBM)
NT = (((1,), (1,)), ((), ()))


def call(kernel, out, in_specs, scratch=(), flops=1 << 20):
    return pl.pallas_call(
        kernel,
        out_shape=out,
        in_specs=in_specs,
        out_specs=jax.tree.map(lambda _: VMEM, out),
        scratch_shapes=scratch,
        compiler_params=pltpu.CompilerParams(vmem_limit_bytes=24 << 20),
        cost_estimate=pl.CostEstimate(flops=flops, bytes_accessed=1 << 20, transcendentals=0),
    )


def in_hbm(array):
    return pltpu.with_memory_space_constraint(array, pltpu.HBM)


def f32(*shape):
    return jax.ShapeDtypeStruct(shape, F32)


def pack_return(acc, ids, scalars, stage, out):
    n_blk = acc.shape[0]
    n_proj = acc.shape[1] // LANES
    stage[...] = jnp.zeros_like(stage)
    for k in range(n_proj):
        stage[pl.ds(k, n_blk, stride=ROWS), :] = acc[:, k * LANES : (k + 1) * LANES]
    stage[pl.ds(n_proj, n_blk, stride=ROWS), :] = ids.astype(F32)
    for i, value in enumerate(scalars):
        stage[n_proj + 1 + i : n_proj + 2 + i, :] = jnp.full((1, LANES), value, F32)
    turned = stage[...].T.reshape(out.shape[0], *out.shape[2:])
    for x in range(out.shape[1]):
        out[:, x] = turned


def rhs_kernel(live, jac, pix, ids, out, jbuf, aux, pixels, lives, index, stage, sem, small):
    n_blk = jac.shape[0]
    minor = [
        pltpu.make_async_copy(pix, pixels, small.at[0]),
        pltpu.make_async_copy(live, lives, small.at[1]),
        pltpu.make_async_copy(ids, index, small.at[2]),
    ]
    copies = [pltpu.make_async_copy(jac.at[b], jbuf.at[b], sem.at[b]) for b in range(n_blk)]
    for copy in minor + copies:
        copy.start()
    for copy in minor:
        copy.wait()
    n_x, n_core = lax.axis_size("x"), lax.axis_size("core")
    position = (lax.axis_index("scene") * n_x + lax.axis_index("x")) * n_core
    position = position + lax.axis_index("core")
    lane = lax.broadcasted_iota(jnp.int32, lives.shape, 1)
    own = jnp.sum(jnp.where(lane == position, lives[...], 0), axis=1, keepdims=True)
    local_ids = index[...] & (LANES * 8 - 1)
    aux[0:n_blk, :] = local_ids
    aux[n_blk : 2 * n_blk, :] = jnp.broadcast_to(own, (n_blk, LANES))
    row = lax.broadcasted_iota(jnp.int32, pix.shape, 0)
    keep = row < jnp.broadcast_to(own, pix.shape)
    values = jnp.where(keep, pixels[...].astype(F32), 0.0)
    acc = jnp.zeros((n_blk, jac.shape[2]), F32)
    for b, copy in enumerate(copies):
        copy.wait()
        signal = jnp.where(row == b, values, 0.0).astype(BF16)
        acc += jnp.dot(signal, jbuf[b], preferred_element_type=F32)
    pack_return(acc, local_ids, (), stage, out)


def block_pass(picks, aux, jac):
    n_blk, n_pix = jac.shape[:2]
    row = lax.broadcasted_iota(jnp.int32, (n_blk, n_pix), 0)
    live = row < aux[n_blk : n_blk + 1, 0:1]
    chosen = picks.astype(BF16)
    acc = jnp.zeros(picks.shape, F32)
    for b in range(n_blk):
        image = lax.dot_general(chosen, jac[b], NT, preferred_element_type=F32)
        signal = jnp.where((row == b) & live, image, 0.0).astype(BF16)
        acc += jnp.dot(signal, jac[b], preferred_element_type=F32)
    return acc


def unpack_picks(recv, turned, n_blk, n_proj):
    turned[...] = recv[...].reshape(LANES, LANES).T
    return jnp.concatenate(
        [turned[pl.ds(k, n_blk, stride=ROWS), :] for k in range(n_proj)], axis=1
    )


def total_of(row, copies):
    return jnp.sum(row) * (1.0 / copies)


def first_kernel(jac, aux, recv, out, picks_out, turned, stage):
    n_blk = jac.shape[0]
    n_proj = jac.shape[2] // LANES
    picks = unpack_picks(recv, turned, n_blk, n_proj)
    picks_out[...] = picks
    acc = block_pass(picks, aux, jac)
    pack_return(acc, aux[0:n_blk, :], (), stage, out)


def second_kernel(
    jac, aux, recv, picks_in, res, dirn, image, precond, damping,
    out, res_out, dir_out, alpha_out, turned, stage,
):
    n_blk = jac.shape[0]
    n_proj = jac.shape[2] // LANES
    fresh = unpack_picks(recv, turned, n_blk, n_proj)
    per = recv.shape[1]
    rz = total_of(turned[n_proj + 1 : n_proj + 2, :], per)
    curve = total_of(turned[n_proj + 2 : n_proj + 3, :], per)
    square = total_of(turned[n_proj + 3 : n_proj + 4, :], per)
    alpha = jnp.full((1, LANES), rz, F32) / jnp.full((1, LANES), curve, F32)
    after = rz - 2.0 * alpha * curve + alpha * alpha * square
    beta = after / jnp.full((1, LANES), rz, F32)
    alpha_out[...] = jnp.broadcast_to(alpha, alpha_out.shape)
    pieces = []
    for k in range(n_proj):
        cols = slice(k * LANES, (k + 1) * LANES)
        pieces.append((1.0 + beta) * picks_in[:, cols] - alpha * fresh[:, cols])
    picks = jnp.concatenate(pieces, axis=1)
    n_par, width = res.shape
    damped = jnp.zeros((n_par, LANES), F32)
    rz_next = jnp.zeros((n_par, LANES), F32)
    for h in range(width // LANES):
        cols = slice(h * LANES, (h + 1) * LANES)
        new_res = res[:, cols] - alpha * image[:, cols]
        precon = precond[:, cols] * new_res
        new_dir = precon + beta * dirn[:, cols]
        res_out[:, cols] = new_res
        dir_out[:, cols] = new_dir
        damped += damping[:, cols] * new_dir * new_dir
        rz_next += new_res * precon
    acc = block_pass(picks, aux, jac)
    scalars = (jnp.sum(picks * acc), jnp.sum(damped), jnp.sum(rz_next))
    pack_return(acc, aux[0:n_blk, :], scalars, stage, out)


def sum_kernel(recv, out, ids_out, turned, left, right):
    n_x = recv.shape[1]
    n_blk = LANES // ROWS
    n_proj = 9
    sub = lax.broadcasted_iota(jnp.int32, (n_blk, LANES), 0)
    deep = lax.broadcasted_iota(jnp.int32, (LANES, LANES), 0)
    half = n_proj * 8
    for x in range(n_x):
        turned[x] = recv[:, x].reshape(LANES, LANES).T
        for b in range(n_blk):
            at = (x * n_blk + b) * LANES
            cols = slice(at, at + LANES)
            base = b * ROWS
            ids = turned[x, base + n_proj : base + n_proj + 1, :].astype(jnp.int32)
            high = jnp.broadcast_to(ids >> 7, (8, LANES)) == sub
            low = jnp.broadcast_to(ids & 127, (LANES, LANES)) == deep
            spread = jnp.concatenate(
                [
                    jnp.where(
                        high,
                        jnp.broadcast_to(turned[x, base + k : base + k + 1, :], (8, LANES)),
                        0.0,
                    )
                    for k in range(n_proj)
                ],
                axis=0,
            )
            coarse = spread.astype(BF16)
            left[0:half, cols] = coarse
            left[80 : 80 + half, cols] = (spread - coarse.astype(F32)).astype(BF16)
            right[:, cols] = jnp.where(low, 1.0, 0.0).astype(BF16)
    summed = lax.dot_general(left[...], right[...], NT, preferred_element_type=F32)
    out[0:half, :] = summed[0:half] + summed[80 : 80 + half]
    per = recv.shape[2]
    mixed = jnp.zeros((1, LANES), F32)
    for x in range(n_x):
        mixed += turned[x, n_proj + 1 : n_proj + 2, :]
    out[half : half + 1, :] = jnp.full((1, LANES), total_of(mixed, per), F32)
    for i in (1, 2):
        line = turned[0, n_proj + 1 + i : n_proj + 2 + i, :]
        out[half + i : half + i + 1, :] = jnp.full((1, LANES), total_of(line, per), F32)
    out[half + 3 : half + 8, :] = jnp.zeros((5, LANES), F32)
    ids_out[...] = turned[lax.axis_index("x"), pl.ds(n_proj, n_blk, stride=ROWS), :].astype(jnp.int32)


def lifted(proj, weights, h):
    cols = slice(h * LANES, (h + 1) * LANES)
    n_proj, n_par, _ = proj.shape
    acc = jnp.zeros((n_par, LANES), F32)
    for k in range(n_proj):
        line = weights[k * 8 + h : k * 8 + h + 1, :]
        acc += proj[k, :, cols].astype(F32) * jnp.broadcast_to(line, (n_par, LANES))
    return acc


def projected(proj, field, h, table):
    cols = slice(h * LANES, (h + 1) * LANES)
    for k in range(proj.shape[0]):
        table[k : k + 1, cols] = jnp.sum(
            proj[k, :, cols].astype(F32) * field, axis=0, keepdims=True
        )


def lane_pick(table, low):
    return jnp.take_along_axis(table, low, axis=1, mode="promise_in_bounds")


def send_picks(table, ids, scalars, stage, out):
    n_blk = ids.shape[0]
    n_chunk = table.shape[1] // LANES
    stage[...] = jnp.zeros_like(stage)
    index = ids[...]
    low = index & 127
    high = index >> 7
    for b in range(n_blk):
        low_b = jnp.broadcast_to(low[b : b + 1, :], (8, LANES))
        high_b = jnp.broadcast_to(high[b : b + 1, :], (8, LANES))
        got = jnp.zeros((8, LANES), F32)
        for h in range(n_chunk):
            piece = lane_pick(table[0:8, h * LANES : (h + 1) * LANES], low_b)
            got = jnp.where(high_b == h, piece, got)
        stage[b * ROWS : b * ROWS + 8, :] = got
    got = jnp.zeros((n_blk, LANES), F32)
    for h in range(n_chunk):
        line = jnp.broadcast_to(table[8:9, h * LANES : (h + 1) * LANES], (n_blk, LANES))
        got = jnp.where(high == h, lane_pick(line, low), got)
    stage[pl.ds(8, n_blk, stride=ROWS), :] = got
    for i, value in enumerate(scalars):
        stage[10 + i : 11 + i, :] = jnp.full((1, LANES), value, F32)
    out[...] = stage[...].T.reshape(out.shape)


def start_kernel(own, partner, proj, precond, ids, out, res_out, dir_out, weights, table, stage):
    weights[...] = own[...] + partner[...]
    n_par, width = precond.shape
    for h in range(width // LANES):
        cols = slice(h * LANES, (h + 1) * LANES)
        res = -lifted(proj, weights, h)
        dirn = precond[:, cols] * res
        res_out[:, cols] = res
        dir_out[:, cols] = dirn
        projected(proj, dirn, h, table)
    send_picks(table, ids, (), stage, out)


def step_kernel(
    own, partner, proj, precond, damping, ids, res, dirn, out, image_out, weights, table, stage
):
    weights[...] = own[...] + partner[...]
    n_par, width = precond.shape
    rz = jnp.zeros((n_par, LANES), F32)
    curve = jnp.zeros((n_par, LANES), F32)
    square = jnp.zeros((n_par, LANES), F32)
    for h in range(width // LANES):
        cols = slice(h * LANES, (h + 1) * LANES)
        image = lifted(proj, weights, h) + damping[:, cols] * dirn[:, cols]
        image_out[:, cols] = image
        scaled = precond[:, cols] * image
        projected(proj, scaled, h, table)
        rz += res[:, cols] * dirn[:, cols]
        curve += dirn[:, cols] * image
        square += scaled * image
    send_picks(table, ids, (jnp.sum(rz), jnp.sum(curve), jnp.sum(square)), stage, out)


def last_kernel(
    own, partner, proj, damping, alpha_in, first_dir, res, dirn, sol_out, res_out, weights
):
    weights[...] = own[...] + partner[...]
    rows = proj.shape[0] * 8
    curve = weights[rows : rows + 1, :] + own[rows + 1 : rows + 2, :]
    alpha = own[rows + 2 : rows + 3, :] / curve
    alpha_first = alpha_in[0:1, :]
    for h in range(damping.shape[1] // LANES):
        cols = slice(h * LANES, (h + 1) * LANES)
        image = lifted(proj, weights, h) + damping[:, cols] * dirn[:, cols]
        sol_out[:, cols] = alpha_first * first_dir[:, cols] + alpha * dirn[:, cols]
        res_out[:, cols] = res[:, cols] - alpha * image


def local(jacobian, splat_ids, pix_residual, live_blocks, proj_jac, damping, precond):
    n_blk, n_pix, n_col = jacobian.shape
    n_par, g_dev = damping.shape
    n_scene, n_x = lax.axis_size("scene"), lax.axis_size("x")
    per = LANES // n_scene
    msg = f32(n_scene, per, LANES)
    wide = f32(n_scene, n_x, per, LANES)
    sums = f32(80, LANES)
    state = f32(n_par, g_dev)
    square = pltpu.VMEM((LANES, LANES), F32)
    whole = jax.ShapeDtypeStruct
    weights = pltpu.VMEM((80, LANES), F32)
    table = pltpu.VMEM((16, g_dev), F32)

    def to_owners(message):
        flat = message.reshape(n_scene * n_x, per, LANES)
        got = lax.all_to_all(flat, ("scene", "x"), 0, 0, tiled=True)
        own, index = call(
            sum_kernel,
            (sums, jax.ShapeDtypeStruct((n_blk, LANES), jnp.int32)),
            [VMEM],
            [
                pltpu.VMEM((n_x, LANES, LANES), F32),
                pltpu.VMEM((160, n_x * n_blk * LANES), BF16),
                pltpu.VMEM((LANES, n_x * n_blk * LANES), BF16),
            ],
        )(got.reshape(n_scene, n_x, per, LANES))
        partner = lax.ppermute(own, "core", [(0, 1), (1, 0)])
        return own, partner, index

    def to_blocks(message):
        return lax.all_to_all(message, "scene", 0, 0, tiled=True)

    message, jac, aux = call(
        rhs_kernel,
        (wide, whole(jacobian.shape, BF16), whole((2 * n_blk, LANES), jnp.int32)),
        [HBM] * 4,
        [
            pltpu.VMEM((n_blk, n_pix), BF16),
            pltpu.VMEM((1, live_blocks.shape[0]), jnp.int32),
            pltpu.VMEM((n_blk, LANES), jnp.int32),
            square,
            pltpu.SemaphoreType.DMA((n_blk,)),
            pltpu.SemaphoreType.DMA((3,)),
        ],
    )(*map(in_hbm, (live_blocks.reshape(1, -1), jacobian, pix_residual, splat_ids)))
    own, partner, index = to_owners(message)
    message, res, first_dir = call(
        start_kernel, (msg, state, state), [VMEM] * 5, [weights, table, square]
    )(own, partner, proj_jac, precond, index)
    arrived = to_blocks(message)
    message, picks = call(
        first_kernel,
        (wide, f32(n_blk, n_col)),
        [VMEM] * 3,
        [square, square],
    )(jac, aux, arrived)
    own, partner, index = to_owners(message)
    message, image = call(step_kernel, (msg, state), [VMEM] * 8, [weights, table, square])(
        own, partner, proj_jac, precond, damping, index, res, first_dir
    )
    arrived = to_blocks(message)
    message, res, second_dir, alpha = call(
        second_kernel,
        (wide, state, state, f32(8, LANES)),
        [VMEM] * 9,
        [square, square],
    )(jac, aux, arrived, picks, res, first_dir, image, precond, damping)
    own, partner, index = to_owners(message)
    return call(last_kernel, (state, state), [VMEM] * 8, [weights])(
        own, partner, proj_jac, damping, alpha, first_dir, res, second_dir
    )


def solution(mesh):
    scene = mesh.shape["scene"]
    finer = Mesh(mesh.devices.reshape(scene, -1, 2), ("scene", "x", "core"))
    everywhere = ("scene", "x", "core")
    in_specs = (
        P(everywhere, None, None),
        P(everywhere, None),
        P(everywhere, None),
        P(),
        P(None, None, "scene"),
        P(None, "scene"),
        P(None, "scene"),
    )
    out_specs = (P(None, "scene"), P(None, "scene"))
    return jax.shard_map(local, mesh=finer, in_specs=in_specs, out_specs=out_specs, check_vma=False)
```

```python
import jax
import jax.numpy as jnp
from jax import lax
from jax.experimental import pallas as pl
from jax.experimental.pallas import tpu as pltpu
from jax.sharding import Mesh
from jax.sharding import PartitionSpec as P

F32 = jnp.float32
BF16 = jnp.bfloat16
LANES = 128
ROWS = 16
VMEM = pl.BlockSpec(memory_space=pltpu.VMEM)
HBM = pl.BlockSpec(memory_space=pltpu.HBM)
NT = (((1,), (1,)), ((), ()))


def call(kernel, out, in_specs, scratch=(), flops=1 << 20):
    return pl.pallas_call(
        kernel,
        out_shape=out,
        in_specs=in_specs,
        out_specs=jax.tree.map(lambda _: VMEM, out),
        scratch_shapes=scratch,
        compiler_params=pltpu.CompilerParams(vmem_limit_bytes=24 << 20),
        cost_estimate=pl.CostEstimate(flops=flops, bytes_accessed=1 << 20, transcendentals=0),
    )


def in_hbm(array):
    return pltpu.with_memory_space_constraint(array, pltpu.HBM)


def f32(*shape):
    return jax.ShapeDtypeStruct(shape, F32)


def pack_return(acc, ids, scalars, stage, out):
    n_blk = acc.shape[0]
    n_proj = acc.shape[1] // LANES
    stage[...] = jnp.zeros_like(stage)
    for k in range(n_proj):
        stage[pl.ds(k, n_blk, stride=ROWS), :] = acc[:, k * LANES : (k + 1) * LANES]
    stage[pl.ds(n_proj, n_blk, stride=ROWS), :] = ids.astype(F32)
    for i, value in enumerate(scalars):
        stage[n_proj + 1 + i : n_proj + 2 + i, :] = jnp.full((1, LANES), value, F32)
    turned = stage[...].T.reshape(out.shape[0], *out.shape[2:])
    for x in range(out.shape[1]):
        out[:, x] = turned


def rhs_kernel(
    live, jac, pix, ids, proj, damping, precond,
    out, jbuf, aux, proj_out, damping_out, precond_out,
    pixels, lives, index, stage, sem, small, late,
):
    n_blk = jac.shape[0]
    later = [
        pltpu.make_async_copy(source, target, late.at[i])
        for i, (source, target) in enumerate(
            ((proj, proj_out), (precond, precond_out), (damping, damping_out))
        )
    ]
    minor = [
        pltpu.make_async_copy(pix, pixels, small.at[0]),
        pltpu.make_async_copy(live, lives, small.at[1]),
        pltpu.make_async_copy(ids, index, small.at[2]),
    ]
    copies = [pltpu.make_async_copy(jac.at[b], jbuf.at[b], sem.at[b]) for b in range(n_blk)]
    for copy in minor + copies:
        copy.start()
    for copy in minor:
        copy.wait()
    n_x, n_core = lax.axis_size("x"), lax.axis_size("core")
    position = (lax.axis_index("scene") * n_x + lax.axis_index("x")) * n_core
    position = position + lax.axis_index("core")
    lane = lax.broadcasted_iota(jnp.int32, lives.shape, 1)
    own = jnp.sum(jnp.where(lane == position, lives[...], 0), axis=1, keepdims=True)
    local_ids = index[...] & (LANES * 8 - 1)
    aux[0:n_blk, :] = local_ids
    aux[n_blk : 2 * n_blk, :] = jnp.broadcast_to(own, (n_blk, LANES))
    row = lax.broadcasted_iota(jnp.int32, pix.shape, 0)
    keep = row < jnp.broadcast_to(own, pix.shape)
    values = jnp.where(keep, pixels[...].astype(F32), 0.0)
    acc = jnp.zeros((n_blk, jac.shape[2]), F32)
    for b, copy in enumerate(copies):
        copy.wait()
        if b == n_blk - 2:
            for extra in later:
                extra.start()
        signal = jnp.where(row == b, values, 0.0).astype(BF16)
        acc += jnp.dot(signal, jbuf[b], preferred_element_type=F32)
    pack_return(acc, local_ids, (), stage, out)
    for extra in later:
        extra.wait()


def block_pass(picks, aux, jac):
    n_blk, n_pix = jac.shape[:2]
    row = lax.broadcasted_iota(jnp.int32, (n_blk, n_pix), 0)
    live = row < aux[n_blk : n_blk + 1, 0:1]
    chosen = picks.astype(BF16)
    signals = []
    for b in range(n_blk):
        image = lax.dot_general(chosen, jac[b], NT, preferred_element_type=F32)
        signals.append(jnp.where((row == b) & live, image, 0.0).astype(BF16))
    stacked = jac[...].reshape(n_blk * n_pix, jac.shape[2])
    return jnp.dot(jnp.concatenate(signals, axis=1), stacked, preferred_element_type=F32)


def unpack_picks(recv, turned, n_blk, n_proj):
    turned[...] = recv[...].reshape(LANES, LANES).T
    return jnp.concatenate(
        [turned[pl.ds(k, n_blk, stride=ROWS), :] for k in range(n_proj)], axis=1
    )


def total_of(row, copies):
    return jnp.sum(row) * (1.0 / copies)


def first_kernel(jac, aux, recv, out, picks_out, turned, stage):
    n_blk = jac.shape[0]
    n_proj = jac.shape[2] // LANES
    picks = unpack_picks(recv, turned, n_blk, n_proj)
    picks_out[...] = picks
    acc = block_pass(picks, aux, jac)
    pack_return(acc, aux[0:n_blk, :], (), stage, out)


def second_kernel(
    jac, aux, recv, picks_in, res, dirn, image, precond, damping,
    out, res_out, dir_out, alpha_out, turned, stage,
):
    n_blk = jac.shape[0]
    n_proj = jac.shape[2] // LANES
    fresh = unpack_picks(recv, turned, n_blk, n_proj)
    per = recv.shape[1]
    rz = total_of(turned[n_proj + 1 : n_proj + 2, :], per)
    curve = total_of(turned[n_proj + 2 : n_proj + 3, :], per)
    square = total_of(turned[n_proj + 3 : n_proj + 4, :], per)
    alpha = jnp.full((1, LANES), rz, F32) / jnp.full((1, LANES), curve, F32)
    after = rz - 2.0 * alpha * curve + alpha * alpha * square
    beta = after / jnp.full((1, LANES), rz, F32)
    alpha_out[...] = jnp.broadcast_to(alpha, alpha_out.shape)
    pieces = []
    for k in range(n_proj):
        cols = slice(k * LANES, (k + 1) * LANES)
        pieces.append((1.0 + beta) * picks_in[:, cols] - alpha * fresh[:, cols])
    picks = jnp.concatenate(pieces, axis=1)
    n_par, width = res.shape
    damped = jnp.zeros((n_par, LANES), F32)
    rz_next = jnp.zeros((n_par, LANES), F32)
    for h in range(width // LANES):
        cols = slice(h * LANES, (h + 1) * LANES)
        new_res = res[:, cols] - alpha * image[:, cols]
        precon = precond[:, cols] * new_res
        new_dir = precon + beta * dirn[:, cols]
        res_out[:, cols] = new_res
        dir_out[:, cols] = new_dir
        damped += damping[:, cols] * new_dir * new_dir
        rz_next += new_res * precon
    acc = block_pass(picks, aux, jac)
    scalars = (jnp.sum(picks * acc), jnp.sum(damped), jnp.sum(rz_next))
    pack_return(acc, aux[0:n_blk, :], scalars, stage, out)


def sum_kernel(recv, out, *rest):
    *ids_outs, turned, left, right = rest
    n_x = recv.shape[1]
    n_blk = LANES // ROWS
    n_proj = 9
    sub = lax.broadcasted_iota(jnp.int32, (n_blk, LANES), 0)
    deep = lax.broadcasted_iota(jnp.int32, (LANES, LANES), 0)
    half = n_proj * 8
    for x in range(n_x):
        turned[x] = recv[:, x].reshape(LANES, LANES).T
        for b in range(n_blk):
            at = (x * n_blk + b) * LANES
            cols = slice(at, at + LANES)
            base = b * ROWS
            ids = turned[x, base + n_proj : base + n_proj + 1, :].astype(jnp.int32)
            high = jnp.broadcast_to(ids >> 7, (8, LANES)) == sub
            low = jnp.broadcast_to(ids & 127, (LANES, LANES)) == deep
            spread = jnp.concatenate(
                [
                    jnp.where(
                        high,
                        jnp.broadcast_to(turned[x, base + k : base + k + 1, :], (8, LANES)),
                        0.0,
                    )
                    for k in range(n_proj)
                ],
                axis=0,
            )
            coarse = spread.astype(BF16)
            left[0:half, cols] = coarse
            left[80 : 80 + half, cols] = (spread - coarse.astype(F32)).astype(BF16)
            right[:, cols] = jnp.where(low, 1.0, 0.0).astype(BF16)
    summed = lax.dot_general(left[...], right[...], NT, preferred_element_type=F32)
    out[0:half, :] = summed[0:half] + summed[80 : 80 + half]
    per = recv.shape[2]
    mixed = jnp.zeros((1, LANES), F32)
    for x in range(n_x):
        mixed += turned[x, n_proj + 1 : n_proj + 2, :]
    out[half : half + 1, :] = jnp.full((1, LANES), total_of(mixed, per), F32)
    for i in (1, 2):
        line = turned[0, n_proj + 1 + i : n_proj + 2 + i, :]
        out[half + i : half + i + 1, :] = jnp.full((1, LANES), total_of(line, per), F32)
    out[half + 3 : half + 8, :] = jnp.zeros((5, LANES), F32)
    for ids_out in ids_outs:
        ids_out[...] = turned[lax.axis_index("x"), pl.ds(n_proj, n_blk, stride=ROWS), :].astype(jnp.int32)


def lifted(proj, weights, h):
    cols = slice(h * LANES, (h + 1) * LANES)
    n_proj, n_par, _ = proj.shape
    acc = jnp.zeros((n_par, LANES), F32)
    for k in range(n_proj):
        line = weights[k * 8 + h : k * 8 + h + 1, :]
        acc += proj[k, :, cols].astype(F32) * jnp.broadcast_to(line, (n_par, LANES))
    return acc


def projected(proj, field, h, table):
    cols = slice(h * LANES, (h + 1) * LANES)
    for k in range(proj.shape[0]):
        table[k : k + 1, cols] = jnp.sum(
            proj[k, :, cols].astype(F32) * field, axis=0, keepdims=True
        )


def lane_pick(table, low):
    return jnp.take_along_axis(table, low, axis=1, mode="promise_in_bounds")


def send_picks(table, ids, scalars, stage, out):
    n_blk = ids.shape[0]
    n_chunk = table.shape[1] // LANES
    stage[...] = jnp.zeros_like(stage)
    index = ids[...]
    low = index & 127
    high = index >> 7
    for b in range(n_blk):
        low_b = jnp.broadcast_to(low[b : b + 1, :], (8, LANES))
        high_b = jnp.broadcast_to(high[b : b + 1, :], (8, LANES))
        got = jnp.zeros((8, LANES), F32)
        for h in range(n_chunk):
            piece = lane_pick(table[0:8, h * LANES : (h + 1) * LANES], low_b)
            got = jnp.where(high_b == h, piece, got)
        stage[b * ROWS : b * ROWS + 8, :] = got
    got = jnp.zeros((n_blk, LANES), F32)
    for h in range(n_chunk):
        line = jnp.broadcast_to(table[8:9, h * LANES : (h + 1) * LANES], (n_blk, LANES))
        got = jnp.where(high == h, lane_pick(line, low), got)
    stage[pl.ds(8, n_blk, stride=ROWS), :] = got
    for i, value in enumerate(scalars):
        stage[10 + i : 11 + i, :] = jnp.full((1, LANES), value, F32)
    out[...] = stage[...].T.reshape(out.shape)


def start_kernel(own, partner, proj, precond, ids, out, res_out, dir_out, weights, table, stage):
    weights[...] = own[...] + partner[...]
    n_par, width = precond.shape
    for h in range(width // LANES):
        cols = slice(h * LANES, (h + 1) * LANES)
        res = -lifted(proj, weights, h)
        dirn = precond[:, cols] * res
        res_out[:, cols] = res
        dir_out[:, cols] = dirn
        projected(proj, dirn, h, table)
    send_picks(table, ids, (), stage, out)


def step_kernel(
    own, partner, proj, precond, damping, ids, res, dirn, out, image_out, weights, table, stage
):
    weights[...] = own[...] + partner[...]
    n_par, width = precond.shape
    rz = jnp.zeros((n_par, LANES), F32)
    curve = jnp.zeros((n_par, LANES), F32)
    square = jnp.zeros((n_par, LANES), F32)
    for h in range(width // LANES):
        cols = slice(h * LANES, (h + 1) * LANES)
        image = lifted(proj, weights, h) + damping[:, cols] * dirn[:, cols]
        image_out[:, cols] = image
        scaled = precond[:, cols] * image
        projected(proj, scaled, h, table)
        rz += res[:, cols] * dirn[:, cols]
        curve += dirn[:, cols] * image
        square += scaled * image
    send_picks(table, ids, (jnp.sum(rz), jnp.sum(curve), jnp.sum(square)), stage, out)


def last_kernel(
    own, partner, proj, damping, alpha_in, first_dir, res, dirn, sol_out, res_out, weights
):
    weights[...] = own[...] + partner[...]
    rows = proj.shape[0] * 8
    curve = weights[rows : rows + 1, :] + own[rows + 1 : rows + 2, :]
    alpha = own[rows + 2 : rows + 3, :] / curve
    alpha_first = alpha_in[0:1, :]
    for h in range(damping.shape[1] // LANES):
        cols = slice(h * LANES, (h + 1) * LANES)
        image = lifted(proj, weights, h) + damping[:, cols] * dirn[:, cols]
        sol_out[:, cols] = alpha_first * first_dir[:, cols] + alpha * dirn[:, cols]
        res_out[:, cols] = res[:, cols] - alpha * image


def local(jacobian, splat_ids, pix_residual, live_blocks, proj_jac, damping, precond):
    n_blk, n_pix, n_col = jacobian.shape
    n_par, g_dev = damping.shape
    n_scene, n_x = lax.axis_size("scene"), lax.axis_size("x")
    per = LANES // n_scene
    msg = f32(n_scene, per, LANES)
    wide = f32(n_scene, n_x, per, LANES)
    sums = f32(80, LANES)
    state = f32(n_par, g_dev)
    square = pltpu.VMEM((LANES, LANES), F32)
    whole = jax.ShapeDtypeStruct
    weights = pltpu.VMEM((80, LANES), F32)
    table = pltpu.VMEM((16, g_dev), F32)

    def to_owners(message, indices):
        flat = message.reshape(n_scene * n_x, per, LANES)
        got = lax.all_to_all(flat, ("scene", "x"), 0, 0, tiled=True)
        own, *index = call(
            sum_kernel,
            (sums,) + (whole((n_blk, LANES), jnp.int32),) * indices,
            [VMEM],
            [
                pltpu.VMEM((n_x, LANES, LANES), F32),
                pltpu.VMEM((160, n_x * n_blk * LANES), BF16),
                pltpu.VMEM((LANES, n_x * n_blk * LANES), BF16),
            ],
        )(got.reshape(n_scene, n_x, per, LANES))
        partner = lax.ppermute(own, "core", [(0, 1), (1, 0)])
        return own, partner, *index

    def to_blocks(message):
        return lax.all_to_all(message, "scene", 0, 0, tiled=True)

    message, jac, aux, proj, damping, precond = call(
        rhs_kernel,
        (wide, whole(jacobian.shape, BF16), whole((2 * n_blk, LANES), jnp.int32))
        + (whole(proj_jac.shape, BF16), state, state),
        [HBM] * 7,
        [
            pltpu.VMEM((n_blk, n_pix), BF16),
            pltpu.VMEM((1, live_blocks.shape[0]), jnp.int32),
            pltpu.VMEM((n_blk, LANES), jnp.int32),
            square,
            pltpu.SemaphoreType.DMA((n_blk,)),
            pltpu.SemaphoreType.DMA((3,)),
            pltpu.SemaphoreType.DMA((3,)),
        ],
    )(
        *map(in_hbm, (live_blocks.reshape(1, -1), jacobian, pix_residual, splat_ids)),
        *map(in_hbm, (proj_jac, damping, precond)),
    )
    own, partner, index = to_owners(message, 1)
    message, res, first_dir = call(
        start_kernel, (msg, state, state), [VMEM] * 5, [weights, table, square]
    )(own, partner, proj, precond, index)
    arrived = to_blocks(message)
    message, picks = call(
        first_kernel,
        (wide, f32(n_blk, n_col)),
        [VMEM] * 3,
        [square, square],
    )(jac, aux, arrived)
    own, partner = to_owners(message, 0)
    message, image = call(step_kernel, (msg, state), [VMEM] * 8, [weights, table, square])(
        own, partner, proj, precond, damping, index, res, first_dir
    )
    arrived = to_blocks(message)
    message, res, second_dir, alpha = call(
        second_kernel,
        (wide, state, state, f32(8, LANES)),
        [VMEM] * 9,
        [square, square],
    )(jac, aux, arrived, picks, res, first_dir, image, precond, damping)
    own, partner = to_owners(message, 0)
    return call(last_kernel, (state, state), [VMEM] * 8, [weights])(
        own, partner, proj, damping, alpha, first_dir, res, second_dir
    )


def solution(mesh):
    scene = mesh.shape["scene"]
    finer = Mesh(mesh.devices.reshape(scene, -1, 2), ("scene", "x", "core"))
    everywhere = ("scene", "x", "core")
    in_specs = (
        P(everywhere, None, None),
        P(everywhere, None),
        P(everywhere, None),
        P(),
        P(None, None, "scene"),
        P(None, "scene"),
        P(None, "scene"),
    )
    out_specs = (P(None, "scene"), P(None, "scene"))
    return jax.shard_map(local, mesh=finer, in_specs=in_specs, out_specs=out_specs, check_vma=False)
```

```python
import jax
import jax.numpy as jnp
from jax import lax
from jax.experimental import pallas as pl
from jax.experimental.pallas import tpu as pltpu
from jax.sharding import Mesh
from jax.sharding import PartitionSpec as P

F32 = jnp.float32
BF16 = jnp.bfloat16
LANES = 128
ROWS = 16
VMEM = pl.BlockSpec(memory_space=pltpu.VMEM)
HBM = pl.BlockSpec(memory_space=pltpu.HBM)
NT = (((1,), (1,)), ((), ()))


def call(kernel, out, in_specs, scratch=(), flops=1 << 20):
    return pl.pallas_call(
        kernel,
        out_shape=out,
        in_specs=in_specs,
        out_specs=jax.tree.map(lambda _: VMEM, out),
        scratch_shapes=scratch,
        compiler_params=pltpu.CompilerParams(vmem_limit_bytes=24 << 20),
        cost_estimate=pl.CostEstimate(flops=flops, bytes_accessed=1 << 20, transcendentals=0),
    )


def in_hbm(array):
    return pltpu.with_memory_space_constraint(array, pltpu.HBM)


def f32(*shape):
    return jax.ShapeDtypeStruct(shape, F32)


def pack_return(acc, ids, scalars, stage, out):
    n_blk = acc.shape[0]
    n_proj = acc.shape[1] // LANES
    stage[...] = jnp.zeros_like(stage)
    for k in range(n_proj):
        stage[pl.ds(k, n_blk, stride=ROWS), :] = acc[:, k * LANES : (k + 1) * LANES]
    stage[pl.ds(n_proj, n_blk, stride=ROWS), :] = ids.astype(F32)
    for i, value in enumerate(scalars):
        stage[n_proj + 1 + i : n_proj + 2 + i, :] = jnp.full((1, LANES), value, F32)
    turned = stage[...].T.reshape(out.shape[0], *out.shape[2:])
    for x in range(out.shape[1]):
        out[:, x] = turned


def rhs_kernel(live, jac, pix, ids, out, jbuf, aux, pixels, lives, index, stage, sem, small):
    n_blk = jac.shape[0]
    minor = [
        pltpu.make_async_copy(pix, pixels, small.at[0]),
        pltpu.make_async_copy(live, lives, small.at[1]),
        pltpu.make_async_copy(ids, index, small.at[2]),
    ]
    copies = [pltpu.make_async_copy(jac.at[b], jbuf.at[b], sem.at[b]) for b in range(n_blk)]
    for copy in minor + copies:
        copy.start()
    for copy in minor:
        copy.wait()
    n_x, n_core = lax.axis_size("x"), lax.axis_size("core")
    position = (lax.axis_index("scene") * n_x + lax.axis_index("x")) * n_core
    position = position + lax.axis_index("core")
    lane = lax.broadcasted_iota(jnp.int32, lives.shape, 1)
    own = jnp.sum(jnp.where(lane == position, lives[...], 0), axis=1, keepdims=True)
    local_ids = index[...] & (LANES * 8 - 1)
    aux[0:n_blk, :] = local_ids
    aux[n_blk : 2 * n_blk, :] = jnp.broadcast_to(own, (n_blk, LANES))
    row = lax.broadcasted_iota(jnp.int32, pix.shape, 0)
    keep = row < jnp.broadcast_to(own, pix.shape)
    values = jnp.where(keep, pixels[...].astype(F32), 0.0)
    acc = jnp.zeros((n_blk, jac.shape[2]), F32)
    for b, copy in enumerate(copies):
        copy.wait()
        signal = jnp.where(row == b, values, 0.0).astype(BF16)
        acc += jnp.dot(signal, jbuf[b], preferred_element_type=F32)
    pack_return(acc, local_ids, (), stage, out)


def block_pass(picks, aux, jac):
    n_blk, n_pix = jac.shape[:2]
    row = lax.broadcasted_iota(jnp.int32, (n_blk, n_pix), 0)
    live = row < aux[n_blk : n_blk + 1, 0:1]
    chosen = picks.astype(BF16)
    signals = []
    for b in range(n_blk):
        image = lax.dot_general(chosen, jac[b], NT, preferred_element_type=F32)
        signals.append(jnp.where((row == b) & live, image, 0.0).astype(BF16))
    stacked = jac[...].reshape(n_blk * n_pix, jac.shape[2])
    return jnp.dot(jnp.concatenate(signals, axis=1), stacked, preferred_element_type=F32)


def unpack_picks(recv, turned, n_blk, n_proj):
    turned[...] = recv[...].reshape(LANES, LANES).T
    return jnp.concatenate(
        [turned[pl.ds(k, n_blk, stride=ROWS), :] for k in range(n_proj)], axis=1
    )


def total_of(row, copies):
    return jnp.sum(row) * (1.0 / copies)


def first_kernel(jac, aux, recv, out, picks_out, turned, stage):
    n_blk = jac.shape[0]
    n_proj = jac.shape[2] // LANES
    picks = unpack_picks(recv, turned, n_blk, n_proj)
    picks_out[...] = picks
    acc = block_pass(picks, aux, jac)
    pack_return(acc, aux[0:n_blk, :], (), stage, out)


def second_kernel(
    jac, aux, recv, picks_in, res, dirn, image, precond, damping,
    out, res_out, dir_out, alpha_out, turned, stage,
):
    n_blk = jac.shape[0]
    n_proj = jac.shape[2] // LANES
    fresh = unpack_picks(recv, turned, n_blk, n_proj)
    per = recv.shape[1]
    rz = total_of(turned[n_proj + 1 : n_proj + 2, :], per)
    curve = total_of(turned[n_proj + 2 : n_proj + 3, :], per)
    square = total_of(turned[n_proj + 3 : n_proj + 4, :], per)
    alpha = jnp.full((1, LANES), rz, F32) / jnp.full((1, LANES), curve, F32)
    after = rz - 2.0 * alpha * curve + alpha * alpha * square
    beta = after / jnp.full((1, LANES), rz, F32)
    alpha_out[...] = jnp.broadcast_to(alpha, alpha_out.shape)
    pieces = []
    for k in range(n_proj):
        cols = slice(k * LANES, (k + 1) * LANES)
        pieces.append((1.0 + beta) * picks_in[:, cols] - alpha * fresh[:, cols])
    picks = jnp.concatenate(pieces, axis=1)
    n_par, width = res.shape
    damped = jnp.zeros((n_par, LANES), F32)
    rz_next = jnp.zeros((n_par, LANES), F32)
    for h in range(width // LANES):
        cols = slice(h * LANES, (h + 1) * LANES)
        new_res = res[:, cols] - alpha * image[:, cols]
        precon = precond[:, cols] * new_res
        new_dir = precon + beta * dirn[:, cols]
        res_out[:, cols] = new_res
        dir_out[:, cols] = new_dir
        damped += damping[:, cols] * new_dir * new_dir
        rz_next += new_res * precon
    acc = block_pass(picks, aux, jac)
    scalars = (jnp.sum(picks * acc), jnp.sum(damped), jnp.sum(rz_next))
    pack_return(acc, aux[0:n_blk, :], scalars, stage, out)


def sum_kernel(recv, out, *rest):
    *ids_outs, turned, left, right = rest
    n_x = recv.shape[1]
    n_blk = LANES // ROWS
    n_proj = 9
    sub = lax.broadcasted_iota(jnp.int32, (n_blk, LANES), 0)
    deep = lax.broadcasted_iota(jnp.int32, (LANES, LANES), 0)
    half = n_proj * 8
    for x in range(n_x):
        turned[x] = recv[:, x].reshape(LANES, LANES).T
        for b in range(n_blk):
            at = (x * n_blk + b) * LANES
            cols = slice(at, at + LANES)
            base = b * ROWS
            ids = turned[x, base + n_proj : base + n_proj + 1, :].astype(jnp.int32)
            high = jnp.broadcast_to(ids >> 7, (8, LANES)) == sub
            low = jnp.broadcast_to(ids & 127, (LANES, LANES)) == deep
            spread = jnp.concatenate(
                [
                    jnp.where(
                        high,
                        jnp.broadcast_to(turned[x, base + k : base + k + 1, :], (8, LANES)),
                        0.0,
                    )
                    for k in range(n_proj)
                ],
                axis=0,
            )
            coarse = spread.astype(BF16)
            left[0:half, cols] = coarse
            left[80 : 80 + half, cols] = (spread - coarse.astype(F32)).astype(BF16)
            right[:, cols] = jnp.where(low, 1.0, 0.0).astype(BF16)
    summed = lax.dot_general(left[...], right[...], NT, preferred_element_type=F32)
    out[0:half, :] = summed[0:half] + summed[80 : 80 + half]
    per = recv.shape[2]
    mixed = jnp.zeros((1, LANES), F32)
    for x in range(n_x):
        mixed += turned[x, n_proj + 1 : n_proj + 2, :]
    out[half : half + 1, :] = jnp.full((1, LANES), total_of(mixed, per), F32)
    for i in (1, 2):
        line = turned[0, n_proj + 1 + i : n_proj + 2 + i, :]
        out[half + i : half + i + 1, :] = jnp.full((1, LANES), total_of(line, per), F32)
    out[half + 3 : half + 8, :] = jnp.zeros((5, LANES), F32)
    for ids_out in ids_outs:
        ids_out[...] = turned[lax.axis_index("x"), pl.ds(n_proj, n_blk, stride=ROWS), :].astype(jnp.int32)


def lifted(proj, weights, h):
    cols = slice(h * LANES, (h + 1) * LANES)
    n_proj, n_par, _ = proj.shape
    acc = jnp.zeros((n_par, LANES), F32)
    for k in range(n_proj):
        line = weights[k * 8 + h : k * 8 + h + 1, :]
        acc += proj[k, :, cols].astype(F32) * jnp.broadcast_to(line, (n_par, LANES))
    return acc


def projected(proj, field, h, table):
    cols = slice(h * LANES, (h + 1) * LANES)
    for k in range(proj.shape[0]):
        table[k : k + 1, cols] = jnp.sum(
            proj[k, :, cols].astype(F32) * field, axis=0, keepdims=True
        )


def lane_pick(table, low):
    return jnp.take_along_axis(table, low, axis=1, mode="promise_in_bounds")


def send_picks(table, ids, scalars, stage, out):
    n_blk = ids.shape[0]
    n_chunk = table.shape[1] // LANES
    stage[...] = jnp.zeros_like(stage)
    index = ids[...]
    low = index & 127
    high = index >> 7
    for b in range(n_blk):
        low_b = jnp.broadcast_to(low[b : b + 1, :], (8, LANES))
        high_b = jnp.broadcast_to(high[b : b + 1, :], (8, LANES))
        got = jnp.zeros((8, LANES), F32)
        for h in range(n_chunk):
            piece = lane_pick(table[0:8, h * LANES : (h + 1) * LANES], low_b)
            got = jnp.where(high_b == h, piece, got)
        stage[b * ROWS : b * ROWS + 8, :] = got
    got = jnp.zeros((n_blk, LANES), F32)
    for h in range(n_chunk):
        line = jnp.broadcast_to(table[8:9, h * LANES : (h + 1) * LANES], (n_blk, LANES))
        got = jnp.where(high == h, lane_pick(line, low), got)
    stage[pl.ds(8, n_blk, stride=ROWS), :] = got
    for i, value in enumerate(scalars):
        stage[10 + i : 11 + i, :] = jnp.full((1, LANES), value, F32)
    out[...] = stage[...].T.reshape(out.shape)


def start_kernel(own, partner, proj, precond, ids, out, res_out, dir_out, weights, table, stage):
    weights[...] = own[...] + partner[...]
    n_par, width = precond.shape
    for h in range(width // LANES):
        cols = slice(h * LANES, (h + 1) * LANES)
        res = -lifted(proj, weights, h)
        dirn = precond[:, cols] * res
        res_out[:, cols] = res
        dir_out[:, cols] = dirn
        projected(proj, dirn, h, table)
    send_picks(table, ids, (), stage, out)


def step_kernel(
    own, partner, proj, precond, damping, ids, res, dirn, out, image_out, weights, table, stage
):
    weights[...] = own[...] + partner[...]
    n_par, width = precond.shape
    rz = jnp.zeros((n_par, LANES), F32)
    curve = jnp.zeros((n_par, LANES), F32)
    square = jnp.zeros((n_par, LANES), F32)
    for h in range(width // LANES):
        cols = slice(h * LANES, (h + 1) * LANES)
        image = lifted(proj, weights, h) + damping[:, cols] * dirn[:, cols]
        image_out[:, cols] = image
        scaled = precond[:, cols] * image
        projected(proj, scaled, h, table)
        rz += res[:, cols] * dirn[:, cols]
        curve += dirn[:, cols] * image
        square += scaled * image
    send_picks(table, ids, (jnp.sum(rz), jnp.sum(curve), jnp.sum(square)), stage, out)


def last_kernel(
    own, partner, proj, damping, alpha_in, first_dir, res, dirn, sol_out, res_out, weights
):
    weights[...] = own[...] + partner[...]
    rows = proj.shape[0] * 8
    curve = weights[rows : rows + 1, :] + own[rows + 1 : rows + 2, :]
    alpha = own[rows + 2 : rows + 3, :] / curve
    alpha_first = alpha_in[0:1, :]
    for h in range(damping.shape[1] // LANES):
        cols = slice(h * LANES, (h + 1) * LANES)
        image = lifted(proj, weights, h) + damping[:, cols] * dirn[:, cols]
        sol_out[:, cols] = alpha_first * first_dir[:, cols] + alpha * dirn[:, cols]
        res_out[:, cols] = res[:, cols] - alpha * image


def local(jacobian, splat_ids, pix_residual, live_blocks, proj_jac, damping, precond):
    n_blk, n_pix, n_col = jacobian.shape
    n_par, g_dev = damping.shape
    n_scene, n_x = lax.axis_size("scene"), lax.axis_size("x")
    per = LANES // n_scene
    msg = f32(n_scene, per, LANES)
    wide = f32(n_scene, n_x, per, LANES)
    sums = f32(80, LANES)
    state = f32(n_par, g_dev)
    square = pltpu.VMEM((LANES, LANES), F32)
    whole = jax.ShapeDtypeStruct
    weights = pltpu.VMEM((80, LANES), F32)
    table = pltpu.VMEM((16, g_dev), F32)

    def to_owners(message, indices):
        flat = message.reshape(n_scene * n_x, per, LANES)
        got = lax.all_to_all(flat, ("scene", "x"), 0, 0, tiled=True)
        own, *index = call(
            sum_kernel,
            (sums,) + (whole((n_blk, LANES), jnp.int32),) * indices,
            [VMEM],
            [
                pltpu.VMEM((n_x, LANES, LANES), F32),
                pltpu.VMEM((160, n_x * n_blk * LANES), BF16),
                pltpu.VMEM((LANES, n_x * n_blk * LANES), BF16),
            ],
            2147483648,
        )(got.reshape(n_scene, n_x, per, LANES))
        partner = lax.ppermute(own, "core", [(0, 1), (1, 0)])
        return own, partner, *index

    def to_blocks(message):
        return lax.all_to_all(message, "scene", 0, 0, tiled=True)

    message, jac, aux = call(
        rhs_kernel,
        (wide, whole(jacobian.shape, BF16), whole((2 * n_blk, LANES), jnp.int32)),
        [HBM] * 4,
        [
            pltpu.VMEM((n_blk, n_pix), BF16),
            pltpu.VMEM((1, live_blocks.shape[0]), jnp.int32),
            pltpu.VMEM((n_blk, LANES), jnp.int32),
            square,
            pltpu.SemaphoreType.DMA((n_blk,)),
            pltpu.SemaphoreType.DMA((3,)),
        ],
    )(*map(in_hbm, (live_blocks.reshape(1, -1), jacobian, pix_residual, splat_ids)))
    own, partner, index = to_owners(message, 1)
    message, res, first_dir = call(
        start_kernel, (msg, state, state), [VMEM] * 5, [weights, table, square]
    )(own, partner, proj_jac, precond, index)
    arrived = to_blocks(message)
    message, picks = call(
        first_kernel,
        (wide, f32(n_blk, n_col)),
        [VMEM] * 3,
        [square, square],
    )(jac, aux, arrived)
    own, partner = to_owners(message, 0)
    message, image = call(step_kernel, (msg, state), [VMEM] * 8, [weights, table, square])(
        own, partner, proj_jac, precond, damping, index, res, first_dir
    )
    arrived = to_blocks(message)
    message, res, second_dir, alpha = call(
        second_kernel,
        (wide, state, state, f32(8, LANES)),
        [VMEM] * 9,
        [square, square],
    )(jac, aux, arrived, picks, res, first_dir, image, precond, damping)
    own, partner = to_owners(message, 0)
    return call(last_kernel, (state, state), [VMEM] * 8, [weights])(
        own, partner, proj_jac, damping, alpha, first_dir, res, second_dir
    )


def solution(mesh):
    scene = mesh.shape["scene"]
    finer = Mesh(mesh.devices.reshape(scene, -1, 2), ("scene", "x", "core"))
    everywhere = ("scene", "x", "core")
    in_specs = (
        P(everywhere, None, None),
        P(everywhere, None),
        P(everywhere, None),
        P(),
        P(None, None, "scene"),
        P(None, "scene"),
        P(None, "scene"),
    )
    out_specs = (P(None, "scene"), P(None, "scene"))
    return jax.shard_map(local, mesh=finer, in_specs=in_specs, out_specs=out_specs, check_vma=False)
```

```python
import functools

import jax
import jax.numpy as jnp
from jax import lax
from jax.experimental import pallas as pl
from jax.experimental.pallas import tpu as pltpu
from jax.sharding import Mesh
from jax.sharding import PartitionSpec as P

F32 = jnp.float32
BF16 = jnp.bfloat16
LANES = 128
ROWS = 16
VMEM = pl.BlockSpec(memory_space=pltpu.VMEM)
HBM = pl.BlockSpec(memory_space=pltpu.HBM)
NT = (((1,), (1,)), ((), ()))


def call(kernel, out, in_specs, scratch=(), flops=1 << 20, out_space=VMEM):
    return pl.pallas_call(
        kernel,
        out_shape=out,
        in_specs=in_specs,
        out_specs=jax.tree.map(lambda _: out_space, out),
        scratch_shapes=scratch,
        compiler_params=pltpu.CompilerParams(vmem_limit_bytes=24 << 20),
        cost_estimate=pl.CostEstimate(flops=flops, bytes_accessed=1 << 20, transcendentals=0),
    )


def in_hbm(array):
    return pltpu.with_memory_space_constraint(array, pltpu.HBM)


def f32(*shape):
    return jax.ShapeDtypeStruct(shape, F32)


def pack_return(acc, ids, scalars, stage, out):
    n_blk = acc.shape[0]
    n_proj = acc.shape[1] // LANES
    stage[...] = jnp.zeros_like(stage)
    for k in range(n_proj):
        stage[pl.ds(k, n_blk, stride=ROWS), :] = acc[:, k * LANES : (k + 1) * LANES]
    stage[pl.ds(n_proj, n_blk, stride=ROWS), :] = ids.astype(F32)
    for i, value in enumerate(scalars):
        stage[n_proj + 1 + i : n_proj + 2 + i, :] = jnp.full((1, LANES), value, F32)
    turned = stage[...].T.reshape(out.shape[0], *out.shape[2:])
    for x in range(out.shape[1]):
        out[:, x] = turned


def rhs_kernel(live, jac, pix, ids, out, jbuf, aux, pixels, lives, index, stage, sem, small):
    n_blk = jac.shape[0]
    minor = [
        pltpu.make_async_copy(pix, pixels, small.at[0]),
        pltpu.make_async_copy(live, lives, small.at[1]),
        pltpu.make_async_copy(ids, index, small.at[2]),
    ]
    copies = [pltpu.make_async_copy(jac.at[b], jbuf.at[b], sem.at[b]) for b in range(n_blk)]
    for copy in minor + copies:
        copy.start()
    for copy in minor:
        copy.wait()
    n_x, n_core = lax.axis_size("x"), lax.axis_size("core")
    position = (lax.axis_index("scene") * n_x + lax.axis_index("x")) * n_core
    position = position + lax.axis_index("core")
    lane = lax.broadcasted_iota(jnp.int32, lives.shape, 1)
    own = jnp.sum(jnp.where(lane == position, lives[...], 0), axis=1, keepdims=True)
    local_ids = index[...] & (LANES * 8 - 1)
    aux[0:n_blk, :] = local_ids
    aux[n_blk : 2 * n_blk, :] = jnp.broadcast_to(own, (n_blk, LANES))
    row = lax.broadcasted_iota(jnp.int32, pix.shape, 0)
    keep = row < jnp.broadcast_to(own, pix.shape)
    values = jnp.where(keep, pixels[...].astype(F32), 0.0)
    n_pix, n_col = jac.shape[1:]
    acc = jnp.zeros((n_blk, n_col), F32)
    cut = n_blk * 3 // 4
    for first, last in ((0, cut), (cut, n_blk)):
        signals = [jnp.where(row == b, values, 0.0).astype(BF16) for b in range(first, last)]
        for copy in copies[first:last]:
            copy.wait()
        stacked = jbuf[first:last].reshape((last - first) * n_pix, n_col)
        acc += jnp.dot(jnp.concatenate(signals, axis=1), stacked, preferred_element_type=F32)
    pack_return(acc, local_ids, (), stage, out)


def block_pass(picks, aux, jac, beside=None):
    n_blk, n_pix = jac.shape[:2]
    row = lax.broadcasted_iota(jnp.int32, (n_blk, n_pix), 0)
    live = row < aux[n_blk : n_blk + 1, 0:1]
    chosen = picks.astype(BF16)
    signals = []
    for b in range(n_blk):
        image = lax.dot_general(chosen, jac[b], NT, preferred_element_type=F32)
        if beside is not None:
            beside(b)
        signals.append(jnp.where((row == b) & live, image, 0.0).astype(BF16))
    stacked = jac[...].reshape(n_blk * n_pix, jac.shape[2])
    return jnp.dot(jnp.concatenate(signals, axis=1), stacked, preferred_element_type=F32)


def unpack_picks(recv, turned, n_blk, n_proj):
    turned[...] = recv[...].reshape(LANES, LANES).T
    return jnp.concatenate(
        [turned[pl.ds(k, n_blk, stride=ROWS), :] for k in range(n_proj)], axis=1
    )


def total_of(row, copies):
    return jnp.sum(row) * (1.0 / copies)


def first_kernel(jac, aux, recv, out, picks_out, turned, stage):
    n_blk = jac.shape[0]
    n_proj = jac.shape[2] // LANES
    picks = unpack_picks(recv, turned, n_blk, n_proj)
    picks_out[...] = picks
    acc = block_pass(picks, aux, jac)
    pack_return(acc, aux[0:n_blk, :], (), stage, out)


def second_kernel(
    jac, aux, recv, picks_in, res, dirn, image, precond, damping,
    out, res_out, dir_out, alpha_out, turned, stage,
):
    n_blk = jac.shape[0]
    n_proj = jac.shape[2] // LANES
    fresh = unpack_picks(recv, turned, n_blk, n_proj)
    per = recv.shape[1]
    rz = total_of(turned[n_proj + 1 : n_proj + 2, :], per)
    curve = total_of(turned[n_proj + 2 : n_proj + 3, :], per)
    square = total_of(turned[n_proj + 3 : n_proj + 4, :], per)
    alpha = jnp.full((1, LANES), rz, F32) / jnp.full((1, LANES), curve, F32)
    after = rz - 2.0 * alpha * curve + alpha * alpha * square
    beta = after / jnp.full((1, LANES), rz, F32)
    alpha_out[...] = jnp.broadcast_to(alpha, alpha_out.shape)
    pieces = []
    for k in range(n_proj):
        cols = slice(k * LANES, (k + 1) * LANES)
        pieces.append((1.0 + beta) * picks_in[:, cols] - alpha * fresh[:, cols])
    picks = jnp.concatenate(pieces, axis=1)
    n_par, width = res.shape
    sums = [jnp.zeros((n_par, LANES), F32)] * 2

    def update(h):
        cols = slice(h * LANES, (h + 1) * LANES)
        new_res = res[:, cols] - alpha * image[:, cols]
        precon = precond[:, cols] * new_res
        new_dir = precon + beta * dirn[:, cols]
        res_out[:, cols] = new_res
        dir_out[:, cols] = new_dir
        sums[0] += damping[:, cols] * new_dir * new_dir
        sums[1] += new_res * precon

    acc = block_pass(picks, aux, jac, update)
    scalars = (jnp.sum(picks * acc), jnp.sum(sums[0]), jnp.sum(sums[1]))
    pack_return(acc, aux[0:n_blk, :], scalars, stage, out)


def sum_kernel(first, recv, *rest):
    if first:
        out, ids_out, right, turned, fine, left = rest
    else:
        right, out, turned, fine, left = rest
    n_x = recv.shape[1]
    n_blk = LANES // ROWS
    n_proj = 9
    sub = lax.broadcasted_iota(jnp.int32, (n_blk, LANES), 0)
    deep = lax.broadcasted_iota(jnp.int32, (LANES, LANES), 0)
    half = n_proj * 8

    def spread(table, x, base, high):
        lines = [
            jnp.broadcast_to(table[x, base + k : base + k + 1, :], (8, LANES))
            for k in range(n_proj)
        ]
        return jnp.concatenate([jnp.where(high, line, 0.0) for line in lines], axis=0)

    for x in range(n_x):
        values = recv[:, x].reshape(LANES, LANES).T
        turned[x] = values
        fine[x] = values - values.astype(BF16).astype(F32)
        for b in range(n_blk):
            at = (x * n_blk + b) * LANES
            cols = slice(at, at + LANES)
            base = b * ROWS
            ids = turned[x, base + n_proj : base + n_proj + 1, :].astype(jnp.int32)
            high = jnp.broadcast_to(ids >> 7, (8, LANES)) == sub
            left[0:half, cols] = spread(turned, x, base, high).astype(BF16)
            left[80 : 80 + half, cols] = spread(fine, x, base, high).astype(BF16)
            if first:
                low = jnp.broadcast_to(ids & 127, (LANES, LANES)) == deep
                right[:, cols] = jnp.where(low, 1.0, 0.0).astype(BF16)
    summed = lax.dot_general(left[...], right[...], NT, preferred_element_type=F32)
    out[0:half, :] = summed[0:half] + summed[80 : 80 + half]
    per = recv.shape[2]
    mixed = jnp.zeros((1, LANES), F32)
    for x in range(n_x):
        mixed += turned[x, n_proj + 1 : n_proj + 2, :]
    out[half : half + 1, :] = jnp.full((1, LANES), total_of(mixed, per), F32)
    for i in (1, 2):
        line = turned[0, n_proj + 1 + i : n_proj + 2 + i, :]
        out[half + i : half + i + 1, :] = jnp.full((1, LANES), total_of(line, per), F32)
    out[half + 3 : half + 8, :] = jnp.zeros((5, LANES), F32)
    if first:
        ids_out[...] = turned[lax.axis_index("x"), pl.ds(n_proj, n_blk, stride=ROWS), :].astype(jnp.int32)


def lifted(proj, weights, h):
    cols = slice(h * LANES, (h + 1) * LANES)
    n_proj, n_par, _ = proj.shape
    acc = jnp.zeros((n_par, LANES), F32)
    for k in range(n_proj):
        line = weights[k * 8 + h : k * 8 + h + 1, :]
        acc += proj[k, :, cols].astype(F32) * jnp.broadcast_to(line, (n_par, LANES))
    return acc


def projected(proj, field, h, table):
    cols = slice(h * LANES, (h + 1) * LANES)
    for k in range(proj.shape[0]):
        table[k : k + 1, cols] = jnp.sum(
            proj[k, :, cols].astype(F32) * field, axis=0, keepdims=True
        )


def lane_pick(table, low):
    return jnp.take_along_axis(table, low, axis=1, mode="promise_in_bounds")


def send_picks(table, ids, scalars, stage, out):
    n_blk = ids.shape[0]
    n_chunk = table.shape[1] // LANES
    stage[...] = jnp.zeros_like(stage)
    index = ids[...]
    low = index & 127
    high = index >> 7
    for b in range(n_blk):
        low_b = jnp.broadcast_to(low[b : b + 1, :], (8, LANES))
        high_b = jnp.broadcast_to(high[b : b + 1, :], (8, LANES))
        got = jnp.zeros((8, LANES), F32)
        for h in range(n_chunk):
            piece = lane_pick(table[0:8, h * LANES : (h + 1) * LANES], low_b)
            got = jnp.where(high_b == h, piece, got)
        stage[b * ROWS : b * ROWS + 8, :] = got
    got = jnp.zeros((n_blk, LANES), F32)
    for h in range(n_chunk):
        line = jnp.broadcast_to(table[8:9, h * LANES : (h + 1) * LANES], (n_blk, LANES))
        got = jnp.where(high == h, lane_pick(line, low), got)
    stage[pl.ds(8, n_blk, stride=ROWS), :] = got
    for i, value in enumerate(scalars):
        stage[10 + i : 11 + i, :] = jnp.full((1, LANES), value, F32)
    out[...] = stage[...].T.reshape(out.shape)


def start_kernel(own, partner, proj, precond, ids, out, res_out, dir_out, weights, table, stage):
    weights[...] = own[...] + partner[...]
    n_par, width = precond.shape
    for h in range(width // LANES):
        cols = slice(h * LANES, (h + 1) * LANES)
        res = -lifted(proj, weights, h)
        dirn = precond[:, cols] * res
        res_out[:, cols] = res
        dir_out[:, cols] = dirn
        projected(proj, dirn, h, table)
    send_picks(table, ids, (), stage, out)


def step_kernel(
    own, partner, proj, precond, damping, ids, res, dirn, out, image_out, weights, table, stage
):
    weights[...] = own[...] + partner[...]
    n_par, width = precond.shape
    rz = jnp.zeros((n_par, LANES), F32)
    curve = jnp.zeros((n_par, LANES), F32)
    square = jnp.zeros((n_par, LANES), F32)
    for h in range(width // LANES):
        cols = slice(h * LANES, (h + 1) * LANES)
        image = lifted(proj, weights, h) + damping[:, cols] * dirn[:, cols]
        image_out[:, cols] = image
        scaled = precond[:, cols] * image
        projected(proj, scaled, h, table)
        rz += res[:, cols] * dirn[:, cols]
        curve += dirn[:, cols] * image
        square += scaled * image
    send_picks(table, ids, (jnp.sum(rz), jnp.sum(curve), jnp.sum(square)), stage, out)


def last_kernel(
    own, partner, proj, damping, alpha_in, first_dir, res, dirn,
    sol_hbm, res_hbm, weights, sol_out, res_out, sem,
):
    weights[...] = own[...] + partner[...]
    rows = proj.shape[0] * 8
    curve = weights[rows : rows + 1, :] + own[rows + 1 : rows + 2, :]
    alpha = own[rows + 2 : rows + 3, :] / curve
    alpha_first = alpha_in[0:1, :]
    chunks = damping.shape[1] // LANES
    copies = []

    def send(end):
        cols = pl.ds((end - 2) * LANES, 2 * LANES)
        for here, there in ((sol_out, sol_hbm), (res_out, res_hbm)):
            copy = pltpu.make_async_copy(here.at[:, cols], there.at[:, cols], sem.at[len(copies)])
            copy.start()
            copies.append(copy)

    for h in range(chunks):
        cols = slice(h * LANES, (h + 1) * LANES)
        image = lifted(proj, weights, h) + damping[:, cols] * dirn[:, cols]
        sol_out[:, cols] = alpha_first * first_dir[:, cols] + alpha * dirn[:, cols]
        res_out[:, cols] = res[:, cols] - alpha * image
        if h >= 2 and h % 2 == 0:
            send(h)
    send(chunks)
    for copy in copies:
        copy.wait()


def local(jacobian, splat_ids, pix_residual, live_blocks, proj_jac, damping, precond):
    n_blk, n_pix, n_col = jacobian.shape
    n_par, g_dev = damping.shape
    n_scene, n_x = lax.axis_size("scene"), lax.axis_size("x")
    per = LANES // n_scene
    msg = f32(n_scene, per, LANES)
    wide = f32(n_scene, n_x, per, LANES)
    sums = f32(80, LANES)
    state = f32(n_par, g_dev)
    square = pltpu.VMEM((LANES, LANES), F32)
    whole = jax.ShapeDtypeStruct
    weights = pltpu.VMEM((80, LANES), F32)
    table = pltpu.VMEM((16, g_dev), F32)

    def to_owners(message, right):
        flat = message.reshape(n_scene * n_x, per, LANES)
        got = lax.all_to_all(flat, ("scene", "x"), 0, 0, tiled=True)
        first = right is None
        wide_k = n_x * n_blk * LANES
        extra = (whole((n_blk, LANES), jnp.int32), whole((LANES, wide_k), BF16))
        own, *kept = call(
            functools.partial(sum_kernel, first),
            (sums,) + (extra if first else ()),
            [VMEM] * (1 if first else 2),
            [
                pltpu.VMEM((n_x, LANES, LANES), F32),
                pltpu.VMEM((n_x, LANES, LANES), F32),
                pltpu.VMEM((160, wide_k), BF16),
            ],
            1 << 31,
        )(got.reshape(n_scene, n_x, per, LANES), *(() if first else (right,)))
        partner = lax.ppermute(own, "core", [(0, 1), (1, 0)])
        return own, partner, *kept

    def to_blocks(message):
        return lax.all_to_all(message, "scene", 0, 0, tiled=True)

    message, jac, aux = call(
        rhs_kernel,
        (wide, whole(jacobian.shape, BF16), whole((2 * n_blk, LANES), jnp.int32)),
        [HBM] * 4,
        [
            pltpu.VMEM((n_blk, n_pix), BF16),
            pltpu.VMEM((1, live_blocks.shape[0]), jnp.int32),
            pltpu.VMEM((n_blk, LANES), jnp.int32),
            square,
            pltpu.SemaphoreType.DMA((n_blk,)),
            pltpu.SemaphoreType.DMA((3,)),
        ],
    )(*map(in_hbm, (live_blocks.reshape(1, -1), jacobian, pix_residual, splat_ids)))
    own, partner, index, right = to_owners(message, None)
    message, res, first_dir = call(
        start_kernel, (msg, state, state), [VMEM] * 5, [weights, table, square]
    )(own, partner, proj_jac, precond, index)
    arrived = to_blocks(message)
    message, picks = call(
        first_kernel,
        (wide, f32(n_blk, n_col)),
        [VMEM] * 3,
        [square, square],
    )(jac, aux, arrived)
    own, partner = to_owners(message, right)
    message, image = call(step_kernel, (msg, state), [VMEM] * 8, [weights, table, square])(
        own, partner, proj_jac, precond, damping, index, res, first_dir
    )
    arrived = to_blocks(message)
    message, res, second_dir, alpha = call(
        second_kernel,
        (wide, state, state, f32(8, LANES)),
        [VMEM] * 9,
        [square, square],
    )(jac, aux, arrived, picks, res, first_dir, image, precond, damping)
    own, partner = to_owners(message, right)
    held = pltpu.VMEM((n_par, g_dev), F32)
    return call(
        last_kernel,
        (state, state),
        [VMEM] * 8,
        [weights, held, held, pltpu.SemaphoreType.DMA((2 * (g_dev // (2 * LANES)),))],
        out_space=HBM,
    )(
        own, partner, proj_jac, damping, alpha, first_dir, res, second_dir
    )


def solution(mesh):
    scene = mesh.shape["scene"]
    finer = Mesh(mesh.devices.reshape(scene, -1, 2), ("scene", "x", "core"))
    everywhere = ("scene", "x", "core")
    in_specs = (
        P(everywhere, None, None),
        P(everywhere, None),
        P(everywhere, None),
        P(),
        P(None, None, "scene"),
        P(None, "scene"),
        P(None, "scene"),
    )
    out_specs = (P(None, "scene"), P(None, "scene"))
    return jax.shard_map(local, mesh=finer, in_specs=in_specs, out_specs=out_specs, check_vma=False)
```

```python
import functools

import jax
import jax.numpy as jnp
from jax import lax
from jax.experimental import pallas as pl
from jax.experimental.pallas import tpu as pltpu
from jax.sharding import Mesh
from jax.sharding import PartitionSpec as P

F32 = jnp.float32
BF16 = jnp.bfloat16
LANES = 128
ROWS = 16
VMEM = pl.BlockSpec(memory_space=pltpu.VMEM)
HBM = pl.BlockSpec(memory_space=pltpu.HBM)
NT = (((1,), (1,)), ((), ()))


def call(kernel, out, in_specs, scratch=(), flops=1 << 20, out_space=VMEM):
    return pl.pallas_call(
        kernel,
        out_shape=out,
        in_specs=in_specs,
        out_specs=jax.tree.map(lambda _: out_space, out),
        scratch_shapes=scratch,
        compiler_params=pltpu.CompilerParams(vmem_limit_bytes=24 << 20),
        cost_estimate=pl.CostEstimate(flops=flops, bytes_accessed=1 << 20, transcendentals=0),
    )


def in_hbm(array):
    return pltpu.with_memory_space_constraint(array, pltpu.HBM)


def f32(*shape):
    return jax.ShapeDtypeStruct(shape, F32)


def pack_return(acc, ids, scalars, stage, out):
    n_blk = acc.shape[0]
    n_proj = acc.shape[1] // LANES
    stage[...] = jnp.zeros_like(stage)
    for k in range(n_proj):
        stage[pl.ds(k, n_blk, stride=ROWS), :] = acc[:, k * LANES : (k + 1) * LANES]
    stage[pl.ds(n_proj, n_blk, stride=ROWS), :] = ids.astype(F32)
    for i, value in enumerate(scalars):
        stage[n_proj + 1 + i : n_proj + 2 + i, :] = jnp.full((1, LANES), value, F32)
    turned = stage[...].T.reshape(out.shape[0], *out.shape[2:])
    for x in range(out.shape[1]):
        out[:, x] = turned


def rhs_kernel(live, jac, pix, ids, out, jbuf, aux, pixels, lives, index, stage, sem, small):
    n_blk = jac.shape[0]
    minor = [
        pltpu.make_async_copy(pix, pixels, small.at[0]),
        pltpu.make_async_copy(live, lives, small.at[1]),
        pltpu.make_async_copy(ids, index, small.at[2]),
    ]
    copies = [pltpu.make_async_copy(jac.at[b], jbuf.at[b], sem.at[b]) for b in range(n_blk)]
    for copy in minor + copies:
        copy.start()
    for copy in minor:
        copy.wait()
    n_x, n_core = lax.axis_size("x"), lax.axis_size("core")
    position = (lax.axis_index("scene") * n_x + lax.axis_index("x")) * n_core
    position = position + lax.axis_index("core")
    lane = lax.broadcasted_iota(jnp.int32, lives.shape, 1)
    own = jnp.sum(jnp.where(lane == position, lives[...], 0), axis=1, keepdims=True)
    local_ids = index[...] & (LANES * 8 - 1)
    aux[0:n_blk, :] = local_ids
    aux[n_blk : 2 * n_blk, :] = jnp.broadcast_to(own, (n_blk, LANES))
    row = lax.broadcasted_iota(jnp.int32, pix.shape, 0)
    keep = row < jnp.broadcast_to(own, pix.shape)
    values = jnp.where(keep, pixels[...].astype(F32), 0.0)
    n_pix, n_col = jac.shape[1:]
    acc = jnp.zeros((n_blk, n_col), F32)
    cut = n_blk * 3 // 4
    for first, last in ((0, cut), (cut, n_blk)):
        signals = [jnp.where(row == b, values, 0.0).astype(BF16) for b in range(first, last)]
        for copy in copies[first:last]:
            copy.wait()
        stacked = jbuf[first:last].reshape((last - first) * n_pix, n_col)
        acc += jnp.dot(jnp.concatenate(signals, axis=1), stacked, preferred_element_type=F32)
    pack_return(acc, local_ids, (), stage, out)


def lane_image(jac, b, line, ones):
    pieces = []
    for top in range(0, jac.shape[1], 64):
        folded = jnp.zeros((64, LANES), F32)
        for at in range(0, jac.shape[2], LANES):
            tile = jac[b, top : top + 64, at : at + LANES].astype(F32)
            folded += tile * line[:, at : at + LANES]
        high = folded.astype(BF16)
        pieces.append(jnp.concatenate([high, (folded - high.astype(F32)).astype(BF16)], axis=1))
    return lax.dot_general(
        ones, jnp.concatenate(pieces, axis=0), NT, preferred_element_type=F32
    )


def block_pass(picks, aux, jac, by_lanes, beside=None):
    n_blk, n_pix = jac.shape[:2]
    row = lax.broadcasted_iota(jnp.int32, (n_blk, n_pix), 0)
    live = row < aux[n_blk : n_blk + 1, 0:1]
    chosen = picks.astype(BF16)
    rounded = chosen.astype(F32)
    ones = jnp.ones((n_blk, 2 * LANES), BF16)
    signals = []
    for b in range(n_blk):
        if (b * by_lanes) // n_blk != ((b + 1) * by_lanes) // n_blk:
            image = lane_image(jac, b, rounded[b : b + 1, :], ones)
        else:
            image = lax.dot_general(chosen, jac[b], NT, preferred_element_type=F32)
        if beside is not None:
            beside(b)
        signals.append(jnp.where((row == b) & live, image, 0.0).astype(BF16))
    stacked = jac[...].reshape(n_blk * n_pix, jac.shape[2])
    return jnp.dot(jnp.concatenate(signals, axis=1), stacked, preferred_element_type=F32)


def unpack_picks(recv, turned, n_blk, n_proj):
    turned[...] = recv[...].reshape(LANES, LANES).T
    return jnp.concatenate(
        [turned[pl.ds(k, n_blk, stride=ROWS), :] for k in range(n_proj)], axis=1
    )


def total_of(row, copies):
    return jnp.sum(row) * (1.0 / copies)


def first_kernel(jac, aux, recv, out, picks_out, turned, stage):
    n_blk = jac.shape[0]
    n_proj = jac.shape[2] // LANES
    picks = unpack_picks(recv, turned, n_blk, n_proj)
    picks_out[...] = picks
    acc = block_pass(picks, aux, jac, 5)
    pack_return(acc, aux[0:n_blk, :], (), stage, out)


def second_kernel(
    jac, aux, recv, picks_in, res, dirn, image, precond, damping,
    out, res_out, dir_out, alpha_out, turned, stage,
):
    n_blk = jac.shape[0]
    n_proj = jac.shape[2] // LANES
    fresh = unpack_picks(recv, turned, n_blk, n_proj)
    per = recv.shape[1]
    rz = total_of(turned[n_proj + 1 : n_proj + 2, :], per)
    curve = total_of(turned[n_proj + 2 : n_proj + 3, :], per)
    square = total_of(turned[n_proj + 3 : n_proj + 4, :], per)
    alpha = jnp.full((1, LANES), rz, F32) / jnp.full((1, LANES), curve, F32)
    after = rz - 2.0 * alpha * curve + alpha * alpha * square
    beta = after / jnp.full((1, LANES), rz, F32)
    alpha_out[...] = jnp.broadcast_to(alpha, alpha_out.shape)
    pieces = []
    for k in range(n_proj):
        cols = slice(k * LANES, (k + 1) * LANES)
        pieces.append((1.0 + beta) * picks_in[:, cols] - alpha * fresh[:, cols])
    picks = jnp.concatenate(pieces, axis=1)
    n_par, width = res.shape
    sums = [jnp.zeros((n_par, LANES), F32)] * 2

    def update(h):
        cols = slice(h * LANES, (h + 1) * LANES)
        new_res = res[:, cols] - alpha * image[:, cols]
        precon = precond[:, cols] * new_res
        new_dir = precon + beta * dirn[:, cols]
        res_out[:, cols] = new_res
        dir_out[:, cols] = new_dir
        sums[0] += damping[:, cols] * new_dir * new_dir
        sums[1] += new_res * precon

    acc = block_pass(picks, aux, jac, 5, update)
    scalars = (jnp.sum(picks * acc), jnp.sum(sums[0]), jnp.sum(sums[1]))
    pack_return(acc, aux[0:n_blk, :], scalars, stage, out)


def sum_kernel(first, recv, *rest):
    if first:
        out, ids_out, right, turned, fine, left = rest
    else:
        right, out, turned, fine, left = rest
    n_x = recv.shape[1]
    n_blk = LANES // ROWS
    n_proj = 9
    sub = lax.broadcasted_iota(jnp.int32, (n_blk, LANES), 0)
    deep = lax.broadcasted_iota(jnp.int32, (LANES, LANES), 0)
    half = n_proj * 8

    def spread(table, x, base, high):
        lines = [
            jnp.broadcast_to(table[x, base + k : base + k + 1, :], (8, LANES))
            for k in range(n_proj)
        ]
        return jnp.concatenate([jnp.where(high, line, 0.0) for line in lines], axis=0)

    for x in range(n_x):
        values = recv[:, x].reshape(LANES, LANES).T
        turned[x] = values
        fine[x] = values - values.astype(BF16).astype(F32)
        for b in range(n_blk):
            at = (x * n_blk + b) * LANES
            cols = slice(at, at + LANES)
            base = b * ROWS
            ids = turned[x, base + n_proj : base + n_proj + 1, :].astype(jnp.int32)
            high = jnp.broadcast_to(ids >> 7, (8, LANES)) == sub
            left[0:half, cols] = spread(turned, x, base, high).astype(BF16)
            left[80 : 80 + half, cols] = spread(fine, x, base, high).astype(BF16)
            if first:
                low = jnp.broadcast_to(ids & 127, (LANES, LANES)) == deep
                right[:, cols] = jnp.where(low, 1.0, 0.0).astype(BF16)
    summed = lax.dot_general(left[...], right[...], NT, preferred_element_type=F32)
    out[0:half, :] = summed[0:half] + summed[80 : 80 + half]
    per = recv.shape[2]
    mixed = jnp.zeros((1, LANES), F32)
    for x in range(n_x):
        mixed += turned[x, n_proj + 1 : n_proj + 2, :]
    out[half : half + 1, :] = jnp.full((1, LANES), total_of(mixed, per), F32)
    for i in (1, 2):
        line = turned[0, n_proj + 1 + i : n_proj + 2 + i, :]
        out[half + i : half + i + 1, :] = jnp.full((1, LANES), total_of(line, per), F32)
    out[half + 3 : half + 8, :] = jnp.zeros((5, LANES), F32)
    if first:
        ids_out[...] = turned[lax.axis_index("x"), pl.ds(n_proj, n_blk, stride=ROWS), :].astype(jnp.int32)


def lifted(proj, weights, h):
    cols = slice(h * LANES, (h + 1) * LANES)
    n_proj, n_par, _ = proj.shape
    acc = jnp.zeros((n_par, LANES), F32)
    for k in range(n_proj):
        line = weights[k * 8 + h : k * 8 + h + 1, :]
        acc += proj[k, :, cols].astype(F32) * jnp.broadcast_to(line, (n_par, LANES))
    return acc


def projected(proj, field, h, table):
    cols = slice(h * LANES, (h + 1) * LANES)
    for k in range(proj.shape[0]):
        table[k : k + 1, cols] = jnp.sum(
            proj[k, :, cols].astype(F32) * field, axis=0, keepdims=True
        )


def lane_pick(table, low):
    return jnp.take_along_axis(table, low, axis=1, mode="promise_in_bounds")


def send_picks(table, ids, scalars, stage, out):
    n_blk = ids.shape[0]
    n_chunk = table.shape[1] // LANES
    stage[...] = jnp.zeros_like(stage)
    index = ids[...]
    low = index & 127
    high = index >> 7
    for b in range(n_blk):
        low_b = jnp.broadcast_to(low[b : b + 1, :], (8, LANES))
        high_b = jnp.broadcast_to(high[b : b + 1, :], (8, LANES))
        got = jnp.zeros((8, LANES), F32)
        for h in range(n_chunk):
            piece = lane_pick(table[0:8, h * LANES : (h + 1) * LANES], low_b)
            got = jnp.where(high_b == h, piece, got)
        stage[b * ROWS : b * ROWS + 8, :] = got
    got = jnp.zeros((n_blk, LANES), F32)
    for h in range(n_chunk):
        line = jnp.broadcast_to(table[8:9, h * LANES : (h + 1) * LANES], (n_blk, LANES))
        got = jnp.where(high == h, lane_pick(line, low), got)
    stage[pl.ds(8, n_blk, stride=ROWS), :] = got
    for i, value in enumerate(scalars):
        stage[10 + i : 11 + i, :] = jnp.full((1, LANES), value, F32)
    out[...] = stage[...].T.reshape(out.shape)


def start_kernel(own, partner, proj, precond, ids, out, res_out, dir_out, weights, table, stage):
    weights[...] = own[...] + partner[...]
    n_par, width = precond.shape
    for h in range(width // LANES):
        cols = slice(h * LANES, (h + 1) * LANES)
        res = -lifted(proj, weights, h)
        dirn = precond[:, cols] * res
        res_out[:, cols] = res
        dir_out[:, cols] = dirn
        projected(proj, dirn, h, table)
    send_picks(table, ids, (), stage, out)


def step_kernel(
    own, partner, proj, precond, damping, ids, res, dirn, out, image_out, weights, table, stage
):
    weights[...] = own[...] + partner[...]
    n_par, width = precond.shape
    rz = jnp.zeros((n_par, LANES), F32)
    curve = jnp.zeros((n_par, LANES), F32)
    square = jnp.zeros((n_par, LANES), F32)
    for h in range(width // LANES):
        cols = slice(h * LANES, (h + 1) * LANES)
        image = lifted(proj, weights, h) + damping[:, cols] * dirn[:, cols]
        image_out[:, cols] = image
        scaled = precond[:, cols] * image
        projected(proj, scaled, h, table)
        rz += res[:, cols] * dirn[:, cols]
        curve += dirn[:, cols] * image
        square += scaled * image
    send_picks(table, ids, (jnp.sum(rz), jnp.sum(curve), jnp.sum(square)), stage, out)


def last_kernel(
    own, partner, proj, damping, alpha_in, first_dir, res, dirn,
    sol_hbm, res_hbm, weights, sol_out, res_out, sem,
):
    weights[...] = own[...] + partner[...]
    rows = proj.shape[0] * 8
    curve = weights[rows : rows + 1, :] + own[rows + 1 : rows + 2, :]
    alpha = own[rows + 2 : rows + 3, :] / curve
    alpha_first = alpha_in[0:1, :]
    chunks = damping.shape[1] // LANES
    copies = []

    def send(end):
        cols = pl.ds((end - 2) * LANES, 2 * LANES)
        for here, there in ((sol_out, sol_hbm), (res_out, res_hbm)):
            copy = pltpu.make_async_copy(here.at[:, cols], there.at[:, cols], sem.at[len(copies)])
            copy.start()
            copies.append(copy)

    for h in range(chunks):
        cols = slice(h * LANES, (h + 1) * LANES)
        image = lifted(proj, weights, h) + damping[:, cols] * dirn[:, cols]
        sol_out[:, cols] = alpha_first * first_dir[:, cols] + alpha * dirn[:, cols]
        res_out[:, cols] = res[:, cols] - alpha * image
        if h >= 2 and h % 2 == 0:
            send(h)
    send(chunks)
    for copy in copies:
        copy.wait()


def local(jacobian, splat_ids, pix_residual, live_blocks, proj_jac, damping, precond):
    n_blk, n_pix, n_col = jacobian.shape
    n_par, g_dev = damping.shape
    n_scene, n_x = lax.axis_size("scene"), lax.axis_size("x")
    per = LANES // n_scene
    msg = f32(n_scene, per, LANES)
    wide = f32(n_scene, n_x, per, LANES)
    sums = f32(80, LANES)
    state = f32(n_par, g_dev)
    square = pltpu.VMEM((LANES, LANES), F32)
    whole = jax.ShapeDtypeStruct
    weights = pltpu.VMEM((80, LANES), F32)
    table = pltpu.VMEM((16, g_dev), F32)

    def to_owners(message, right):
        flat = message.reshape(n_scene * n_x, per, LANES)
        got = lax.all_to_all(flat, ("scene", "x"), 0, 0, tiled=True)
        first = right is None
        wide_k = n_x * n_blk * LANES
        extra = (whole((n_blk, LANES), jnp.int32), whole((LANES, wide_k), BF16))
        own, *kept = call(
            functools.partial(sum_kernel, first),
            (sums,) + (extra if first else ()),
            [VMEM] * (1 if first else 2),
            [
                pltpu.VMEM((n_x, LANES, LANES), F32),
                pltpu.VMEM((n_x, LANES, LANES), F32),
                pltpu.VMEM((160, wide_k), BF16),
            ],
            1 << 31,
        )(got.reshape(n_scene, n_x, per, LANES), *(() if first else (right,)))
        partner = lax.ppermute(own, "core", [(0, 1), (1, 0)])
        return own, partner, *kept

    def to_blocks(message):
        return lax.all_to_all(message, "scene", 0, 0, tiled=True)

    message, jac, aux = call(
        rhs_kernel,
        (wide, whole(jacobian.shape, BF16), whole((2 * n_blk, LANES), jnp.int32)),
        [HBM] * 4,
        [
            pltpu.VMEM((n_blk, n_pix), BF16),
            pltpu.VMEM((1, live_blocks.shape[0]), jnp.int32),
            pltpu.VMEM((n_blk, LANES), jnp.int32),
            square,
            pltpu.SemaphoreType.DMA((n_blk,)),
            pltpu.SemaphoreType.DMA((3,)),
        ],
    )(*map(in_hbm, (live_blocks.reshape(1, -1), jacobian, pix_residual, splat_ids)))
    own, partner, index, right = to_owners(message, None)
    message, res, first_dir = call(
        start_kernel, (msg, state, state), [VMEM] * 5, [weights, table, square]
    )(own, partner, proj_jac, precond, index)
    arrived = to_blocks(message)
    message, picks = call(
        first_kernel,
        (wide, f32(n_blk, n_col)),
        [VMEM] * 3,
        [square, square],
    )(jac, aux, arrived)
    own, partner = to_owners(message, right)
    message, image = call(step_kernel, (msg, state), [VMEM] * 8, [weights, table, square])(
        own, partner, proj_jac, precond, damping, index, res, first_dir
    )
    arrived = to_blocks(message)
    message, res, second_dir, alpha = call(
        second_kernel,
        (wide, state, state, f32(8, LANES)),
        [VMEM] * 9,
        [square, square],
    )(jac, aux, arrived, picks, res, first_dir, image, precond, damping)
    own, partner = to_owners(message, right)
    held = pltpu.VMEM((n_par, g_dev), F32)
    return call(
        last_kernel,
        (state, state),
        [VMEM] * 8,
        [weights, held, held, pltpu.SemaphoreType.DMA((2 * (g_dev // (2 * LANES)),))],
        out_space=HBM,
    )(
        own, partner, proj_jac, damping, alpha, first_dir, res, second_dir
    )


def solution(mesh):
    scene = mesh.shape["scene"]
    finer = Mesh(mesh.devices.reshape(scene, -1, 2), ("scene", "x", "core"))
    everywhere = ("scene", "x", "core")
    in_specs = (
        P(everywhere, None, None),
        P(everywhere, None),
        P(everywhere, None),
        P(),
        P(None, None, "scene"),
        P(None, "scene"),
        P(None, "scene"),
    )
    out_specs = (P(None, "scene"), P(None, "scene"))
    return jax.shard_map(local, mesh=finer, in_specs=in_specs, out_specs=out_specs, check_vma=False)
```

```python
import functools

import jax
import jax.numpy as jnp
from jax import lax
from jax.experimental import pallas as pl
from jax.experimental.pallas import tpu as pltpu
from jax.sharding import Mesh
from jax.sharding import PartitionSpec as P

F32 = jnp.float32
BF16 = jnp.bfloat16
LANES = 128
ROWS = 16
VMEM = pl.BlockSpec(memory_space=pltpu.VMEM)
HBM = pl.BlockSpec(memory_space=pltpu.HBM)
NT = (((1,), (1,)), ((), ()))


def call(kernel, out, in_specs, scratch=(), flops=1 << 20, out_space=VMEM):
    return pl.pallas_call(
        kernel,
        out_shape=out,
        in_specs=in_specs,
        out_specs=jax.tree.map(lambda _: out_space, out),
        scratch_shapes=scratch,
        compiler_params=pltpu.CompilerParams(vmem_limit_bytes=24 << 20),
        cost_estimate=pl.CostEstimate(flops=flops, bytes_accessed=1 << 20, transcendentals=0),
    )


def in_hbm(array):
    return pltpu.with_memory_space_constraint(array, pltpu.HBM)


def f32(*shape):
    return jax.ShapeDtypeStruct(shape, F32)


def pack_return(acc, ids, scalars, stage, out):
    n_blk = acc.shape[0]
    n_proj = acc.shape[1] // LANES
    stage[...] = jnp.zeros_like(stage)
    for k in range(n_proj):
        stage[pl.ds(k, n_blk, stride=ROWS), :] = acc[:, k * LANES : (k + 1) * LANES]
    stage[pl.ds(n_proj, n_blk, stride=ROWS), :] = ids.astype(F32)
    for i, value in enumerate(scalars):
        stage[n_proj + 1 + i : n_proj + 2 + i, :] = jnp.full((1, LANES), value, F32)
    turned = stage[...].T.reshape(out.shape[0], *out.shape[2:])
    for x in range(out.shape[1]):
        out[:, x] = turned


def rhs_kernel(live, jac, pix, ids, out, jbuf, aux, pixels, lives, index, stage, sem, small):
    n_blk = jac.shape[0]
    minor = [
        pltpu.make_async_copy(pix, pixels, small.at[0]),
        pltpu.make_async_copy(live, lives, small.at[1]),
        pltpu.make_async_copy(ids, index, small.at[2]),
    ]
    copies = [pltpu.make_async_copy(jac.at[b], jbuf.at[b], sem.at[b]) for b in range(n_blk)]
    for copy in minor + copies:
        copy.start()
    for copy in minor:
        copy.wait()
    n_x, n_core = lax.axis_size("x"), lax.axis_size("core")
    position = (lax.axis_index("scene") * n_x + lax.axis_index("x")) * n_core
    position = position + lax.axis_index("core")
    lane = lax.broadcasted_iota(jnp.int32, lives.shape, 1)
    own = jnp.sum(jnp.where(lane == position, lives[...], 0), axis=1, keepdims=True)
    local_ids = index[...] & (LANES * 8 - 1)
    aux[0:n_blk, :] = local_ids
    aux[n_blk : 2 * n_blk, :] = jnp.broadcast_to(own, (n_blk, LANES))
    row = lax.broadcasted_iota(jnp.int32, pix.shape, 0)
    keep = row < jnp.broadcast_to(own, pix.shape)
    values = jnp.where(keep, pixels[...].astype(F32), 0.0)
    n_pix, n_col = jac.shape[1:]
    acc = jnp.zeros((n_blk, n_col), F32)
    cut = n_blk - 1
    for first, last in ((0, cut), (cut, n_blk)):
        signals = [jnp.where(row == b, values, 0.0).astype(BF16) for b in range(first, last)]
        for copy in copies[first:last]:
            copy.wait()
        stacked = jbuf[first:last].reshape((last - first) * n_pix, n_col)
        acc += jnp.dot(jnp.concatenate(signals, axis=1), stacked, preferred_element_type=F32)
    pack_return(acc, local_ids, (), stage, out)


def lane_image(jac, b, line, ones):
    pieces = []
    for top in range(0, jac.shape[1], 64):
        folded = jnp.zeros((64, LANES), F32)
        for at in range(0, jac.shape[2], LANES):
            tile = jac[b, top : top + 64, at : at + LANES].astype(F32)
            folded += tile * line[:, at : at + LANES]
        high = folded.astype(BF16)
        pieces.append(jnp.concatenate([high, (folded - high.astype(F32)).astype(BF16)], axis=1))
    return lax.dot_general(
        ones, jnp.concatenate(pieces, axis=0), NT, preferred_element_type=F32
    )


def block_pass(picks, aux, jac, by_lanes, beside=None):
    n_blk, n_pix = jac.shape[:2]
    row = lax.broadcasted_iota(jnp.int32, (n_blk, n_pix), 0)
    live = row < aux[n_blk : n_blk + 1, 0:1]
    chosen = picks.astype(BF16)
    rounded = chosen.astype(F32)
    ones = jnp.ones((n_blk, 2 * LANES), BF16)
    signals = []
    for b in range(n_blk):
        if (b * by_lanes) // n_blk != ((b + 1) * by_lanes) // n_blk:
            image = lane_image(jac, b, rounded[b : b + 1, :], ones)
        else:
            image = lax.dot_general(chosen, jac[b], NT, preferred_element_type=F32)
        if beside is not None:
            beside(b)
        signals.append(jnp.where((row == b) & live, image, 0.0).astype(BF16))
    stacked = jac[...].reshape(n_blk * n_pix, jac.shape[2])
    return jnp.dot(jnp.concatenate(signals, axis=1), stacked, preferred_element_type=F32)


def unpack_picks(recv, turned, n_blk, n_proj):
    turned[...] = recv[...].reshape(LANES, LANES).T
    return jnp.concatenate(
        [turned[pl.ds(k, n_blk, stride=ROWS), :] for k in range(n_proj)], axis=1
    )


def total_of(row, copies):
    return jnp.sum(row) * (1.0 / copies)


def first_kernel(jac, aux, recv, out, picks_out, turned, stage):
    n_blk = jac.shape[0]
    n_proj = jac.shape[2] // LANES
    picks = unpack_picks(recv, turned, n_blk, n_proj)
    picks_out[...] = picks
    acc = block_pass(picks, aux, jac, 5)
    pack_return(acc, aux[0:n_blk, :], (), stage, out)


def second_kernel(
    jac, aux, recv, picks_in, res, dirn, image, precond, damping,
    out, res_out, dir_out, alpha_out, turned, stage,
):
    n_blk = jac.shape[0]
    n_proj = jac.shape[2] // LANES
    fresh = unpack_picks(recv, turned, n_blk, n_proj)
    per = recv.shape[1]
    rz = total_of(turned[n_proj + 1 : n_proj + 2, :], per)
    curve = total_of(turned[n_proj + 2 : n_proj + 3, :], per)
    square = total_of(turned[n_proj + 3 : n_proj + 4, :], per)
    alpha = jnp.full((1, LANES), rz, F32) / jnp.full((1, LANES), curve, F32)
    after = rz - 2.0 * alpha * curve + alpha * alpha * square
    beta = after / jnp.full((1, LANES), rz, F32)
    alpha_out[...] = jnp.broadcast_to(alpha, alpha_out.shape)
    pieces = []
    for k in range(n_proj):
        cols = slice(k * LANES, (k + 1) * LANES)
        pieces.append((1.0 + beta) * picks_in[:, cols] - alpha * fresh[:, cols])
    picks = jnp.concatenate(pieces, axis=1)
    n_par, width = res.shape
    sums = [jnp.zeros((n_par, LANES), F32)] * 2

    def update(h):
        cols = slice(h * LANES, (h + 1) * LANES)
        new_res = res[:, cols] - alpha * image[:, cols]
        precon = precond[:, cols] * new_res
        new_dir = precon + beta * dirn[:, cols]
        res_out[:, cols] = new_res
        dir_out[:, cols] = new_dir
        sums[0] += damping[:, cols] * new_dir * new_dir
        sums[1] += new_res * precon

    acc = block_pass(picks, aux, jac, 4, update)
    scalars = (jnp.sum(picks * acc), jnp.sum(sums[0]), jnp.sum(sums[1]))
    pack_return(acc, aux[0:n_blk, :], scalars, stage, out)


def sum_kernel(first, recv, *rest):
    if first:
        out, ids_out, right, turned, fine, left = rest
    else:
        right, out, turned, fine, left = rest
    n_x = recv.shape[1]
    n_blk = LANES // ROWS
    n_proj = 9
    sub = lax.broadcasted_iota(jnp.int32, (n_blk, LANES), 0)
    deep = lax.broadcasted_iota(jnp.int32, (LANES, LANES), 0)
    half = n_proj * 8

    def spread(table, x, base, high):
        lines = [
            jnp.broadcast_to(table[x, base + k : base + k + 1, :], (8, LANES))
            for k in range(n_proj)
        ]
        return jnp.concatenate([jnp.where(high, line, 0.0) for line in lines], axis=0)

    for x in range(n_x):
        values = recv[:, x].reshape(LANES, LANES).T
        turned[x] = values
        fine[x] = values - values.astype(BF16).astype(F32)
        for b in range(n_blk):
            at = (x * n_blk + b) * LANES
            cols = slice(at, at + LANES)
            base = b * ROWS
            ids = turned[x, base + n_proj : base + n_proj + 1, :].astype(jnp.int32)
            high = jnp.broadcast_to(ids >> 7, (8, LANES)) == sub
            left[0:half, cols] = spread(turned, x, base, high).astype(BF16)
            left[80 : 80 + half, cols] = spread(fine, x, base, high).astype(BF16)
            if first:
                low = jnp.broadcast_to(ids & 127, (LANES, LANES)) == deep
                right[:, cols] = jnp.where(low, 1.0, 0.0).astype(BF16)
    summed = lax.dot_general(left[...], right[...], NT, preferred_element_type=F32)
    out[0:half, :] = summed[0:half] + summed[80 : 80 + half]
    per = recv.shape[2]
    mixed = jnp.zeros((1, LANES), F32)
    for x in range(n_x):
        mixed += turned[x, n_proj + 1 : n_proj + 2, :]
    out[half : half + 1, :] = jnp.full((1, LANES), total_of(mixed, per), F32)
    for i in (1, 2):
        line = turned[0, n_proj + 1 + i : n_proj + 2 + i, :]
        out[half + i : half + i + 1, :] = jnp.full((1, LANES), total_of(line, per), F32)
    out[half + 3 : half + 8, :] = jnp.zeros((5, LANES), F32)
    if first:
        ids_out[...] = turned[lax.axis_index("x"), pl.ds(n_proj, n_blk, stride=ROWS), :].astype(jnp.int32)


def lifted(proj, weights, h):
    cols = slice(h * LANES, (h + 1) * LANES)
    n_proj, n_par, _ = proj.shape
    acc = jnp.zeros((n_par, LANES), F32)
    for k in range(n_proj):
        line = weights[k * 8 + h : k * 8 + h + 1, :]
        acc += proj[k, :, cols].astype(F32) * jnp.broadcast_to(line, (n_par, LANES))
    return acc


def projected(proj, field, h, table):
    cols = slice(h * LANES, (h + 1) * LANES)
    for k in range(proj.shape[0]):
        table[k * 8 + h : k * 8 + h + 1, :] = jnp.sum(
            proj[k, :, cols].astype(F32) * field, axis=0, keepdims=True
        )


def pairs(n_proj):
    return [(k, m) for k in range(n_proj) for m in range(k, n_proj)]


def form_kernel(after, proj, precond, out):
    del after
    n_proj = proj.shape[0]
    for h in range(precond.shape[1] // LANES):
        cols = slice(h * LANES, (h + 1) * LANES)
        tiles = [proj[k, :, cols].astype(F32) for k in range(n_proj)]
        scaled = [tile * precond[:, cols] for tile in tiles]
        for i, (k, m) in enumerate(pairs(n_proj)):
            out[i * 8 + h : i * 8 + h + 1, :] = jnp.sum(
                scaled[k] * tiles[m], axis=0, keepdims=True
            )


def blended(matrix, weights):
    n_proj = 9
    sums = [None] * n_proj

    def add(k, tile, m):
        term = tile * weights[m * 8 : m * 8 + 8, :]
        sums[k] = term if sums[k] is None else sums[k] + term

    for i, (k, m) in enumerate(pairs(n_proj)):
        tile = matrix[i * 8 : i * 8 + 8, :]
        add(k, tile, m)
        if k != m:
            add(m, tile, k)
    return sums


def lane_pick(table, low):
    return jnp.take_along_axis(table, low, axis=1, mode="promise_in_bounds")


def send_picks(table, ids, scalars, stage, out):
    n_blk = ids.shape[0]
    n_chunk = 8
    stage[...] = jnp.zeros_like(stage)
    index = ids[...]
    low = index & 127
    high = index >> 7
    for b in range(n_blk):
        low_b = jnp.broadcast_to(low[b : b + 1, :], (8, LANES))
        high_b = jnp.broadcast_to(high[b : b + 1, :], (8, LANES))
        got = jnp.zeros((8, LANES), F32)
        for h in range(n_chunk):
            piece = lane_pick(table[pl.ds(h, 8, stride=8), :], low_b)
            got = jnp.where(high_b == h, piece, got)
        stage[b * ROWS : b * ROWS + 8, :] = got
    got = jnp.zeros((n_blk, LANES), F32)
    for h in range(n_chunk):
        line = jnp.broadcast_to(table[64 + h : 65 + h, :], (n_blk, LANES))
        got = jnp.where(high == h, lane_pick(line, low), got)
    stage[pl.ds(8, n_blk, stride=ROWS), :] = got
    for i, value in enumerate(scalars):
        stage[10 + i : 11 + i, :] = jnp.broadcast_to(value, (1, LANES))
    out[...] = stage[...].T.reshape(out.shape)


def start_kernel(own, partner, matrix, ids, out, weights, table, stage):
    weights[...] = own[...] + partner[...]
    for k, tile in enumerate(blended(matrix, weights)):
        table[k * 8 : k * 8 + 8, :] = -tile
    send_picks(table, ids, (), stage, out)


def state_kernel(
    after, own, partner, proj, precond, damping, res_out, dir_out, cross, rz_out, weights
):
    del after
    weights[...] = own[...] + partner[...]
    n_par, width = precond.shape
    rz = jnp.zeros((n_par, LANES), F32)
    for h in range(width // LANES):
        cols = slice(h * LANES, (h + 1) * LANES)
        res = -lifted(proj, weights, h)
        dirn = precond[:, cols] * res
        res_out[:, cols] = res
        dir_out[:, cols] = dirn
        rz += res * dirn
        projected(proj, precond[:, cols] * damping[:, cols] * dirn, h, cross)
    rz_out[...] = jnp.full(rz_out.shape, jnp.sum(rz), F32)


def step_kernel(
    own, partner, proj, precond, damping, matrix, cross, rz_in, ids, dirn,
    out, image_out, weights, table, stage,
):
    weights[...] = own[...] + partner[...]
    n_par, width = precond.shape
    for k, tile in enumerate(blended(matrix, weights)):
        table[k * 8 : k * 8 + 8, :] = tile + cross[k * 8 : k * 8 + 8, :]
    curve = jnp.zeros((n_par, LANES), F32)
    square = jnp.zeros((n_par, LANES), F32)
    for h in range(width // LANES):
        cols = slice(h * LANES, (h + 1) * LANES)
        image = lifted(proj, weights, h) + damping[:, cols] * dirn[:, cols]
        image_out[:, cols] = image
        curve += dirn[:, cols] * image
        square += precond[:, cols] * image * image
    scalars = (rz_in[0:1, :], jnp.sum(curve), jnp.sum(square))
    send_picks(table, ids, scalars, stage, out)


def last_kernel(
    own, partner, proj, damping, alpha_in, first_dir, res, dirn,
    sol_hbm, res_hbm, weights, sol_out, res_out, sem,
):
    weights[...] = own[...] + partner[...]
    rows = proj.shape[0] * 8
    curve = weights[rows : rows + 1, :] + own[rows + 1 : rows + 2, :]
    alpha = own[rows + 2 : rows + 3, :] / curve
    alpha_first = alpha_in[0:1, :]
    chunks = damping.shape[1] // LANES
    copies = []

    def send(end):
        cols = pl.ds((end - 2) * LANES, 2 * LANES)
        for here, there in ((sol_out, sol_hbm), (res_out, res_hbm)):
            copy = pltpu.make_async_copy(here.at[:, cols], there.at[:, cols], sem.at[len(copies)])
            copy.start()
            copies.append(copy)

    for h in range(chunks):
        cols = slice(h * LANES, (h + 1) * LANES)
        image = lifted(proj, weights, h) + damping[:, cols] * dirn[:, cols]
        sol_out[:, cols] = alpha_first * first_dir[:, cols] + alpha * dirn[:, cols]
        res_out[:, cols] = res[:, cols] - alpha * image
        if h >= 2 and h % 2 == 0:
            send(h)
    send(chunks)
    for copy in copies:
        copy.wait()


def local(jacobian, splat_ids, pix_residual, live_blocks, proj_jac, damping, precond):
    n_blk, n_pix, n_col = jacobian.shape
    n_par, g_dev = damping.shape
    n_scene, n_x = lax.axis_size("scene"), lax.axis_size("x")
    per = LANES // n_scene
    msg = f32(n_scene, per, LANES)
    wide = f32(n_scene, n_x, per, LANES)
    sums = f32(80, LANES)
    state = f32(n_par, g_dev)
    square = pltpu.VMEM((LANES, LANES), F32)
    whole = jax.ShapeDtypeStruct
    weights = pltpu.VMEM((80, LANES), F32)
    table = pltpu.VMEM((72, LANES), F32)

    def to_owners(message, right):
        flat = message.reshape(n_scene * n_x, per, LANES)
        got = lax.all_to_all(flat, ("scene", "x"), 0, 0, tiled=True)
        first = right is None
        wide_k = n_x * n_blk * LANES
        extra = (whole((n_blk, LANES), jnp.int32), whole((LANES, wide_k), BF16))
        own, *kept = call(
            functools.partial(sum_kernel, first),
            (sums,) + (extra if first else ()),
            [VMEM] * (1 if first else 2),
            [
                pltpu.VMEM((n_x, LANES, LANES), F32),
                pltpu.VMEM((n_x, LANES, LANES), F32),
                pltpu.VMEM((160, wide_k), BF16),
            ],
            1 << 31,
        )(got.reshape(n_scene, n_x, per, LANES), *(() if first else (right,)))
        partner = lax.ppermute(own, "core", [(0, 1), (1, 0)])
        return own, partner, *kept

    def to_blocks(message):
        return lax.all_to_all(message, "scene", 0, 0, tiled=True)

    message, jac, aux = call(
        rhs_kernel,
        (wide, whole(jacobian.shape, BF16), whole((2 * n_blk, LANES), jnp.int32)),
        [HBM] * 4,
        [
            pltpu.VMEM((n_blk, n_pix), BF16),
            pltpu.VMEM((1, live_blocks.shape[0]), jnp.int32),
            pltpu.VMEM((n_blk, LANES), jnp.int32),
            square,
            pltpu.SemaphoreType.DMA((n_blk,)),
            pltpu.SemaphoreType.DMA((3,)),
        ],
    )(*map(in_hbm, (live_blocks.reshape(1, -1), jacobian, pix_residual, splat_ids)))
    own, partner, index, right = to_owners(message, None)
    matrix = call(form_kernel, (f32(45 * 8, LANES),), [VMEM] * 3, (), 1 << 31)(
        own, proj_jac, precond
    )[0]
    message = call(start_kernel, (msg,), [VMEM] * 4, [weights, table, square])(
        own, partner, matrix, index
    )[0]
    first_own, first_partner = own, partner
    arrived = to_blocks(message)
    message, picks = call(
        first_kernel,
        (wide, f32(n_blk, n_col)),
        [VMEM] * 3,
        [square, square],
    )(jac, aux, arrived)
    own, partner = to_owners(message, right)
    res, first_dir, cross, rz = call(
        state_kernel, (state, state, f32(72, LANES), f32(8, LANES)), [VMEM] * 6, [weights], 1 << 31
    )(own, first_own, first_partner, proj_jac, precond, damping)
    message, image = call(step_kernel, (msg, state), [VMEM] * 10, [weights, table, square])(
        own, partner, proj_jac, precond, damping, matrix, cross, rz, index, first_dir
    )
    arrived = to_blocks(message)
    message, res, second_dir, alpha = call(
        second_kernel,
        (wide, state, state, f32(8, LANES)),
        [VMEM] * 9,
        [square, square],
    )(jac, aux, arrived, picks, res, first_dir, image, precond, damping)
    own, partner = to_owners(message, right)
    held = pltpu.VMEM((n_par, g_dev), F32)
    return call(
        last_kernel,
        (state, state),
        [VMEM] * 8,
        [weights, held, held, pltpu.SemaphoreType.DMA((2 * (g_dev // (2 * LANES)),))],
        out_space=HBM,
    )(
        own, partner, proj_jac, damping, alpha, first_dir, res, second_dir
    )


def solution(mesh):
    scene = mesh.shape["scene"]
    finer = Mesh(mesh.devices.reshape(scene, -1, 2), ("scene", "x", "core"))
    everywhere = ("scene", "x", "core")
    in_specs = (
        P(everywhere, None, None),
        P(everywhere, None),
        P(everywhere, None),
        P(),
        P(None, None, "scene"),
        P(None, "scene"),
        P(None, "scene"),
    )
    out_specs = (P(None, "scene"), P(None, "scene"))
    return jax.shard_map(local, mesh=finer, in_specs=in_specs, out_specs=out_specs, check_vma=False)
```

```python
import functools

import jax
import jax.numpy as jnp
from jax import lax
from jax.experimental import pallas as pl
from jax.experimental.pallas import tpu as pltpu
from jax.sharding import Mesh
from jax.sharding import PartitionSpec as P

F32 = jnp.float32
BF16 = jnp.bfloat16
LANES = 128
ROWS = 16
VMEM = pl.BlockSpec(memory_space=pltpu.VMEM)
HBM = pl.BlockSpec(memory_space=pltpu.HBM)
NT = (((1,), (1,)), ((), ()))


def call(kernel, out, in_specs, scratch=(), flops=1 << 20, out_space=VMEM):
    return pl.pallas_call(
        kernel,
        out_shape=out,
        in_specs=in_specs,
        out_specs=jax.tree.map(lambda _: out_space, out),
        scratch_shapes=scratch,
        compiler_params=pltpu.CompilerParams(vmem_limit_bytes=24 << 20),
        cost_estimate=pl.CostEstimate(flops=flops, bytes_accessed=1 << 20, transcendentals=0),
    )


def in_hbm(array):
    return pltpu.with_memory_space_constraint(array, pltpu.HBM)


def f32(*shape):
    return jax.ShapeDtypeStruct(shape, F32)


def pack_return(acc, ids, scalars, stage, out):
    n_blk = acc.shape[0]
    n_proj = acc.shape[1] // LANES
    stage[...] = jnp.zeros_like(stage)
    for k in range(n_proj):
        stage[pl.ds(k, n_blk, stride=ROWS), :] = acc[:, k * LANES : (k + 1) * LANES]
    stage[pl.ds(n_proj, n_blk, stride=ROWS), :] = ids.astype(F32)
    for i, value in enumerate(scalars):
        stage[n_proj + 1 + i : n_proj + 2 + i, :] = jnp.full((1, LANES), value, F32)
    turned = stage[...].T.reshape(out.shape[0], *out.shape[2:])
    for x in range(out.shape[1]):
        out[:, x] = turned


def rhs_kernel(live, jac, pix, ids, out, jbuf, aux, pixels, lives, index, stage, sem, small):
    n_blk = jac.shape[0]
    minor = [
        pltpu.make_async_copy(pix, pixels, small.at[0]),
        pltpu.make_async_copy(live, lives, small.at[1]),
        pltpu.make_async_copy(ids, index, small.at[2]),
    ]
    copies = [pltpu.make_async_copy(jac.at[b], jbuf.at[b], sem.at[b]) for b in range(n_blk)]
    for copy in minor + copies:
        copy.start()
    for copy in minor:
        copy.wait()
    n_x, n_core = lax.axis_size("x"), lax.axis_size("core")
    position = (lax.axis_index("scene") * n_x + lax.axis_index("x")) * n_core
    position = position + lax.axis_index("core")
    lane = lax.broadcasted_iota(jnp.int32, lives.shape, 1)
    own = jnp.sum(jnp.where(lane == position, lives[...], 0), axis=1, keepdims=True)
    local_ids = index[...] & (LANES * 8 - 1)
    aux[0:n_blk, :] = local_ids
    aux[n_blk : 2 * n_blk, :] = jnp.broadcast_to(own, (n_blk, LANES))
    row = lax.broadcasted_iota(jnp.int32, pix.shape, 0)
    keep = row < jnp.broadcast_to(own, pix.shape)
    values = jnp.where(keep, pixels[...].astype(F32), 0.0)
    n_pix, n_col = jac.shape[1:]
    acc = jnp.zeros((n_blk, n_col), F32)
    cut = n_blk * 3 // 4
    for first, last in ((0, cut), (cut, n_blk)):
        signals = [jnp.where(row == b, values, 0.0).astype(BF16) for b in range(first, last)]
        for copy in copies[first:last]:
            copy.wait()
        stacked = jbuf[first:last].reshape((last - first) * n_pix, n_col)
        acc += jnp.dot(jnp.concatenate(signals, axis=1), stacked, preferred_element_type=F32)
    pack_return(acc, local_ids, (), stage, out)


def lane_image(jac, b, line, ones):
    pieces = []
    for top in range(0, jac.shape[1], 64):
        folded = jnp.zeros((64, LANES), F32)
        for at in range(0, jac.shape[2], LANES):
            tile = jac[b, top : top + 64, at : at + LANES].astype(F32)
            folded += tile * line[:, at : at + LANES]
        high = folded.astype(BF16)
        pieces.append(jnp.concatenate([high, (folded - high.astype(F32)).astype(BF16)], axis=1))
    return lax.dot_general(
        ones, jnp.concatenate(pieces, axis=0), NT, preferred_element_type=F32
    )


def block_pass(picks, aux, jac, by_lanes):
    n_blk, n_pix = jac.shape[:2]
    row = lax.broadcasted_iota(jnp.int32, (n_blk, n_pix), 0)
    live = row < aux[n_blk : n_blk + 1, 0:1]
    chosen = picks.astype(BF16)
    rounded = chosen.astype(F32)
    ones = jnp.ones((n_blk, 2 * LANES), BF16)
    signals = []
    for b in range(n_blk):
        if (b * by_lanes) // n_blk != ((b + 1) * by_lanes) // n_blk:
            image = lane_image(jac, b, rounded[b : b + 1, :], ones)
        else:
            image = lax.dot_general(chosen, jac[b], NT, preferred_element_type=F32)
        signals.append(jnp.where((row == b) & live, image, 0.0).astype(BF16))
    stacked = jac[...].reshape(n_blk * n_pix, jac.shape[2])
    return jnp.dot(jnp.concatenate(signals, axis=1), stacked, preferred_element_type=F32)


def unpack_picks(recv, turned, n_blk, n_proj):
    turned[...] = recv[...].reshape(LANES, LANES).T
    return jnp.concatenate(
        [turned[pl.ds(k, n_blk, stride=ROWS), :] for k in range(n_proj)], axis=1
    )


def total_of(row, copies):
    return jnp.sum(row) * (1.0 / copies)


def first_kernel(jac, aux, recv, out, picks_out, turned, stage):
    n_blk = jac.shape[0]
    n_proj = jac.shape[2] // LANES
    picks = unpack_picks(recv, turned, n_blk, n_proj)
    picks_out[...] = picks
    acc = block_pass(picks, aux, jac, 5)
    pack_return(acc, aux[0:n_blk, :], (), stage, out)


def second_kernel(jac, aux, recv, picks_in, out, steps_out, turned, stage):
    n_blk = jac.shape[0]
    n_proj = jac.shape[2] // LANES
    fresh = unpack_picks(recv, turned, n_blk, n_proj)
    per = recv.shape[1]
    rz, curve, square, damped, mixed, scaled = (
        jnp.full((1, LANES), total_of(turned[n_proj + 1 + i : n_proj + 2 + i, :], per), F32)
        for i in range(6)
    )
    alpha = rz / curve
    after = rz - 2.0 * alpha * curve + alpha * alpha * square
    beta = after / rz
    grown = 1.0 + beta
    steps_out[0:1, :] = alpha
    steps_out[1:2, :] = beta
    steps_out[2:3, :] = after
    steps_out[3:4, :] = (
        grown * grown * damped - 2.0 * grown * alpha * mixed + alpha * alpha * scaled
    )
    steps_out[4:8, :] = jnp.zeros((4, LANES), F32)
    pieces = []
    for k in range(n_proj):
        cols = slice(k * LANES, (k + 1) * LANES)
        pieces.append(grown * picks_in[:, cols] - alpha * fresh[:, cols])
    picks = jnp.concatenate(pieces, axis=1)
    acc = block_pass(picks, aux, jac, 5)
    pack_return(acc, aux[0:n_blk, :], (jnp.sum(picks * acc),), stage, out)


def update_kernel(after, steps, res, dirn, image, precond, res_out, dir_out):
    del after
    alpha, beta = steps[0:1, :], steps[1:2, :]
    for h in range(res.shape[1] // LANES):
        cols = slice(h * LANES, (h + 1) * LANES)
        new_res = res[:, cols] - alpha * image[:, cols]
        res_out[:, cols] = new_res
        dir_out[:, cols] = precond[:, cols] * new_res + beta * dirn[:, cols]


def sum_kernel(first, recv, *rest):
    if first:
        out, ids_out, right, turned, fine, left = rest
    else:
        right, out, turned, fine, left = rest
    n_x = recv.shape[1]
    n_blk = LANES // ROWS
    n_proj = 9
    sub = lax.broadcasted_iota(jnp.int32, (n_blk, LANES), 0)
    deep = lax.broadcasted_iota(jnp.int32, (LANES, LANES), 0)
    half = n_proj * 8

    def spread(table, x, base, high):
        lines = [
            jnp.broadcast_to(table[x, base + k : base + k + 1, :], (8, LANES))
            for k in range(n_proj)
        ]
        return jnp.concatenate([jnp.where(high, line, 0.0) for line in lines], axis=0)

    for x in range(n_x):
        values = recv[:, x].reshape(LANES, LANES).T
        turned[x] = values
        fine[x] = values - values.astype(BF16).astype(F32)
        for b in range(n_blk):
            at = (x * n_blk + b) * LANES
            cols = slice(at, at + LANES)
            base = b * ROWS
            ids = turned[x, base + n_proj : base + n_proj + 1, :].astype(jnp.int32)
            high = jnp.broadcast_to(ids >> 7, (8, LANES)) == sub
            left[0:half, cols] = spread(turned, x, base, high).astype(BF16)
            left[80 : 80 + half, cols] = spread(fine, x, base, high).astype(BF16)
            if first:
                low = jnp.broadcast_to(ids & 127, (LANES, LANES)) == deep
                right[:, cols] = jnp.where(low, 1.0, 0.0).astype(BF16)
    summed = lax.dot_general(left[...], right[...], NT, preferred_element_type=F32)
    out[0:half, :] = summed[0:half] + summed[80 : 80 + half]
    per = recv.shape[2]
    mixed = jnp.zeros((1, LANES), F32)
    for x in range(n_x):
        mixed += turned[x, n_proj + 1 : n_proj + 2, :]
    out[half : half + 1, :] = jnp.full((1, LANES), total_of(mixed, per), F32)
    out[half + 1 : half + 8, :] = jnp.zeros((7, LANES), F32)
    if first:
        ids_out[...] = turned[lax.axis_index("x"), pl.ds(n_proj, n_blk, stride=ROWS), :].astype(jnp.int32)


def lifted(proj, weights, h):
    cols = slice(h * LANES, (h + 1) * LANES)
    n_proj, n_par, _ = proj.shape
    acc = jnp.zeros((n_par, LANES), F32)
    for k in range(n_proj):
        line = weights[k * 8 + h : k * 8 + h + 1, :]
        acc += proj[k, :, cols].astype(F32) * jnp.broadcast_to(line, (n_par, LANES))
    return acc


def projected(proj, field, h, table):
    cols = slice(h * LANES, (h + 1) * LANES)
    for k in range(proj.shape[0]):
        table[k * 8 + h : k * 8 + h + 1, :] = jnp.sum(
            proj[k, :, cols].astype(F32) * field, axis=0, keepdims=True
        )


def pairs(n_proj):
    return [(k, m) for k in range(n_proj) for m in range(k, n_proj)]


def form_kernel(after, proj, precond, out):
    del after
    n_proj = proj.shape[0]
    for h in range(precond.shape[1] // LANES):
        cols = slice(h * LANES, (h + 1) * LANES)
        tiles = [proj[k, :, cols].astype(F32) for k in range(n_proj)]
        scaled = [tile * precond[:, cols] for tile in tiles]
        for i, (k, m) in enumerate(pairs(n_proj)):
            out[i * 8 + h : i * 8 + h + 1, :] = jnp.sum(
                scaled[k] * tiles[m], axis=0, keepdims=True
            )


def blended(matrix, weights):
    n_proj = 9
    sums = [None] * n_proj

    def add(k, tile, m):
        term = tile * weights[m * 8 : m * 8 + 8, :]
        sums[k] = term if sums[k] is None else sums[k] + term

    for i, (k, m) in enumerate(pairs(n_proj)):
        tile = matrix[i * 8 : i * 8 + 8, :]
        add(k, tile, m)
        if k != m:
            add(m, tile, k)
    return sums


def lane_pick(table, low):
    return jnp.take_along_axis(table, low, axis=1, mode="promise_in_bounds")


def send_picks(table, ids, scalars, stage, out):
    n_blk = ids.shape[0]
    n_chunk = 8
    stage[...] = jnp.zeros_like(stage)
    index = ids[...]
    low = index & 127
    high = index >> 7
    for b in range(n_blk):
        low_b = jnp.broadcast_to(low[b : b + 1, :], (8, LANES))
        high_b = jnp.broadcast_to(high[b : b + 1, :], (8, LANES))
        got = jnp.zeros((8, LANES), F32)
        for h in range(n_chunk):
            piece = lane_pick(table[pl.ds(h, 8, stride=8), :], low_b)
            got = jnp.where(high_b == h, piece, got)
        stage[b * ROWS : b * ROWS + 8, :] = got
    got = jnp.zeros((n_blk, LANES), F32)
    for h in range(n_chunk):
        line = jnp.broadcast_to(table[64 + h : 65 + h, :], (n_blk, LANES))
        got = jnp.where(high == h, lane_pick(line, low), got)
    stage[pl.ds(8, n_blk, stride=ROWS), :] = got
    for i, value in enumerate(scalars):
        stage[10 + i : 11 + i, :] = jnp.broadcast_to(value, (1, LANES))
    out[...] = stage[...].T.reshape(out.shape)


def start_kernel(own, partner, matrix, ids, out, weights, table, stage):
    weights[...] = own[...] + partner[...]
    for k, tile in enumerate(blended(matrix, weights)):
        table[k * 8 : k * 8 + 8, :] = -tile
    send_picks(table, ids, (), stage, out)


def state_kernel(
    after, own, partner, proj, precond, damping, res_out, dir_out, cross, rz_out, weights
):
    del after
    weights[...] = own[...] + partner[...]
    n_par, width = precond.shape
    rz = jnp.zeros((n_par, LANES), F32)
    for h in range(width // LANES):
        cols = slice(h * LANES, (h + 1) * LANES)
        res = -lifted(proj, weights, h)
        dirn = precond[:, cols] * res
        res_out[:, cols] = res
        dir_out[:, cols] = dirn
        rz += res * dirn
        projected(proj, precond[:, cols] * damping[:, cols] * dirn, h, cross)
    rz_out[...] = jnp.full(rz_out.shape, jnp.sum(rz), F32)


def step_kernel(
    own, partner, proj, precond, damping, matrix, cross, rz_in, ids, dirn,
    out, image_out, weights, table, stage,
):
    weights[...] = own[...] + partner[...]
    n_par, width = precond.shape
    for k, tile in enumerate(blended(matrix, weights)):
        table[k * 8 : k * 8 + 8, :] = tile + cross[k * 8 : k * 8 + 8, :]
    curve, square, damped, mixed, scaled = [jnp.zeros((n_par, LANES), F32)] * 5
    for h in range(width // LANES):
        cols = slice(h * LANES, (h + 1) * LANES)
        pull = damping[:, cols] * dirn[:, cols]
        image = lifted(proj, weights, h) + pull
        image_out[:, cols] = image
        change = precond[:, cols] * image
        curve += dirn[:, cols] * image
        square += change * image
        damped += pull * dirn[:, cols]
        mixed += pull * change
        scaled += damping[:, cols] * change * change
    scalars = (rz_in[0:1, :],) + tuple(map(jnp.sum, (curve, square, damped, mixed, scaled)))
    send_picks(table, ids, scalars, stage, out)


def last_kernel(
    own, partner, proj, damping, steps, first_dir, res, dirn,
    sol_hbm, res_hbm, weights, sol_out, res_out, sem,
):
    weights[...] = own[...] + partner[...]
    rows = proj.shape[0] * 8
    curve = weights[rows : rows + 1, :] + steps[3:4, :]
    alpha = steps[2:3, :] / curve
    alpha_first = steps[0:1, :]
    chunks = damping.shape[1] // LANES
    copies = []

    def send(here, there, first, last):
        cols = pl.ds(first * LANES, (last - first) * LANES)
        copy = pltpu.make_async_copy(here.at[:, cols], there.at[:, cols], sem.at[len(copies)])
        copy.start()
        copies.append(copy)

    for h in range(chunks):
        cols = slice(h * LANES, (h + 1) * LANES)
        sol_out[:, cols] = alpha_first * first_dir[:, cols] + alpha * dirn[:, cols]
    for h in range(chunks):
        cols = slice(h * LANES, (h + 1) * LANES)
        image = lifted(proj, weights, h) + damping[:, cols] * dirn[:, cols]
        res_out[:, cols] = res[:, cols] - alpha * image
        if h == 0:
            send(sol_out, sol_hbm, 0, chunks)
        elif h % 2 == 0:
            send(res_out, res_hbm, h - 2, h)
    send(res_out, res_hbm, chunks - 2, chunks)
    for copy in copies:
        copy.wait()


def local(jacobian, splat_ids, pix_residual, live_blocks, proj_jac, damping, precond):
    n_blk, n_pix, n_col = jacobian.shape
    n_par, g_dev = damping.shape
    n_scene, n_x = lax.axis_size("scene"), lax.axis_size("x")
    per = LANES // n_scene
    msg = f32(n_scene, per, LANES)
    wide = f32(n_scene, n_x, per, LANES)
    sums = f32(80, LANES)
    state = f32(n_par, g_dev)
    square = pltpu.VMEM((LANES, LANES), F32)
    whole = jax.ShapeDtypeStruct
    weights = pltpu.VMEM((80, LANES), F32)
    table = pltpu.VMEM((72, LANES), F32)

    def to_owners(message, right):
        flat = message.reshape(n_scene * n_x, per, LANES)
        got = lax.all_to_all(flat, ("scene", "x"), 0, 0, tiled=True)
        first = right is None
        wide_k = n_x * n_blk * LANES
        extra = (whole((n_blk, LANES), jnp.int32), whole((LANES, wide_k), BF16))
        own, *kept = call(
            functools.partial(sum_kernel, first),
            (sums,) + (extra if first else ()),
            [VMEM] * (1 if first else 2),
            [
                pltpu.VMEM((n_x, LANES, LANES), F32),
                pltpu.VMEM((n_x, LANES, LANES), F32),
                pltpu.VMEM((160, wide_k), BF16),
            ],
            1 << 31,
        )(got.reshape(n_scene, n_x, per, LANES), *(() if first else (right,)))
        partner = lax.ppermute(own, "core", [(0, 1), (1, 0)])
        return own, partner, *kept

    def to_blocks(message):
        return lax.all_to_all(message, "scene", 0, 0, tiled=True)

    message, jac, aux = call(
        rhs_kernel,
        (wide, whole(jacobian.shape, BF16), whole((2 * n_blk, LANES), jnp.int32)),
        [HBM] * 4,
        [
            pltpu.VMEM((n_blk, n_pix), BF16),
            pltpu.VMEM((1, live_blocks.shape[0]), jnp.int32),
            pltpu.VMEM((n_blk, LANES), jnp.int32),
            square,
            pltpu.SemaphoreType.DMA((n_blk,)),
            pltpu.SemaphoreType.DMA((3,)),
        ],
    )(*map(in_hbm, (live_blocks.reshape(1, -1), jacobian, pix_residual, splat_ids)))
    own, partner, index, right = to_owners(message, None)
    matrix = call(form_kernel, (f32(45 * 8, LANES),), [VMEM] * 3, (), 1 << 31)(
        own, proj_jac, precond
    )[0]
    message = call(start_kernel, (msg,), [VMEM] * 4, [weights, table, square])(
        own, partner, matrix, index
    )[0]
    first_own, first_partner = own, partner
    arrived = to_blocks(message)
    message, picks = call(
        first_kernel,
        (wide, f32(n_blk, n_col)),
        [VMEM] * 3,
        [square, square],
    )(jac, aux, arrived)
    own, partner = to_owners(message, right)
    res, first_dir, cross, rz = call(
        state_kernel, (state, state, f32(72, LANES), f32(8, LANES)), [VMEM] * 6, [weights], 1 << 31
    )(own, first_own, first_partner, proj_jac, precond, damping)
    message, image = call(step_kernel, (msg, state), [VMEM] * 10, [weights, table, square])(
        own, partner, proj_jac, precond, damping, matrix, cross, rz, index, first_dir
    )
    arrived = to_blocks(message)
    message, steps = call(
        second_kernel, (wide, f32(8, LANES)), [VMEM] * 4, [square, square]
    )(jac, aux, arrived, picks)
    own, partner = to_owners(message, right)
    res, second_dir = call(update_kernel, (state, state), [VMEM] * 6, (), 1 << 31)(
        own, steps, res, first_dir, image, precond
    )
    held = pltpu.VMEM((n_par, g_dev), F32)
    return call(
        last_kernel,
        (state, state),
        [VMEM] * 8,
        [weights, held, held, pltpu.SemaphoreType.DMA((1 + g_dev // (2 * LANES),))],
        out_space=HBM,
    )(
        own, partner, proj_jac, damping, steps, first_dir, res, second_dir
    )


def solution(mesh):
    scene = mesh.shape["scene"]
    finer = Mesh(mesh.devices.reshape(scene, -1, 2), ("scene", "x", "core"))
    everywhere = ("scene", "x", "core")
    in_specs = (
        P(everywhere, None, None),
        P(everywhere, None),
        P(everywhere, None),
        P(),
        P(None, None, "scene"),
        P(None, "scene"),
        P(None, "scene"),
    )
    out_specs = (P(None, "scene"), P(None, "scene"))
    return jax.shard_map(local, mesh=finer, in_specs=in_specs, out_specs=out_specs, check_vma=False)
```

```python
import functools

import jax
import jax.numpy as jnp
from jax import lax
from jax.experimental import pallas as pl
from jax.experimental.pallas import tpu as pltpu
from jax.sharding import Mesh
from jax.sharding import PartitionSpec as P

F32 = jnp.float32
BF16 = jnp.bfloat16
LANES = 128
ROWS = 16
VMEM = pl.BlockSpec(memory_space=pltpu.VMEM)
HBM = pl.BlockSpec(memory_space=pltpu.HBM)
NT = (((1,), (1,)), ((), ()))


def call(kernel, out, in_specs, scratch=(), flops=1 << 20, out_space=VMEM):
    return pl.pallas_call(
        kernel,
        out_shape=out,
        in_specs=in_specs,
        out_specs=jax.tree.map(lambda _: out_space, out),
        scratch_shapes=scratch,
        compiler_params=pltpu.CompilerParams(vmem_limit_bytes=24 << 20),
        cost_estimate=pl.CostEstimate(flops=flops, bytes_accessed=1 << 20, transcendentals=0),
    )


def in_hbm(array):
    return pltpu.with_memory_space_constraint(array, pltpu.HBM)


def f32(*shape):
    return jax.ShapeDtypeStruct(shape, F32)


def clear_stage(ids, stage, n_proj):
    stage[...] = jnp.zeros_like(stage)
    stage[pl.ds(n_proj, ids.shape[0], stride=ROWS), :] = ids.astype(F32)


def pack_return(acc, scalars, stage, out):
    n_blk = acc.shape[0]
    n_proj = acc.shape[1] // LANES
    for k in range(n_proj):
        stage[pl.ds(k, n_blk, stride=ROWS), :] = acc[:, k * LANES : (k + 1) * LANES]
    for i, value in enumerate(scalars):
        stage[n_proj + 1 + i : n_proj + 2 + i, :] = value
    turned = stage[...].T.reshape(out.shape[0], *out.shape[2:])
    for x in range(out.shape[1]):
        out[:, x] = turned


def rhs_kernel(live, jac, pix, ids, out, jbuf, aux, pixels, lives, index, stage, sem, small):
    n_blk = jac.shape[0]
    minor = [
        pltpu.make_async_copy(pix, pixels, small.at[0]),
        pltpu.make_async_copy(live, lives, small.at[1]),
        pltpu.make_async_copy(ids, index, small.at[2]),
    ]
    copies = [pltpu.make_async_copy(jac.at[b], jbuf.at[b], sem.at[b]) for b in range(n_blk)]
    for copy in minor + copies:
        copy.start()
    for copy in minor:
        copy.wait()
    n_x, n_core = lax.axis_size("x"), lax.axis_size("core")
    position = (lax.axis_index("scene") * n_x + lax.axis_index("x")) * n_core
    position = position + lax.axis_index("core")
    lane = lax.broadcasted_iota(jnp.int32, lives.shape, 1)
    own = jnp.sum(jnp.where(lane == position, lives[...], 0), axis=1, keepdims=True)
    local_ids = index[...] & (LANES * 8 - 1)
    aux[0:n_blk, :] = local_ids
    aux[n_blk : 2 * n_blk, :] = jnp.broadcast_to(own, (n_blk, LANES))
    clear_stage(local_ids, stage, jac.shape[2] // LANES)
    row = lax.broadcasted_iota(jnp.int32, pix.shape, 0)
    keep = row < jnp.broadcast_to(own, pix.shape)
    values = jnp.where(keep, pixels[...].astype(F32), 0.0)
    n_pix, n_col = jac.shape[1:]
    acc = jnp.zeros((n_blk, n_col), F32)
    cut = n_blk * 3 // 4
    for first, last in ((0, cut), (cut, n_blk)):
        signals = [jnp.where(row == b, values, 0.0).astype(BF16) for b in range(first, last)]
        for copy in copies[first:last]:
            copy.wait()
        stacked = jbuf[first:last].reshape((last - first) * n_pix, n_col)
        acc += jnp.dot(jnp.concatenate(signals, axis=1), stacked, preferred_element_type=F32)
    pack_return(acc, (), stage, out)


def lane_image(jac, b, line, ones):
    pieces = []
    for top in range(0, jac.shape[1], 64):
        folded = jnp.zeros((64, LANES), F32)
        for at in range(0, jac.shape[2], LANES):
            tile = jac[b, top : top + 64, at : at + LANES].astype(F32)
            folded += tile * line[:, at : at + LANES]
        high = folded.astype(BF16)
        pieces.append(jnp.concatenate([high, (folded - high.astype(F32)).astype(BF16)], axis=1))
    return lax.dot_general(
        ones, jnp.concatenate(pieces, axis=0), NT, preferred_element_type=F32
    )


def block_pass(picks, aux, jac, by_lanes):
    n_blk, n_pix = jac.shape[:2]
    row = lax.broadcasted_iota(jnp.int32, (n_blk, n_pix), 0)
    live = row < aux[n_blk : n_blk + 1, 0:1]
    chosen = picks.astype(BF16)
    rounded = chosen.astype(F32)
    ones = jnp.ones((n_blk, 2 * LANES), BF16)
    signals = []
    for b in range(n_blk):
        if (b * by_lanes) // n_blk != ((b + 1) * by_lanes) // n_blk:
            image = lane_image(jac, b, rounded[b : b + 1, :], ones)
        else:
            image = lax.dot_general(chosen, jac[b], NT, preferred_element_type=F32)
        signals.append(jnp.where((row == b) & live, image, 0.0).astype(BF16))
    stacked = jac[...].reshape(n_blk * n_pix, jac.shape[2])
    return jnp.dot(jnp.concatenate(signals, axis=1), stacked, preferred_element_type=F32)


def unpack_picks(recv, turned, n_blk, n_proj):
    turned[...] = recv[...].reshape(LANES, LANES).T
    return jnp.concatenate(
        [turned[pl.ds(k, n_blk, stride=ROWS), :] for k in range(n_proj)], axis=1
    )


def over_lanes(rows):
    return jnp.broadcast_to(jnp.sum(rows, axis=1, keepdims=True), rows.shape)


def first_kernel(jac, aux, recv, out, picks_out, turned, stage):
    n_blk = jac.shape[0]
    n_proj = jac.shape[2] // LANES
    picks = unpack_picks(recv, turned, n_blk, n_proj)
    picks_out[...] = picks
    acc = block_pass(picks, aux, jac, 5)
    clear_stage(aux[0:n_blk, :], stage, n_proj)
    pack_return(acc, (), stage, out)


def second_kernel(jac, aux, recv, picks_in, out, steps_out, turned, stage):
    n_blk = jac.shape[0]
    n_proj = jac.shape[2] // LANES
    fresh = unpack_picks(recv, turned, n_blk, n_proj)
    per = recv.shape[1]
    totals = over_lanes(turned[8:16, :]) * (1.0 / per)
    rz, curve, square, damped, mixed, scaled = (totals[i : i + 1, :] for i in range(2, 8))
    alpha = rz / curve
    after = rz - 2.0 * alpha * curve + alpha * alpha * square
    beta = after / rz
    grown = 1.0 + beta
    steps_out[0:1, :] = alpha
    steps_out[1:2, :] = beta
    steps_out[2:3, :] = after
    steps_out[3:4, :] = (
        grown * grown * damped - 2.0 * grown * alpha * mixed + alpha * alpha * scaled
    )
    steps_out[4:8, :] = jnp.zeros((4, LANES), F32)
    pieces = []
    for k in range(n_proj):
        cols = slice(k * LANES, (k + 1) * LANES)
        pieces.append(grown * picks_in[:, cols] - alpha * fresh[:, cols])
    picks = jnp.concatenate(pieces, axis=1)
    acc = block_pass(picks, aux, jac, 5)
    weighed = picks * acc
    line = jnp.zeros((n_blk, LANES), F32)
    for k in range(n_proj):
        line += weighed[:, k * LANES : (k + 1) * LANES]
    line = over_lanes(jnp.sum(line, axis=0, keepdims=True))
    clear_stage(aux[0:n_blk, :], stage, n_proj)
    pack_return(acc, (line,), stage, out)


def update_kernel(after, steps, res, dirn, image, precond, res_out, dir_out):
    del after
    alpha, beta = steps[0:1, :], steps[1:2, :]
    for h in range(res.shape[1] // LANES):
        cols = slice(h * LANES, (h + 1) * LANES)
        new_res = res[:, cols] - alpha * image[:, cols]
        res_out[:, cols] = new_res
        dir_out[:, cols] = precond[:, cols] * new_res + beta * dirn[:, cols]


def sum_kernel(first, recv, *rest):
    if first:
        out, ids_out, right, turned, fine, left = rest
    else:
        right, out, turned, fine, left = rest
    n_x = recv.shape[1]
    n_blk = LANES // ROWS
    n_proj = 9
    sub = lax.broadcasted_iota(jnp.int32, (n_blk, LANES), 0)
    deep = lax.broadcasted_iota(jnp.int32, (LANES, LANES), 0).astype(BF16)
    half = n_proj * 8

    def spread(table, x, base, high):
        lines = [
            jnp.broadcast_to(table[x, base + k : base + k + 1, :], (8, LANES))
            for k in range(n_proj)
        ]
        return jnp.concatenate([jnp.where(high, line, 0.0) for line in lines], axis=0)

    for x in range(n_x):
        values = recv[:, x].reshape(LANES, LANES).T
        turned[x] = values
        fine[x] = values - values.astype(BF16).astype(F32)
        for b in range(n_blk):
            at = (x * n_blk + b) * LANES
            cols = slice(at, at + LANES)
            base = b * ROWS
            ids = turned[x, base + n_proj : base + n_proj + 1, :].astype(jnp.int32)
            high = jnp.broadcast_to(ids >> 7, (8, LANES)) == sub
            left[0:half, cols] = spread(turned, x, base, high).astype(BF16)
            left[80 : 80 + half, cols] = spread(fine, x, base, high).astype(BF16)
            if first:
                low = jnp.broadcast_to((ids & 127).astype(BF16), (LANES, LANES)) == deep
                right[:, cols] = jnp.where(low, jnp.ones_like(deep), jnp.zeros_like(deep))
    summed = lax.dot_general(left[...], right[...], NT, preferred_element_type=F32)
    out[0:half, :] = summed[0:half] + summed[80 : 80 + half]
    per = recv.shape[2]
    mixed = jnp.zeros((1, LANES), F32)
    for x in range(n_x):
        mixed += turned[x, n_proj + 1 : n_proj + 2, :]
    out[half : half + 1, :] = over_lanes(mixed) * (1.0 / per)
    out[half + 1 : half + 8, :] = jnp.zeros((7, LANES), F32)
    if first:
        ids_out[...] = turned[lax.axis_index("x"), pl.ds(n_proj, n_blk, stride=ROWS), :].astype(jnp.int32)


def lifted(proj, weights, h):
    cols = slice(h * LANES, (h + 1) * LANES)
    n_proj, n_par, _ = proj.shape
    acc = jnp.zeros((n_par, LANES), F32)
    for k in range(n_proj):
        line = weights[k * 8 + h : k * 8 + h + 1, :]
        acc += proj[k, :, cols].astype(F32) * jnp.broadcast_to(line, (n_par, LANES))
    return acc


def projected(proj, field, h, table):
    cols = slice(h * LANES, (h + 1) * LANES)
    for k in range(proj.shape[0]):
        table[k * 8 + h : k * 8 + h + 1, :] = jnp.sum(
            proj[k, :, cols].astype(F32) * field, axis=0, keepdims=True
        )


def pairs(n_proj):
    return [(k, m) for k in range(n_proj) for m in range(k, n_proj)]


def form_kernel(after, proj, precond, out):
    del after
    n_proj = proj.shape[0]
    for h in range(precond.shape[1] // LANES):
        cols = slice(h * LANES, (h + 1) * LANES)
        tiles = [proj[k, :, cols].astype(F32) for k in range(n_proj)]
        scaled = [tile * precond[:, cols] for tile in tiles]
        for i, (k, m) in enumerate(pairs(n_proj)):
            out[i * 8 + h : i * 8 + h + 1, :] = jnp.sum(
                scaled[k] * tiles[m], axis=0, keepdims=True
            )


def blended(matrix, weights):
    n_proj = 9
    sums = [None] * n_proj

    def add(k, tile, m):
        term = tile * weights[m * 8 : m * 8 + 8, :]
        sums[k] = term if sums[k] is None else sums[k] + term

    for i, (k, m) in enumerate(pairs(n_proj)):
        tile = matrix[i * 8 : i * 8 + 8, :]
        add(k, tile, m)
        if k != m:
            add(m, tile, k)
    return sums


def lane_pick(table, low):
    return jnp.take_along_axis(table, low, axis=1, mode="promise_in_bounds")


def send_picks(table, ids, scalars, stage, out):
    n_blk = ids.shape[0]
    n_chunk = 8
    stage[...] = jnp.zeros_like(stage)
    index = ids[...]
    low = index & 127
    high = index >> 7
    for b in range(n_blk):
        low_b = jnp.broadcast_to(low[b : b + 1, :], (8, LANES))
        high_b = jnp.broadcast_to(high[b : b + 1, :], (8, LANES))
        got = jnp.zeros((8, LANES), F32)
        for h in range(n_chunk):
            piece = lane_pick(table[pl.ds(h, 8, stride=8), :], low_b)
            got = jnp.where(high_b == h, piece, got)
        stage[b * ROWS : b * ROWS + 8, :] = got
    got = jnp.zeros((n_blk, LANES), F32)
    for h in range(n_chunk):
        line = jnp.broadcast_to(table[64 + h : 65 + h, :], (n_blk, LANES))
        got = jnp.where(high == h, lane_pick(line, low), got)
    stage[pl.ds(8, n_blk, stride=ROWS), :] = got
    at = 10
    for rows in scalars:
        stage[at : at + rows.shape[0], :] = rows
        at += rows.shape[0]
    out[...] = stage[...].T.reshape(out.shape)


def start_kernel(own, partner, matrix, ids, out, weights, table, stage):
    weights[...] = own[...] + partner[...]
    for k, tile in enumerate(blended(matrix, weights)):
        table[k * 8 : k * 8 + 8, :] = -tile
    send_picks(table, ids, (), stage, out)


def state_kernel(
    after, own, partner, proj, precond, damping, res_out, dir_out, cross, rz_out, weights
):
    del after
    weights[...] = own[...] + partner[...]
    n_par, width = precond.shape
    rz = jnp.zeros((n_par, LANES), F32)
    for h in range(width // LANES):
        cols = slice(h * LANES, (h + 1) * LANES)
        res = -lifted(proj, weights, h)
        dirn = precond[:, cols] * res
        res_out[:, cols] = res
        dir_out[:, cols] = dirn
        rz += res * dirn
        projected(proj, precond[:, cols] * damping[:, cols] * dirn, h, cross)
    rz_out[...] = jnp.full(rz_out.shape, jnp.sum(rz), F32)


def step_kernel(
    own, partner, proj, precond, damping, matrix, cross, rz_in, ids, dirn,
    out, image_out, weights, table, stage,
):
    weights[...] = own[...] + partner[...]
    n_par, width = precond.shape
    for k, tile in enumerate(blended(matrix, weights)):
        table[k * 8 : k * 8 + 8, :] = tile + cross[k * 8 : k * 8 + 8, :]
    curve, square, damped, mixed, scaled = [jnp.zeros((n_par, LANES), F32)] * 5
    for h in range(width // LANES):
        cols = slice(h * LANES, (h + 1) * LANES)
        pull = damping[:, cols] * dirn[:, cols]
        image = lifted(proj, weights, h) + pull
        image_out[:, cols] = image
        change = precond[:, cols] * image
        curve += dirn[:, cols] * image
        square += change * image
        damped += pull * dirn[:, cols]
        mixed += pull * change
        scaled += damping[:, cols] * change * change
    lines = [jnp.sum(each, axis=0, keepdims=True) for each in (curve, square, damped, mixed, scaled)]
    send_picks(table, ids, (rz_in[0:1, :], over_lanes(jnp.concatenate(lines, axis=0))), stage, out)


def last_kernel(
    own, partner, proj, damping, steps, first_dir, res, dirn,
    sol_hbm, res_hbm, weights, sol_out, res_out, sem,
):
    weights[...] = own[...] + partner[...]
    rows = proj.shape[0] * 8
    curve = weights[rows : rows + 1, :] + steps[3:4, :]
    alpha = steps[2:3, :] / curve
    alpha_first = steps[0:1, :]
    chunks = damping.shape[1] // LANES
    copies = []

    def send(here, there, first, last):
        cols = pl.ds(first * LANES, (last - first) * LANES)
        copy = pltpu.make_async_copy(here.at[:, cols], there.at[:, cols], sem.at[len(copies)])
        copy.start()
        copies.append(copy)

    for h in range(chunks):
        cols = slice(h * LANES, (h + 1) * LANES)
        sol_out[:, cols] = alpha_first * first_dir[:, cols] + alpha * dirn[:, cols]
    for h in range(chunks):
        cols = slice(h * LANES, (h + 1) * LANES)
        image = lifted(proj, weights, h) + damping[:, cols] * dirn[:, cols]
        res_out[:, cols] = res[:, cols] - alpha * image
        if h == 0:
            send(sol_out, sol_hbm, 0, chunks)
        elif h % 2 == 0:
            send(res_out, res_hbm, h - 2, h)
    send(res_out, res_hbm, chunks - 2, chunks)
    for copy in copies:
        copy.wait()


def local(jacobian, splat_ids, pix_residual, live_blocks, proj_jac, damping, precond):
    n_blk, n_pix, n_col = jacobian.shape
    n_par, g_dev = damping.shape
    n_scene, n_x = lax.axis_size("scene"), lax.axis_size("x")
    per = LANES // n_scene
    msg = f32(n_scene, per, LANES)
    wide = f32(n_scene, n_x, per, LANES)
    sums = f32(80, LANES)
    state = f32(n_par, g_dev)
    square = pltpu.VMEM((LANES, LANES), F32)
    whole = jax.ShapeDtypeStruct
    weights = pltpu.VMEM((80, LANES), F32)
    table = pltpu.VMEM((72, LANES), F32)

    def to_owners(message, right):
        flat = message.reshape(n_scene * n_x, per, LANES)
        got = lax.all_to_all(flat, ("scene", "x"), 0, 0, tiled=True)
        first = right is None
        wide_k = n_x * n_blk * LANES
        extra = (whole((n_blk, LANES), jnp.int32), whole((LANES, wide_k), BF16))
        own, *kept = call(
            functools.partial(sum_kernel, first),
            (sums,) + (extra if first else ()),
            [VMEM] * (1 if first else 2),
            [
                pltpu.VMEM((n_x, LANES, LANES), F32),
                pltpu.VMEM((n_x, LANES, LANES), F32),
                pltpu.VMEM((160, wide_k), BF16),
            ],
            1 << 31,
        )(got.reshape(n_scene, n_x, per, LANES), *(() if first else (right,)))
        partner = lax.ppermute(own, "core", [(0, 1), (1, 0)])
        return own, partner, *kept

    def to_blocks(message):
        return lax.all_to_all(message, "scene", 0, 0, tiled=True)

    message, jac, aux = call(
        rhs_kernel,
        (wide, whole(jacobian.shape, BF16), whole((2 * n_blk, LANES), jnp.int32)),
        [HBM] * 4,
        [
            pltpu.VMEM((n_blk, n_pix), BF16),
            pltpu.VMEM((1, live_blocks.shape[0]), jnp.int32),
            pltpu.VMEM((n_blk, LANES), jnp.int32),
            square,
            pltpu.SemaphoreType.DMA((n_blk,)),
            pltpu.SemaphoreType.DMA((3,)),
        ],
    )(*map(in_hbm, (live_blocks.reshape(1, -1), jacobian, pix_residual, splat_ids)))
    own, partner, index, right = to_owners(message, None)
    matrix = call(form_kernel, (f32(45 * 8, LANES),), [VMEM] * 3, (), 1 << 31)(
        own, proj_jac, precond
    )[0]
    message = call(start_kernel, (msg,), [VMEM] * 4, [weights, table, square])(
        own, partner, matrix, index
    )[0]
    first_own, first_partner = own, partner
    arrived = to_blocks(message)
    message, picks = call(
        first_kernel,
        (wide, f32(n_blk, n_col)),
        [VMEM] * 3,
        [square, square],
    )(jac, aux, arrived)
    own, partner = to_owners(message, right)
    res, first_dir, cross, rz = call(
        state_kernel, (state, state, f32(72, LANES), f32(8, LANES)), [VMEM] * 6, [weights], 1 << 31
    )(own, first_own, first_partner, proj_jac, precond, damping)
    message, image = call(step_kernel, (msg, state), [VMEM] * 10, [weights, table, square])(
        own, partner, proj_jac, precond, damping, matrix, cross, rz, index, first_dir
    )
    arrived = to_blocks(message)
    message, steps = call(
        second_kernel, (wide, f32(8, LANES)), [VMEM] * 4, [square, square]
    )(jac, aux, arrived, picks)
    own, partner = to_owners(message, right)
    res, second_dir = call(update_kernel, (state, state), [VMEM] * 6, (), 1 << 31)(
        own, steps, res, first_dir, image, precond
    )
    held = pltpu.VMEM((n_par, g_dev), F32)
    return call(
        last_kernel,
        (state, state),
        [VMEM] * 8,
        [weights, held, held, pltpu.SemaphoreType.DMA((1 + g_dev // (2 * LANES),))],
        out_space=HBM,
    )(
        own, partner, proj_jac, damping, steps, first_dir, res, second_dir
    )


def solution(mesh):
    scene = mesh.shape["scene"]
    finer = Mesh(mesh.devices.reshape(scene, -1, 2), ("scene", "x", "core"))
    everywhere = ("scene", "x", "core")
    in_specs = (
        P(everywhere, None, None),
        P(everywhere, None),
        P(everywhere, None),
        P(),
        P(None, None, "scene"),
        P(None, "scene"),
        P(None, "scene"),
    )
    out_specs = (P(None, "scene"), P(None, "scene"))
    return jax.shard_map(local, mesh=finer, in_specs=in_specs, out_specs=out_specs, check_vma=False)
```

```python
import functools

import jax
import jax.numpy as jnp
from jax import lax
from jax.experimental import pallas as pl
from jax.experimental.pallas import tpu as pltpu
from jax.sharding import Mesh
from jax.sharding import PartitionSpec as P

F32 = jnp.float32
BF16 = jnp.bfloat16
LANES = 128
ROWS = 16
VMEM = pl.BlockSpec(memory_space=pltpu.VMEM)
HBM = pl.BlockSpec(memory_space=pltpu.HBM)
NT = (((1,), (1,)), ((), ()))


def call(kernel, out, in_specs, scratch=(), flops=1 << 20, out_space=VMEM):
    return pl.pallas_call(
        kernel,
        out_shape=out,
        in_specs=in_specs,
        out_specs=jax.tree.map(lambda _: out_space, out),
        scratch_shapes=scratch,
        compiler_params=pltpu.CompilerParams(vmem_limit_bytes=24 << 20),
        cost_estimate=pl.CostEstimate(flops=flops, bytes_accessed=1 << 20, transcendentals=0),
    )


def in_hbm(array):
    return pltpu.with_memory_space_constraint(array, pltpu.HBM)


def f32(*shape):
    return jax.ShapeDtypeStruct(shape, F32)


def clear_stage(ids, stage, n_proj):
    stage[...] = jnp.zeros_like(stage)
    stage[pl.ds(n_proj, ids.shape[0], stride=ROWS), :] = ids.astype(F32)


def send_return(stage, out):
    turned = stage[...].T.reshape(out.shape[0], *out.shape[2:])
    for x in range(out.shape[1]):
        out[:, x] = turned


def pack_return(acc, scalars, stage, out):
    n_blk = acc.shape[0]
    n_proj = acc.shape[1] // LANES
    for k in range(n_proj):
        stage[pl.ds(k, n_blk, stride=ROWS), :] = acc[:, k * LANES : (k + 1) * LANES]
    for i, value in enumerate(scalars):
        stage[n_proj + 1 + i : n_proj + 2 + i, :] = value
    send_return(stage, out)


def rhs_kernel(
    live, jac, pix, ids, out, jbuf, aux, pixels, lives, index, stage, spread, sem, small
):
    n_blk = jac.shape[0]
    minor = [
        pltpu.make_async_copy(pix, pixels, small.at[0]),
        pltpu.make_async_copy(live, lives, small.at[1]),
        pltpu.make_async_copy(ids, index, small.at[2]),
    ]
    copies = [pltpu.make_async_copy(jac.at[b], jbuf.at[b], sem.at[b]) for b in range(n_blk)]
    for copy in minor + copies:
        copy.start()
    for copy in minor:
        copy.wait()
    n_x, n_core = lax.axis_size("x"), lax.axis_size("core")
    position = (lax.axis_index("scene") * n_x + lax.axis_index("x")) * n_core
    position = position + lax.axis_index("core")
    lane = lax.broadcasted_iota(jnp.int32, lives.shape, 1)
    own = jnp.sum(jnp.where(lane == position, lives[...], 0), axis=1, keepdims=True)
    local_ids = index[...] & (LANES * 8 - 1)
    aux[0:n_blk, :] = local_ids
    aux[n_blk : 2 * n_blk, :] = jnp.broadcast_to(own, (n_blk, LANES))
    clear_stage(local_ids, stage, jac.shape[2] // LANES)
    row = lax.broadcasted_iota(jnp.int32, pix.shape, 0)
    keep = row < jnp.broadcast_to(own, pix.shape)
    values = jnp.where(keep, pixels[...].astype(F32), 0.0)
    n_pix, n_col = jac.shape[1:]
    for half in range(0, n_pix, LANES):
        turned = values[:, half : half + LANES].T
        for b in range(n_blk):
            spread[b, half : half + LANES, :] = jnp.broadcast_to(
                turned[:, b : b + 1], (LANES, LANES)
            )
    for b, copy in enumerate(copies):
        copy.wait()
        sums = [jnp.zeros((16, LANES), F32)] * (n_col // LANES)
        for top in range(0, n_pix, 16):
            line = spread[b, top : top + 16, :]
            for k in range(len(sums)):
                tile = jbuf[b, top : top + 16, k * LANES : (k + 1) * LANES].astype(F32)
                sums[k] = sums[k] + tile * line
        for k, each in enumerate(sums):
            at = b * ROWS + k
            stage[at : at + 1, :] = jnp.sum(each, axis=0, keepdims=True)
    send_return(stage, out)


def lane_image(jac, b, line, ones):
    pieces = []
    for top in range(0, jac.shape[1], 64):
        folded = jnp.zeros((64, LANES), F32)
        for at in range(0, jac.shape[2], LANES):
            tile = jac[b, top : top + 64, at : at + LANES].astype(F32)
            folded += tile * line[:, at : at + LANES]
        high = folded.astype(BF16)
        pieces.append(jnp.concatenate([high, (folded - high.astype(F32)).astype(BF16)], axis=1))
    return lax.dot_general(
        ones, jnp.concatenate(pieces, axis=0), NT, preferred_element_type=F32
    )


def block_pass(picks, aux, jac, by_lanes):
    n_blk, n_pix = jac.shape[:2]
    row = lax.broadcasted_iota(jnp.int32, (n_blk, n_pix), 0)
    live = row < aux[n_blk : n_blk + 1, 0:1]
    chosen = picks.astype(BF16)
    rounded = chosen.astype(F32)
    ones = jnp.ones((n_blk, 2 * LANES), BF16)
    signals = []
    for b in range(n_blk):
        if (b * by_lanes) // n_blk != ((b + 1) * by_lanes) // n_blk:
            image = lane_image(jac, b, rounded[b : b + 1, :], ones)
        else:
            image = lax.dot_general(chosen, jac[b], NT, preferred_element_type=F32)
        signals.append(jnp.where((row == b) & live, image, 0.0).astype(BF16))
    stacked = jac[...].reshape(n_blk * n_pix, jac.shape[2])
    return jnp.dot(jnp.concatenate(signals, axis=1), stacked, preferred_element_type=F32)


def unpack_picks(recv, turned, n_blk, n_proj):
    turned[...] = recv[...].reshape(LANES, LANES).T
    return jnp.concatenate(
        [turned[pl.ds(k, n_blk, stride=ROWS), :] for k in range(n_proj)], axis=1
    )


def over_lanes(rows):
    return jnp.broadcast_to(jnp.sum(rows, axis=1, keepdims=True), rows.shape)


def first_kernel(jac, aux, recv, out, picks_out, turned, stage):
    n_blk = jac.shape[0]
    n_proj = jac.shape[2] // LANES
    picks = unpack_picks(recv, turned, n_blk, n_proj)
    picks_out[...] = picks
    acc = block_pass(picks, aux, jac, 5)
    clear_stage(aux[0:n_blk, :], stage, n_proj)
    pack_return(acc, (), stage, out)


def second_kernel(jac, aux, recv, picks_in, out, steps_out, turned, stage):
    n_blk = jac.shape[0]
    n_proj = jac.shape[2] // LANES
    fresh = unpack_picks(recv, turned, n_blk, n_proj)
    per = recv.shape[1]
    totals = over_lanes(turned[8:16, :]) * (1.0 / per)
    rz, curve, square, damped, mixed, scaled = (totals[i : i + 1, :] for i in range(2, 8))
    alpha = rz / curve
    after = rz - 2.0 * alpha * curve + alpha * alpha * square
    beta = after / rz
    grown = 1.0 + beta
    steps_out[0:1, :] = alpha
    steps_out[1:2, :] = beta
    steps_out[2:3, :] = after
    steps_out[3:4, :] = (
        grown * grown * damped - 2.0 * grown * alpha * mixed + alpha * alpha * scaled
    )
    steps_out[4:8, :] = jnp.zeros((4, LANES), F32)
    pieces = []
    for k in range(n_proj):
        cols = slice(k * LANES, (k + 1) * LANES)
        pieces.append(grown * picks_in[:, cols] - alpha * fresh[:, cols])
    picks = jnp.concatenate(pieces, axis=1)
    acc = block_pass(picks, aux, jac, 5)
    weighed = picks * acc
    line = jnp.zeros((n_blk, LANES), F32)
    for k in range(n_proj):
        line += weighed[:, k * LANES : (k + 1) * LANES]
    line = over_lanes(jnp.sum(line, axis=0, keepdims=True))
    clear_stage(aux[0:n_blk, :], stage, n_proj)
    pack_return(acc, (line,), stage, out)


def update_kernel(after, steps, res, dirn, image, precond, res_out, dir_out):
    del after
    alpha, beta = steps[0:1, :], steps[1:2, :]
    for h in range(res.shape[1] // LANES):
        cols = slice(h * LANES, (h + 1) * LANES)
        new_res = res[:, cols] - alpha * image[:, cols]
        res_out[:, cols] = new_res
        dir_out[:, cols] = precond[:, cols] * new_res + beta * dirn[:, cols]


def sum_kernel(first, recv, *rest):
    if first:
        out, ids_out, right, turned, fine, left = rest
    else:
        right, out, turned, fine, left = rest
    n_x = recv.shape[1]
    n_blk = LANES // ROWS
    n_proj = 9
    sub = lax.broadcasted_iota(jnp.int32, (n_blk, LANES), 0)
    deep = lax.broadcasted_iota(jnp.int32, (LANES, LANES), 0).astype(BF16)
    half = n_proj * 8

    def spread(table, x, base, high):
        lines = [
            jnp.broadcast_to(table[x, base + k : base + k + 1, :], (8, LANES))
            for k in range(n_proj)
        ]
        return jnp.concatenate([jnp.where(high, line, 0.0) for line in lines], axis=0)

    for x in range(n_x):
        values = recv[:, x].reshape(LANES, LANES).T
        turned[x] = values
        fine[x] = values - values.astype(BF16).astype(F32)
        for b in range(n_blk):
            at = (x * n_blk + b) * LANES
            cols = slice(at, at + LANES)
            base = b * ROWS
            ids = turned[x, base + n_proj : base + n_proj + 1, :].astype(jnp.int32)
            high = jnp.broadcast_to(ids >> 7, (8, LANES)) == sub
            left[0:half, cols] = spread(turned, x, base, high).astype(BF16)
            left[80 : 80 + half, cols] = spread(fine, x, base, high).astype(BF16)
            if first:
                low = jnp.broadcast_to((ids & 127).astype(BF16), (LANES, LANES)) == deep
                right[:, cols] = jnp.where(low, jnp.ones_like(deep), jnp.zeros_like(deep))
    summed = lax.dot_general(left[...], right[...], NT, preferred_element_type=F32)
    out[0:half, :] = summed[0:half] + summed[80 : 80 + half]
    per = recv.shape[2]
    mixed = jnp.zeros((1, LANES), F32)
    for x in range(n_x):
        mixed += turned[x, n_proj + 1 : n_proj + 2, :]
    out[half : half + 1, :] = over_lanes(mixed) * (1.0 / per)
    out[half + 1 : half + 8, :] = jnp.zeros((7, LANES), F32)
    if first:
        ids_out[...] = turned[lax.axis_index("x"), pl.ds(n_proj, n_blk, stride=ROWS), :].astype(jnp.int32)


def lifted(proj, weights, h):
    cols = slice(h * LANES, (h + 1) * LANES)
    n_proj, n_par, _ = proj.shape
    acc = jnp.zeros((n_par, LANES), F32)
    for k in range(n_proj):
        line = weights[k * 8 + h : k * 8 + h + 1, :]
        acc += proj[k, :, cols].astype(F32) * jnp.broadcast_to(line, (n_par, LANES))
    return acc


def projected(proj, field, h, table):
    cols = slice(h * LANES, (h + 1) * LANES)
    for k in range(proj.shape[0]):
        table[k * 8 + h : k * 8 + h + 1, :] = jnp.sum(
            proj[k, :, cols].astype(F32) * field, axis=0, keepdims=True
        )


def pairs(n_proj):
    return [(k, m) for k in range(n_proj) for m in range(k, n_proj)]


def form_kernel(after, proj, precond, out):
    del after
    n_proj = proj.shape[0]
    for h in range(precond.shape[1] // LANES):
        cols = slice(h * LANES, (h + 1) * LANES)
        tiles = [proj[k, :, cols].astype(F32) for k in range(n_proj)]
        scaled = [tile * precond[:, cols] for tile in tiles]
        for i, (k, m) in enumerate(pairs(n_proj)):
            out[i * 8 + h : i * 8 + h + 1, :] = jnp.sum(
                scaled[k] * tiles[m], axis=0, keepdims=True
            )


def blended(matrix, weights):
    n_proj = 9
    sums = [None] * n_proj

    def add(k, tile, m):
        term = tile * weights[m * 8 : m * 8 + 8, :]
        sums[k] = term if sums[k] is None else sums[k] + term

    for i, (k, m) in enumerate(pairs(n_proj)):
        tile = matrix[i * 8 : i * 8 + 8, :]
        add(k, tile, m)
        if k != m:
            add(m, tile, k)
    return sums


def lane_pick(table, low):
    return jnp.take_along_axis(table, low, axis=1, mode="promise_in_bounds")


def send_picks(table, ids, scalars, stage, out):
    n_blk = ids.shape[0]
    n_chunk = 8
    stage[...] = jnp.zeros_like(stage)
    index = ids[...]
    low = index & 127
    high = index >> 7
    for b in range(n_blk):
        low_b = jnp.broadcast_to(low[b : b + 1, :], (8, LANES))
        high_b = jnp.broadcast_to(high[b : b + 1, :], (8, LANES))
        got = jnp.zeros((8, LANES), F32)
        for h in range(n_chunk):
            piece = lane_pick(table[pl.ds(h, 8, stride=8), :], low_b)
            got = jnp.where(high_b == h, piece, got)
        stage[b * ROWS : b * ROWS + 8, :] = got
    got = jnp.zeros((n_blk, LANES), F32)
    for h in range(n_chunk):
        line = jnp.broadcast_to(table[64 + h : 65 + h, :], (n_blk, LANES))
        got = jnp.where(high == h, lane_pick(line, low), got)
    stage[pl.ds(8, n_blk, stride=ROWS), :] = got
    at = 10
    for rows in scalars:
        stage[at : at + rows.shape[0], :] = rows
        at += rows.shape[0]
    out[...] = stage[...].T.reshape(out.shape)


def start_kernel(own, partner, matrix, ids, out, weights, table, stage):
    weights[...] = own[...] + partner[...]
    for k, tile in enumerate(blended(matrix, weights)):
        table[k * 8 : k * 8 + 8, :] = -tile
    send_picks(table, ids, (), stage, out)


def state_kernel(
    after, own, partner, proj, precond, damping, res_out, dir_out, cross, rz_out, weights
):
    del after
    weights[...] = own[...] + partner[...]
    n_par, width = precond.shape
    rz = jnp.zeros((n_par, LANES), F32)
    for h in range(width // LANES):
        cols = slice(h * LANES, (h + 1) * LANES)
        res = -lifted(proj, weights, h)
        dirn = precond[:, cols] * res
        res_out[:, cols] = res
        dir_out[:, cols] = dirn
        rz += res * dirn
        projected(proj, precond[:, cols] * damping[:, cols] * dirn, h, cross)
    rz_out[...] = jnp.full(rz_out.shape, jnp.sum(rz), F32)


def step_kernel(
    own, partner, proj, precond, damping, matrix, cross, rz_in, ids, dirn,
    out, image_out, weights, table, stage,
):
    weights[...] = own[...] + partner[...]
    n_par, width = precond.shape
    for k, tile in enumerate(blended(matrix, weights)):
        table[k * 8 : k * 8 + 8, :] = tile + cross[k * 8 : k * 8 + 8, :]
    curve, square, damped, mixed, scaled = [jnp.zeros((n_par, LANES), F32)] * 5
    for h in range(width // LANES):
        cols = slice(h * LANES, (h + 1) * LANES)
        pull = damping[:, cols] * dirn[:, cols]
        image = lifted(proj, weights, h) + pull
        image_out[:, cols] = image
        change = precond[:, cols] * image
        curve += dirn[:, cols] * image
        square += change * image
        damped += pull * dirn[:, cols]
        mixed += pull * change
        scaled += damping[:, cols] * change * change
    lines = [jnp.sum(each, axis=0, keepdims=True) for each in (curve, square, damped, mixed, scaled)]
    send_picks(table, ids, (rz_in[0:1, :], over_lanes(jnp.concatenate(lines, axis=0))), stage, out)


def last_kernel(
    own, partner, proj, damping, steps, first_dir, res, dirn,
    sol_hbm, res_hbm, weights, sol_out, res_out, sem,
):
    weights[...] = own[...] + partner[...]
    rows = proj.shape[0] * 8
    curve = weights[rows : rows + 1, :] + steps[3:4, :]
    alpha = steps[2:3, :] / curve
    alpha_first = steps[0:1, :]
    chunks = damping.shape[1] // LANES
    copies = []

    def send(here, there, first, last):
        cols = pl.ds(first * LANES, (last - first) * LANES)
        copy = pltpu.make_async_copy(here.at[:, cols], there.at[:, cols], sem.at[len(copies)])
        copy.start()
        copies.append(copy)

    for h in range(chunks):
        cols = slice(h * LANES, (h + 1) * LANES)
        sol_out[:, cols] = alpha_first * first_dir[:, cols] + alpha * dirn[:, cols]
    for h in range(chunks):
        cols = slice(h * LANES, (h + 1) * LANES)
        image = lifted(proj, weights, h) + damping[:, cols] * dirn[:, cols]
        res_out[:, cols] = res[:, cols] - alpha * image
        if h == 0:
            send(sol_out, sol_hbm, 0, chunks)
        elif h % 2 == 0:
            send(res_out, res_hbm, h - 2, h)
    send(res_out, res_hbm, chunks - 2, chunks)
    for copy in copies:
        copy.wait()


def local(jacobian, splat_ids, pix_residual, live_blocks, proj_jac, damping, precond):
    n_blk, n_pix, n_col = jacobian.shape
    n_par, g_dev = damping.shape
    n_scene, n_x = lax.axis_size("scene"), lax.axis_size("x")
    per = LANES // n_scene
    msg = f32(n_scene, per, LANES)
    wide = f32(n_scene, n_x, per, LANES)
    sums = f32(80, LANES)
    state = f32(n_par, g_dev)
    square = pltpu.VMEM((LANES, LANES), F32)
    whole = jax.ShapeDtypeStruct
    weights = pltpu.VMEM((80, LANES), F32)
    table = pltpu.VMEM((72, LANES), F32)

    def to_owners(message, right):
        flat = message.reshape(n_scene * n_x, per, LANES)
        got = lax.all_to_all(flat, ("scene", "x"), 0, 0, tiled=True)
        first = right is None
        wide_k = n_x * n_blk * LANES
        extra = (whole((n_blk, LANES), jnp.int32), whole((LANES, wide_k), BF16))
        own, *kept = call(
            functools.partial(sum_kernel, first),
            (sums,) + (extra if first else ()),
            [VMEM] * (1 if first else 2),
            [
                pltpu.VMEM((n_x, LANES, LANES), F32),
                pltpu.VMEM((n_x, LANES, LANES), F32),
                pltpu.VMEM((160, wide_k), BF16),
            ],
            1 << 31,
        )(got.reshape(n_scene, n_x, per, LANES), *(() if first else (right,)))
        partner = lax.ppermute(own, "core", [(0, 1), (1, 0)])
        return own, partner, *kept

    def to_blocks(message):
        return lax.all_to_all(message, "scene", 0, 0, tiled=True)

    message, jac, aux = call(
        rhs_kernel,
        (wide, whole(jacobian.shape, BF16), whole((2 * n_blk, LANES), jnp.int32)),
        [HBM] * 4,
        [
            pltpu.VMEM((n_blk, n_pix), BF16),
            pltpu.VMEM((1, live_blocks.shape[0]), jnp.int32),
            pltpu.VMEM((n_blk, LANES), jnp.int32),
            square,
            pltpu.VMEM((n_blk, n_pix, LANES), F32),
            pltpu.SemaphoreType.DMA((n_blk,)),
            pltpu.SemaphoreType.DMA((3,)),
        ],
    )(*map(in_hbm, (live_blocks.reshape(1, -1), jacobian, pix_residual, splat_ids)))
    own, partner, index, right = to_owners(message, None)
    matrix = call(form_kernel, (f32(45 * 8, LANES),), [VMEM] * 3, (), 1 << 31)(
        own, proj_jac, precond
    )[0]
    message = call(start_kernel, (msg,), [VMEM] * 4, [weights, table, square])(
        own, partner, matrix, index
    )[0]
    first_own, first_partner = own, partner
    arrived = to_blocks(message)
    message, picks = call(
        first_kernel,
        (wide, f32(n_blk, n_col)),
        [VMEM] * 3,
        [square, square],
    )(jac, aux, arrived)
    own, partner = to_owners(message, right)
    res, first_dir, cross, rz = call(
        state_kernel, (state, state, f32(72, LANES), f32(8, LANES)), [VMEM] * 6, [weights], 1 << 31
    )(own, first_own, first_partner, proj_jac, precond, damping)
    message, image = call(step_kernel, (msg, state), [VMEM] * 10, [weights, table, square])(
        own, partner, proj_jac, precond, damping, matrix, cross, rz, index, first_dir
    )
    arrived = to_blocks(message)
    message, steps = call(
        second_kernel, (wide, f32(8, LANES)), [VMEM] * 4, [square, square]
    )(jac, aux, arrived, picks)
    own, partner = to_owners(message, right)
    res, second_dir = call(update_kernel, (state, state), [VMEM] * 6, (), 1 << 31)(
        own, steps, res, first_dir, image, precond
    )
    held = pltpu.VMEM((n_par, g_dev), F32)
    return call(
        last_kernel,
        (state, state),
        [VMEM] * 8,
        [weights, held, held, pltpu.SemaphoreType.DMA((1 + g_dev // (2 * LANES),))],
        out_space=HBM,
    )(
        own, partner, proj_jac, damping, steps, first_dir, res, second_dir
    )


def solution(mesh):
    scene = mesh.shape["scene"]
    finer = Mesh(mesh.devices.reshape(scene, -1, 2), ("scene", "x", "core"))
    everywhere = ("scene", "x", "core")
    in_specs = (
        P(everywhere, None, None),
        P(everywhere, None),
        P(everywhere, None),
        P(),
        P(None, None, "scene"),
        P(None, "scene"),
        P(None, "scene"),
    )
    out_specs = (P(None, "scene"), P(None, "scene"))
    return jax.shard_map(local, mesh=finer, in_specs=in_specs, out_specs=out_specs, check_vma=False)
```

```python
import functools

import jax
import jax.numpy as jnp
from jax import lax
from jax.experimental import pallas as pl
from jax.experimental.pallas import tpu as pltpu
from jax.sharding import Mesh
from jax.sharding import PartitionSpec as P

F32 = jnp.float32
BF16 = jnp.bfloat16
LANES = 128
ROWS = 16
VMEM = pl.BlockSpec(memory_space=pltpu.VMEM)
HBM = pl.BlockSpec(memory_space=pltpu.HBM)
NT = (((1,), (1,)), ((), ()))


def call(kernel, out, in_specs, scratch=(), flops=1 << 20, out_space=VMEM):
    return pl.pallas_call(
        kernel,
        out_shape=out,
        in_specs=in_specs,
        out_specs=jax.tree.map(lambda _: out_space, out),
        scratch_shapes=scratch,
        compiler_params=pltpu.CompilerParams(vmem_limit_bytes=24 << 20),
        cost_estimate=pl.CostEstimate(flops=flops, bytes_accessed=1 << 20, transcendentals=0),
    )


def in_hbm(array):
    return pltpu.with_memory_space_constraint(array, pltpu.HBM)


def f32(*shape):
    return jax.ShapeDtypeStruct(shape, F32)


def clear_stage(ids, stage, n_proj):
    stage[...] = jnp.zeros_like(stage)
    stage[pl.ds(n_proj, ids.shape[0], stride=ROWS), :] = ids.astype(F32)


def pack_return(acc, scalars, stage, out):
    n_blk = acc.shape[0]
    n_proj = acc.shape[1] // LANES
    for k in range(n_proj):
        stage[pl.ds(k, n_blk, stride=ROWS), :] = acc[:, k * LANES : (k + 1) * LANES]
    for i, value in enumerate(scalars):
        stage[n_proj + 1 + i : n_proj + 2 + i, :] = value
    turned = stage[...].T.reshape(out.shape[0], *out.shape[2:])
    for x in range(out.shape[1]):
        out[:, x] = turned


def rhs_kernel(live, jac, pix, ids, out, jbuf, aux, pixels, lives, index, stage, sem, small):
    n_blk = jac.shape[0]
    minor = [
        pltpu.make_async_copy(pix, pixels, small.at[0]),
        pltpu.make_async_copy(live, lives, small.at[1]),
        pltpu.make_async_copy(ids, index, small.at[2]),
    ]
    copies = [pltpu.make_async_copy(jac.at[b], jbuf.at[b], sem.at[b]) for b in range(n_blk)]
    for copy in minor + copies:
        copy.start()
    for copy in minor:
        copy.wait()
    n_x, n_core = lax.axis_size("x"), lax.axis_size("core")
    position = (lax.axis_index("scene") * n_x + lax.axis_index("x")) * n_core
    position = position + lax.axis_index("core")
    lane = lax.broadcasted_iota(jnp.int32, lives.shape, 1)
    own = jnp.sum(jnp.where(lane == position, lives[...], 0), axis=1, keepdims=True)
    local_ids = index[...] & (LANES * 8 - 1)
    aux[0:n_blk, :] = local_ids
    aux[n_blk : 2 * n_blk, :] = jnp.broadcast_to(own, (n_blk, LANES))
    clear_stage(local_ids, stage, jac.shape[2] // LANES)
    row = lax.broadcasted_iota(jnp.int32, pix.shape, 0)
    keep = row < jnp.broadcast_to(own, pix.shape)
    values = jnp.where(keep, pixels[...].astype(F32), 0.0)
    n_pix, n_col = jac.shape[1:]
    acc = jnp.zeros((n_blk, n_col), F32)
    cut = n_blk * 5 // 8
    for first, last in ((0, cut), (cut, n_blk)):
        signals = [jnp.where(row == b, values, 0.0).astype(BF16) for b in range(first, last)]
        for copy in copies[first:last]:
            copy.wait()
        stacked = jbuf[first:last].reshape((last - first) * n_pix, n_col)
        acc += jnp.dot(jnp.concatenate(signals, axis=1), stacked, preferred_element_type=F32)
    pack_return(acc, (), stage, out)


def lane_image(jac, b, line, ones):
    pieces = []
    for top in range(0, jac.shape[1], 64):
        folded = jnp.zeros((64, LANES), F32)
        for at in range(0, jac.shape[2], LANES):
            tile = jac[b, top : top + 64, at : at + LANES].astype(F32)
            folded += tile * line[:, at : at + LANES]
        high = folded.astype(BF16)
        pieces.append(jnp.concatenate([high, (folded - high.astype(F32)).astype(BF16)], axis=1))
    return lax.dot_general(
        ones, jnp.concatenate(pieces, axis=0), NT, preferred_element_type=F32
    )


def block_pass(picks, aux, jac, by_lanes):
    n_blk, n_pix = jac.shape[:2]
    row = lax.broadcasted_iota(jnp.int32, (n_blk, n_pix), 0)
    live = row < aux[n_blk : n_blk + 1, 0:1]
    chosen = picks.astype(BF16)
    rounded = chosen.astype(F32)
    ones = jnp.ones((n_blk, 2 * LANES), BF16)
    signals = []
    for b in range(n_blk):
        if (b * by_lanes) // n_blk != ((b + 1) * by_lanes) // n_blk:
            image = lane_image(jac, b, rounded[b : b + 1, :], ones)
        else:
            image = lax.dot_general(chosen, jac[b], NT, preferred_element_type=F32)
        signals.append(jnp.where((row == b) & live, image, 0.0).astype(BF16))
    stacked = jac[...].reshape(n_blk * n_pix, jac.shape[2])
    return jnp.dot(jnp.concatenate(signals, axis=1), stacked, preferred_element_type=F32)


def unpack_picks(recv, turned, n_blk, n_proj):
    turned[...] = recv[...].reshape(LANES, LANES).T
    return jnp.concatenate(
        [turned[pl.ds(k, n_blk, stride=ROWS), :] for k in range(n_proj)], axis=1
    )


def over_lanes(rows):
    return jnp.broadcast_to(jnp.sum(rows, axis=1, keepdims=True), rows.shape)


def first_kernel(jac, aux, recv, out, picks_out, turned, stage):
    n_blk = jac.shape[0]
    n_proj = jac.shape[2] // LANES
    picks = unpack_picks(recv, turned, n_blk, n_proj)
    picks_out[...] = picks
    acc = block_pass(picks, aux, jac, 5)
    clear_stage(aux[0:n_blk, :], stage, n_proj)
    pack_return(acc, (), stage, out)


def second_kernel(jac, aux, recv, picks_in, out, steps_out, turned, stage):
    n_blk = jac.shape[0]
    n_proj = jac.shape[2] // LANES
    fresh = unpack_picks(recv, turned, n_blk, n_proj)
    per = recv.shape[1]
    totals = over_lanes(turned[8:16, :]) * (1.0 / per)
    rz, curve, square, damped, mixed, scaled = (totals[i : i + 1, :] for i in range(2, 8))
    alpha = rz / curve
    after = rz - 2.0 * alpha * curve + alpha * alpha * square
    beta = after / rz
    grown = 1.0 + beta
    steps_out[0:1, :] = alpha
    steps_out[1:2, :] = beta
    steps_out[2:3, :] = after
    steps_out[3:4, :] = (
        grown * grown * damped - 2.0 * grown * alpha * mixed + alpha * alpha * scaled
    )
    steps_out[4:8, :] = jnp.zeros((4, LANES), F32)
    pieces = []
    for k in range(n_proj):
        cols = slice(k * LANES, (k + 1) * LANES)
        pieces.append(grown * picks_in[:, cols] - alpha * fresh[:, cols])
    picks = jnp.concatenate(pieces, axis=1)
    acc = block_pass(picks, aux, jac, 5)
    weighed = picks * acc
    line = jnp.zeros((n_blk, LANES), F32)
    for k in range(n_proj):
        line += weighed[:, k * LANES : (k + 1) * LANES]
    line = over_lanes(jnp.sum(line, axis=0, keepdims=True))
    clear_stage(aux[0:n_blk, :], stage, n_proj)
    pack_return(acc, (line,), stage, out)


def update_kernel(after, steps, res, dirn, image, precond, res_out, dir_out):
    del after
    alpha, beta = steps[0:1, :], steps[1:2, :]
    for h in range(res.shape[1] // LANES):
        cols = slice(h * LANES, (h + 1) * LANES)
        new_res = res[:, cols] - alpha * image[:, cols]
        res_out[:, cols] = new_res
        dir_out[:, cols] = precond[:, cols] * new_res + beta * dirn[:, cols]


def sum_kernel(first, recv, *rest):
    if first:
        out, ids_out, right, turned, fine, left = rest
    else:
        right, out, turned, fine, left = rest
    n_x = recv.shape[1]
    n_blk = LANES // ROWS
    n_proj = 9
    sub = lax.broadcasted_iota(jnp.int32, (n_blk, LANES), 0)
    deep = lax.broadcasted_iota(jnp.int32, (LANES, LANES), 0).astype(BF16)
    half = n_proj * 8

    def spread(table, x, base, high):
        lines = [
            jnp.broadcast_to(table[x, base + k : base + k + 1, :], (8, LANES))
            for k in range(n_proj)
        ]
        return jnp.concatenate([jnp.where(high, line, 0.0) for line in lines], axis=0)

    for x in range(n_x):
        values = recv[:, x].reshape(LANES, LANES).T
        turned[x] = values
        fine[x] = values - values.astype(BF16).astype(F32)
        for b in range(n_blk):
            at = (x * n_blk + b) * LANES
            cols = slice(at, at + LANES)
            base = b * ROWS
            ids = turned[x, base + n_proj : base + n_proj + 1, :].astype(jnp.int32)
            high = jnp.broadcast_to(ids >> 7, (8, LANES)) == sub
            left[0:half, cols] = spread(turned, x, base, high).astype(BF16)
            left[80 : 80 + half, cols] = spread(fine, x, base, high).astype(BF16)
            if first:
                low = jnp.broadcast_to((ids & 127).astype(BF16), (LANES, LANES)) == deep
                right[:, cols] = jnp.where(low, jnp.ones_like(deep), jnp.zeros_like(deep))
    summed = lax.dot_general(left[...], right[...], NT, preferred_element_type=F32)
    out[0:half, :] = summed[0:half] + summed[80 : 80 + half]
    per = recv.shape[2]
    mixed = jnp.zeros((1, LANES), F32)
    for x in range(n_x):
        mixed += turned[x, n_proj + 1 : n_proj + 2, :]
    out[half : half + 1, :] = over_lanes(mixed) * (1.0 / per)
    out[half + 1 : half + 8, :] = jnp.zeros((7, LANES), F32)
    if first:
        ids_out[...] = turned[lax.axis_index("x"), pl.ds(n_proj, n_blk, stride=ROWS), :].astype(jnp.int32)


def lifted(proj, weights, h):
    cols = slice(h * LANES, (h + 1) * LANES)
    n_proj, n_par, _ = proj.shape
    acc = jnp.zeros((n_par, LANES), F32)
    for k in range(n_proj):
        line = weights[k * 8 + h : k * 8 + h + 1, :]
        acc += proj[k, :, cols].astype(F32) * jnp.broadcast_to(line, (n_par, LANES))
    return acc


def projected(proj, field, h, table):
    cols = slice(h * LANES, (h + 1) * LANES)
    for k in range(proj.shape[0]):
        table[k * 8 + h : k * 8 + h + 1, :] = jnp.sum(
            proj[k, :, cols].astype(F32) * field, axis=0, keepdims=True
        )


def pairs(n_proj):
    return [(k, m) for k in range(n_proj) for m in range(k, n_proj)]


def form_kernel(after, proj, precond, out):
    del after
    n_proj = proj.shape[0]
    for h in range(precond.shape[1] // LANES):
        cols = slice(h * LANES, (h + 1) * LANES)
        tiles = [proj[k, :, cols].astype(F32) for k in range(n_proj)]
        scaled = [tile * precond[:, cols] for tile in tiles]
        for i, (k, m) in enumerate(pairs(n_proj)):
            out[i * 8 + h : i * 8 + h + 1, :] = jnp.sum(
                scaled[k] * tiles[m], axis=0, keepdims=True
            )


def blended(matrix, weights):
    n_proj = 9
    sums = [None] * n_proj

    def add(k, tile, m):
        term = tile * weights[m * 8 : m * 8 + 8, :]
        sums[k] = term if sums[k] is None else sums[k] + term

    for i, (k, m) in enumerate(pairs(n_proj)):
        tile = matrix[i * 8 : i * 8 + 8, :]
        add(k, tile, m)
        if k != m:
            add(m, tile, k)
    return sums


def lane_pick(table, low):
    return jnp.take_along_axis(table, low, axis=1, mode="promise_in_bounds")


def send_picks(table, ids, scalars, stage, out):
    n_blk = ids.shape[0]
    n_chunk = 8
    stage[...] = jnp.zeros_like(stage)
    index = ids[...]
    low = index & 127
    high = index >> 7
    for b in range(n_blk):
        low_b = jnp.broadcast_to(low[b : b + 1, :], (8, LANES))
        high_b = jnp.broadcast_to(high[b : b + 1, :], (8, LANES))
        got = jnp.zeros((8, LANES), F32)
        for h in range(n_chunk):
            piece = lane_pick(table[pl.ds(h, 8, stride=8), :], low_b)
            got = jnp.where(high_b == h, piece, got)
        stage[b * ROWS : b * ROWS + 8, :] = got
    got = jnp.zeros((n_blk, LANES), F32)
    for h in range(n_chunk):
        line = jnp.broadcast_to(table[64 + h : 65 + h, :], (n_blk, LANES))
        got = jnp.where(high == h, lane_pick(line, low), got)
    stage[pl.ds(8, n_blk, stride=ROWS), :] = got
    at = 10
    for rows in scalars:
        stage[at : at + rows.shape[0], :] = rows
        at += rows.shape[0]
    out[...] = stage[...].T.reshape(out.shape)


def start_kernel(own, partner, matrix, ids, out, weights, table, stage):
    weights[...] = own[...] + partner[...]
    for k, tile in enumerate(blended(matrix, weights)):
        table[k * 8 : k * 8 + 8, :] = -tile
    send_picks(table, ids, (), stage, out)


def state_kernel(
    after, own, partner, proj, precond, damping, res_out, dir_out, cross, rz_out, weights
):
    del after
    weights[...] = own[...] + partner[...]
    n_par, width = precond.shape
    rz = jnp.zeros((n_par, LANES), F32)
    for h in range(width // LANES):
        cols = slice(h * LANES, (h + 1) * LANES)
        res = -lifted(proj, weights, h)
        dirn = precond[:, cols] * res
        res_out[:, cols] = res
        dir_out[:, cols] = dirn
        rz += res * dirn
        projected(proj, precond[:, cols] * damping[:, cols] * dirn, h, cross)
    rz_out[...] = jnp.full(rz_out.shape, jnp.sum(rz), F32)


def step_kernel(
    own, partner, proj, precond, damping, matrix, cross, rz_in, ids, dirn,
    out, image_out, weights, table, stage,
):
    weights[...] = own[...] + partner[...]
    n_par, width = precond.shape
    for k, tile in enumerate(blended(matrix, weights)):
        table[k * 8 : k * 8 + 8, :] = tile + cross[k * 8 : k * 8 + 8, :]
    curve, square, damped, mixed, scaled = [jnp.zeros((n_par, LANES), F32)] * 5
    for h in range(width // LANES):
        cols = slice(h * LANES, (h + 1) * LANES)
        pull = damping[:, cols] * dirn[:, cols]
        image = lifted(proj, weights, h) + pull
        image_out[:, cols] = image
        change = precond[:, cols] * image
        curve += dirn[:, cols] * image
        square += change * image
        damped += pull * dirn[:, cols]
        mixed += pull * change
        scaled += damping[:, cols] * change * change
    lines = [jnp.sum(each, axis=0, keepdims=True) for each in (curve, square, damped, mixed, scaled)]
    send_picks(table, ids, (rz_in[0:1, :], over_lanes(jnp.concatenate(lines, axis=0))), stage, out)


def last_kernel(
    own, partner, proj, damping, steps, first_dir, res, dirn,
    sol_hbm, res_hbm, weights, sol_out, res_out, sem,
):
    weights[...] = own[...] + partner[...]
    rows = proj.shape[0] * 8
    curve = weights[rows : rows + 1, :] + steps[3:4, :]
    alpha = steps[2:3, :] / curve
    alpha_first = steps[0:1, :]
    chunks = damping.shape[1] // LANES
    copies = []

    def send(here, there, first, last):
        cols = pl.ds(first * LANES, (last - first) * LANES)
        copy = pltpu.make_async_copy(here.at[:, cols], there.at[:, cols], sem.at[len(copies)])
        copy.start()
        copies.append(copy)

    for h in range(chunks):
        cols = slice(h * LANES, (h + 1) * LANES)
        sol_out[:, cols] = alpha_first * first_dir[:, cols] + alpha * dirn[:, cols]
    for h in range(chunks):
        cols = slice(h * LANES, (h + 1) * LANES)
        image = lifted(proj, weights, h) + damping[:, cols] * dirn[:, cols]
        res_out[:, cols] = res[:, cols] - alpha * image
        if h == 0:
            send(sol_out, sol_hbm, 0, chunks)
        else:
            send(res_out, res_hbm, h - 1, h)
    send(res_out, res_hbm, chunks - 1, chunks)
    for copy in copies:
        copy.wait()


def local(jacobian, splat_ids, pix_residual, live_blocks, proj_jac, damping, precond):
    n_blk, n_pix, n_col = jacobian.shape
    n_par, g_dev = damping.shape
    n_scene, n_x = lax.axis_size("scene"), lax.axis_size("x")
    per = LANES // n_scene
    msg = f32(n_scene, per, LANES)
    wide = f32(n_scene, n_x, per, LANES)
    sums = f32(80, LANES)
    state = f32(n_par, g_dev)
    square = pltpu.VMEM((LANES, LANES), F32)
    whole = jax.ShapeDtypeStruct
    weights = pltpu.VMEM((80, LANES), F32)
    table = pltpu.VMEM((72, LANES), F32)

    def to_owners(message, right):
        flat = message.reshape(n_scene * n_x, per, LANES)
        got = lax.all_to_all(flat, ("scene", "x"), 0, 0, tiled=True)
        first = right is None
        wide_k = n_x * n_blk * LANES
        extra = (whole((n_blk, LANES), jnp.int32), whole((LANES, wide_k), BF16))
        own, *kept = call(
            functools.partial(sum_kernel, first),
            (sums,) + (extra if first else ()),
            [VMEM] * (1 if first else 2),
            [
                pltpu.VMEM((n_x, LANES, LANES), F32),
                pltpu.VMEM((n_x, LANES, LANES), F32),
                pltpu.VMEM((160, wide_k), BF16),
            ],
            1 << 31,
        )(got.reshape(n_scene, n_x, per, LANES), *(() if first else (right,)))
        partner = lax.ppermute(own, "core", [(0, 1), (1, 0)])
        return own, partner, *kept

    def to_blocks(message):
        return lax.all_to_all(message, "scene", 0, 0, tiled=True)

    message, jac, aux = call(
        rhs_kernel,
        (wide, whole(jacobian.shape, BF16), whole((2 * n_blk, LANES), jnp.int32)),
        [HBM] * 4,
        [
            pltpu.VMEM((n_blk, n_pix), BF16),
            pltpu.VMEM((1, live_blocks.shape[0]), jnp.int32),
            pltpu.VMEM((n_blk, LANES), jnp.int32),
            square,
            pltpu.SemaphoreType.DMA((n_blk,)),
            pltpu.SemaphoreType.DMA((3,)),
        ],
    )(*map(in_hbm, (live_blocks.reshape(1, -1), jacobian, pix_residual, splat_ids)))
    own, partner, index, right = to_owners(message, None)
    matrix = call(form_kernel, (f32(45 * 8, LANES),), [VMEM] * 3, (), 1 << 31)(
        own, proj_jac, precond
    )[0]
    message = call(start_kernel, (msg,), [VMEM] * 4, [weights, table, square])(
        own, partner, matrix, index
    )[0]
    first_own, first_partner = own, partner
    arrived = to_blocks(message)
    message, picks = call(
        first_kernel,
        (wide, f32(n_blk, n_col)),
        [VMEM] * 3,
        [square, square],
    )(jac, aux, arrived)
    own, partner = to_owners(message, right)
    res, first_dir, cross, rz = call(
        state_kernel, (state, state, f32(72, LANES), f32(8, LANES)), [VMEM] * 6, [weights], 1 << 31
    )(own, first_own, first_partner, proj_jac, precond, damping)
    message, image = call(step_kernel, (msg, state), [VMEM] * 10, [weights, table, square])(
        own, partner, proj_jac, precond, damping, matrix, cross, rz, index, first_dir
    )
    arrived = to_blocks(message)
    message, steps = call(
        second_kernel, (wide, f32(8, LANES)), [VMEM] * 4, [square, square]
    )(jac, aux, arrived, picks)
    own, partner = to_owners(message, right)
    res, second_dir = call(update_kernel, (state, state), [VMEM] * 6, (), 1 << 31)(
        own, steps, res, first_dir, image, precond
    )
    held = pltpu.VMEM((n_par, g_dev), F32)
    return call(
        last_kernel,
        (state, state),
        [VMEM] * 8,
        [weights, held, held, pltpu.SemaphoreType.DMA((1 + g_dev // LANES,))],
        out_space=HBM,
    )(
        own, partner, proj_jac, damping, steps, first_dir, res, second_dir
    )


def solution(mesh):
    scene = mesh.shape["scene"]
    finer = Mesh(mesh.devices.reshape(scene, -1, 2), ("scene", "x", "core"))
    everywhere = ("scene", "x", "core")
    in_specs = (
        P(everywhere, None, None),
        P(everywhere, None),
        P(everywhere, None),
        P(),
        P(None, None, "scene"),
        P(None, "scene"),
        P(None, "scene"),
    )
    out_specs = (P(None, "scene"), P(None, "scene"))
    return jax.shard_map(local, mesh=finer, in_specs=in_specs, out_specs=out_specs, check_vma=False)
```

```python
import functools

import jax
import jax.numpy as jnp
from jax import lax
from jax.experimental import pallas as pl
from jax.experimental.pallas import tpu as pltpu
from jax.sharding import Mesh
from jax.sharding import PartitionSpec as P

F32 = jnp.float32
BF16 = jnp.bfloat16
LANES = 128
ROWS = 16
VMEM = pl.BlockSpec(memory_space=pltpu.VMEM)
HBM = pl.BlockSpec(memory_space=pltpu.HBM)
NT = (((1,), (1,)), ((), ()))


def call(kernel, out, in_specs, scratch=(), flops=1 << 20, out_space=VMEM):
    return pl.pallas_call(
        kernel,
        out_shape=out,
        in_specs=in_specs,
        out_specs=jax.tree.map(lambda _: out_space, out),
        scratch_shapes=scratch,
        compiler_params=pltpu.CompilerParams(vmem_limit_bytes=24 << 20),
        cost_estimate=pl.CostEstimate(flops=flops, bytes_accessed=1 << 20, transcendentals=0),
    )


def in_hbm(array):
    return pltpu.with_memory_space_constraint(array, pltpu.HBM)


def f32(*shape):
    return jax.ShapeDtypeStruct(shape, F32)


def clear_stage(ids, stage, n_proj):
    stage[...] = jnp.zeros_like(stage)
    stage[pl.ds(n_proj, ids.shape[0], stride=ROWS), :] = ids.astype(F32)


def pack_return(acc, scalars, stage, out):
    n_blk = acc.shape[0]
    n_proj = acc.shape[1] // LANES
    for k in range(n_proj):
        stage[pl.ds(k, n_blk, stride=ROWS), :] = acc[:, k * LANES : (k + 1) * LANES]
    for i, value in enumerate(scalars):
        stage[n_proj + 1 + i : n_proj + 2 + i, :] = value
    turned = stage[...].T.reshape(out.shape[0], *out.shape[2:])
    for x in range(out.shape[1]):
        out[:, x] = turned


def rhs_kernel(live, jac, pix, ids, out, jbuf, aux, pixels, lives, index, stage, sem, small):
    n_blk = jac.shape[0]
    minor = [
        pltpu.make_async_copy(pix, pixels, small.at[0]),
        pltpu.make_async_copy(live, lives, small.at[1]),
        pltpu.make_async_copy(ids, index, small.at[2]),
    ]
    copies = [pltpu.make_async_copy(jac.at[b], jbuf.at[b], sem.at[b]) for b in range(n_blk)]
    for copy in minor + copies:
        copy.start()
    for copy in minor:
        copy.wait()
    n_x, n_core = lax.axis_size("x"), lax.axis_size("core")
    position = (lax.axis_index("scene") * n_x + lax.axis_index("x")) * n_core
    position = position + lax.axis_index("core")
    lane = lax.broadcasted_iota(jnp.int32, lives.shape, 1)
    own = jnp.sum(jnp.where(lane == position, lives[...], 0), axis=1, keepdims=True)
    local_ids = index[...] & (LANES * 8 - 1)
    aux[0:n_blk, :] = local_ids
    aux[n_blk : 2 * n_blk, :] = jnp.broadcast_to(own, (n_blk, LANES))
    clear_stage(local_ids, stage, jac.shape[2] // LANES)
    row = lax.broadcasted_iota(jnp.int32, pix.shape, 0)
    keep = row < jnp.broadcast_to(own, pix.shape)
    values = jnp.where(keep, pixels[...].astype(F32), 0.0)
    n_pix, n_col = jac.shape[1:]
    acc = jnp.zeros((n_blk, n_col), F32)
    cut = n_blk * 3 // 4
    for first, last in ((0, cut), (cut, n_blk)):
        signals = [jnp.where(row == b, values, 0.0).astype(BF16) for b in range(first, last)]
        for copy in copies[first:last]:
            copy.wait()
        stacked = jbuf[first:last].reshape((last - first) * n_pix, n_col)
        acc += jnp.dot(jnp.concatenate(signals, axis=1), stacked, preferred_element_type=F32)
    pack_return(acc, (), stage, out)


def lane_image(jac, b, line, ones):
    pieces = []
    for top in range(0, jac.shape[1], 64):
        folded = jnp.zeros((64, LANES), F32)
        for at in range(0, jac.shape[2], LANES):
            tile = jac[b, top : top + 64, at : at + LANES].astype(F32)
            folded += tile * line[:, at : at + LANES]
        high = folded.astype(BF16)
        pieces.append(jnp.concatenate([high, (folded - high.astype(F32)).astype(BF16)], axis=1))
    return lax.dot_general(
        ones, jnp.concatenate(pieces, axis=0), NT, preferred_element_type=F32
    )


def block_pass(picks, aux, jac, by_lanes):
    n_blk, n_pix = jac.shape[:2]
    row = lax.broadcasted_iota(jnp.int32, (n_blk, n_pix), 0)
    live = row < aux[n_blk : n_blk + 1, 0:1]
    chosen = picks.astype(BF16)
    rounded = chosen.astype(F32)
    ones = jnp.ones((n_blk, 2 * LANES), BF16)
    signals = []
    for b in range(n_blk):
        if (b * by_lanes) // n_blk != ((b + 1) * by_lanes) // n_blk:
            image = lane_image(jac, b, rounded[b : b + 1, :], ones)
        else:
            image = lax.dot_general(chosen, jac[b], NT, preferred_element_type=F32)
        signals.append(jnp.where((row == b) & live, image, 0.0).astype(BF16))
    stacked = jac[...].reshape(n_blk * n_pix, jac.shape[2])
    return jnp.dot(jnp.concatenate(signals, axis=1), stacked, preferred_element_type=F32)


def unpack_picks(recv, turned, n_blk, n_proj):
    turned[...] = recv[...].reshape(LANES, LANES).T
    return jnp.concatenate(
        [turned[pl.ds(k, n_blk, stride=ROWS), :] for k in range(n_proj)], axis=1
    )


def over_lanes(rows):
    return jnp.broadcast_to(jnp.sum(rows, axis=1, keepdims=True), rows.shape)


def first_kernel(jac, aux, recv, out, picks_out, turned, stage):
    n_blk = jac.shape[0]
    n_proj = jac.shape[2] // LANES
    picks = unpack_picks(recv, turned, n_blk, n_proj)
    picks_out[...] = picks
    acc = block_pass(picks, aux, jac, 5)
    clear_stage(aux[0:n_blk, :], stage, n_proj)
    pack_return(acc, (), stage, out)


def second_kernel(jac, aux, recv, picks_in, out, steps_out, turned, stage):
    n_blk = jac.shape[0]
    n_proj = jac.shape[2] // LANES
    fresh = unpack_picks(recv, turned, n_blk, n_proj)
    per = recv.shape[1]
    totals = over_lanes(turned[8:16, :]) * (1.0 / per)
    rz, damped, curve, square, mixed, scaled = (totals[i : i + 1, :] for i in range(2, 8))
    alpha = rz / curve
    after = rz - 2.0 * alpha * curve + alpha * alpha * square
    beta = after / rz
    grown = 1.0 + beta
    steps_out[0:1, :] = alpha
    steps_out[1:2, :] = beta
    steps_out[2:3, :] = after
    steps_out[3:4, :] = (
        grown * grown * damped - 2.0 * grown * alpha * mixed + alpha * alpha * scaled
    )
    steps_out[4:8, :] = jnp.zeros((4, LANES), F32)
    pieces = []
    for k in range(n_proj):
        cols = slice(k * LANES, (k + 1) * LANES)
        pieces.append(grown * picks_in[:, cols] - alpha * fresh[:, cols])
    picks = jnp.concatenate(pieces, axis=1)
    acc = block_pass(picks, aux, jac, 5)
    weighed = picks * acc
    line = jnp.zeros((n_blk, LANES), F32)
    for k in range(n_proj):
        line += weighed[:, k * LANES : (k + 1) * LANES]
    line = over_lanes(jnp.sum(line, axis=0, keepdims=True))
    clear_stage(aux[0:n_blk, :], stage, n_proj)
    pack_return(acc, (line,), stage, out)


def update_kernel(after, steps, res, dirn, image, precond, res_out, dir_out):
    del after
    alpha, beta = steps[0:1, :], steps[1:2, :]
    for h in range(res.shape[1] // LANES):
        cols = slice(h * LANES, (h + 1) * LANES)
        new_res = res[:, cols] - alpha * image[:, cols]
        res_out[:, cols] = new_res
        dir_out[:, cols] = precond[:, cols] * new_res + beta * dirn[:, cols]


def sum_kernel(first, recv, *rest):
    if first:
        out, ids_out, right, turned, fine, left = rest
    else:
        right, out, turned, fine, left = rest
    n_x = recv.shape[1]
    n_blk = LANES // ROWS
    n_proj = 9
    sub = lax.broadcasted_iota(jnp.int32, (n_blk, LANES), 0)
    deep = lax.broadcasted_iota(jnp.int32, (LANES, LANES), 0).astype(BF16)
    half = n_proj * 8

    def spread(table, x, base, high):
        lines = [
            jnp.broadcast_to(table[x, base + k : base + k + 1, :], (8, LANES))
            for k in range(n_proj)
        ]
        return jnp.concatenate([jnp.where(high, line, 0.0) for line in lines], axis=0)

    for x in range(n_x):
        values = recv[:, x].reshape(LANES, LANES).T
        turned[x] = values
        fine[x] = values - values.astype(BF16).astype(F32)
        for b in range(n_blk):
            at = (x * n_blk + b) * LANES
            cols = slice(at, at + LANES)
            base = b * ROWS
            ids = turned[x, base + n_proj : base + n_proj + 1, :].astype(jnp.int32)
            high = jnp.broadcast_to(ids >> 7, (8, LANES)) == sub
            left[0:half, cols] = spread(turned, x, base, high).astype(BF16)
            left[80 : 80 + half, cols] = spread(fine, x, base, high).astype(BF16)
            if first:
                low = jnp.broadcast_to((ids & 127).astype(BF16), (LANES, LANES)) == deep
                right[:, cols] = jnp.where(low, jnp.ones_like(deep), jnp.zeros_like(deep))
    summed = lax.dot_general(left[...], right[...], NT, preferred_element_type=F32)
    out[0:half, :] = summed[0:half] + summed[80 : 80 + half]
    per = recv.shape[2]
    mixed = jnp.zeros((1, LANES), F32)
    for x in range(n_x):
        mixed += turned[x, n_proj + 1 : n_proj + 2, :]
    out[half : half + 1, :] = over_lanes(mixed) * (1.0 / per)
    out[half + 1 : half + 8, :] = jnp.zeros((7, LANES), F32)
    if first:
        ids_out[...] = turned[lax.axis_index("x"), pl.ds(n_proj, n_blk, stride=ROWS), :].astype(jnp.int32)


def lifted(proj, weights, h):
    cols = slice(h * LANES, (h + 1) * LANES)
    n_proj, n_par, _ = proj.shape
    acc = jnp.zeros((n_par, LANES), F32)
    for k in range(n_proj):
        line = weights[k * 8 + h : k * 8 + h + 1, :]
        acc += proj[k, :, cols].astype(F32) * jnp.broadcast_to(line, (n_par, LANES))
    return acc


def projected(proj, field, h, table):
    cols = slice(h * LANES, (h + 1) * LANES)
    for k in range(proj.shape[0]):
        table[k * 8 + h : k * 8 + h + 1, :] = jnp.sum(
            proj[k, :, cols].astype(F32) * field, axis=0, keepdims=True
        )


def pairs(n_proj):
    return [(k, m) for k in range(n_proj) for m in range(k, n_proj)]


def form_kernel(after, proj, precond, out):
    del after
    n_proj = proj.shape[0]
    for h in range(precond.shape[1] // LANES):
        cols = slice(h * LANES, (h + 1) * LANES)
        tiles = [proj[k, :, cols].astype(F32) for k in range(n_proj)]
        scaled = [tile * precond[:, cols] for tile in tiles]
        for i, (k, m) in enumerate(pairs(n_proj)):
            out[i * 8 + h : i * 8 + h + 1, :] = jnp.sum(
                scaled[k] * tiles[m], axis=0, keepdims=True
            )


def blended(matrix, weights):
    n_proj = 9
    sums = [None] * n_proj

    def add(k, tile, m):
        term = tile * weights[m * 8 : m * 8 + 8, :]
        sums[k] = term if sums[k] is None else sums[k] + term

    for i, (k, m) in enumerate(pairs(n_proj)):
        tile = matrix[i * 8 : i * 8 + 8, :]
        add(k, tile, m)
        if k != m:
            add(m, tile, k)
    return sums


def lane_pick(table, low):
    return jnp.take_along_axis(table, low, axis=1, mode="promise_in_bounds")


def send_picks(table, ids, scalars, stage, out):
    n_blk = ids.shape[0]
    n_chunk = 8
    stage[...] = jnp.zeros_like(stage)
    index = ids[...]
    low = index & 127
    high = index >> 7
    for b in range(n_blk):
        low_b = jnp.broadcast_to(low[b : b + 1, :], (8, LANES))
        high_b = jnp.broadcast_to(high[b : b + 1, :], (8, LANES))
        got = jnp.zeros((8, LANES), F32)
        for h in range(n_chunk):
            piece = lane_pick(table[pl.ds(h, 8, stride=8), :], low_b)
            got = jnp.where(high_b == h, piece, got)
        stage[b * ROWS : b * ROWS + 8, :] = got
    got = jnp.zeros((n_blk, LANES), F32)
    for h in range(n_chunk):
        line = jnp.broadcast_to(table[64 + h : 65 + h, :], (n_blk, LANES))
        got = jnp.where(high == h, lane_pick(line, low), got)
    stage[pl.ds(8, n_blk, stride=ROWS), :] = got
    at = 10
    for rows in scalars:
        stage[at : at + rows.shape[0], :] = rows
        at += rows.shape[0]
    out[...] = stage[...].T.reshape(out.shape)


def start_kernel(own, partner, matrix, ids, out, weights, table, stage):
    weights[...] = own[...] + partner[...]
    for k, tile in enumerate(blended(matrix, weights)):
        table[k * 8 : k * 8 + 8, :] = -tile
    send_picks(table, ids, (), stage, out)


def state_kernel(
    after, own, partner, proj, precond, damping,
    res_out, dir_out, cross, rz_out, wide_proj, weights,
):
    del after
    weights[...] = own[...] + partner[...]
    n_par, width = precond.shape
    rz, damped = jnp.zeros((n_par, LANES), F32), jnp.zeros((n_par, LANES), F32)
    for h in range(width // LANES):
        cols = slice(h * LANES, (h + 1) * LANES)
        for k in range(proj.shape[0]):
            wide_proj[k, :, cols] = proj[k, :, cols].astype(F32)
        res = -lifted(proj, weights, h)
        dirn = precond[:, cols] * res
        res_out[:, cols] = res
        dir_out[:, cols] = dirn
        rz += res * dirn
        pull = damping[:, cols] * dirn
        damped += pull * dirn
        projected(proj, precond[:, cols] * pull, h, cross)
    rz_out[0:4, :] = jnp.full((4, LANES), jnp.sum(rz), F32)
    rz_out[4:8, :] = jnp.full((4, LANES), jnp.sum(damped), F32)


def step_kernel(
    own, partner, proj, precond, damping, matrix, cross, rz_in, ids, dirn,
    out, image_out, weights, table, stage,
):
    weights[...] = own[...] + partner[...]
    n_par, width = precond.shape
    for k, tile in enumerate(blended(matrix, weights)):
        table[k * 8 : k * 8 + 8, :] = tile + cross[k * 8 : k * 8 + 8, :]
    curve, square, mixed, scaled = [jnp.zeros((n_par, LANES), F32)] * 4
    for h in range(width // LANES):
        cols = slice(h * LANES, (h + 1) * LANES)
        pull = damping[:, cols] * dirn[:, cols]
        image = lifted(proj, weights, h) + pull
        image_out[:, cols] = image
        change = precond[:, cols] * image
        curve += dirn[:, cols] * image
        square += change * image
        mixed += pull * change
        scaled += damping[:, cols] * change * change
    lines = [jnp.sum(each, axis=0, keepdims=True) for each in (curve, square, mixed, scaled)]
    totals = over_lanes(jnp.concatenate(lines, axis=0))
    send_picks(table, ids, (rz_in[0:1, :], rz_in[4:5, :], totals), stage, out)


def last_kernel(
    own, partner, proj, damping, steps, first_dir, res, dirn,
    sol_hbm, res_hbm, weights, sol_out, res_out, sem,
):
    weights[...] = own[...] + partner[...]
    rows = proj.shape[0] * 8
    curve = weights[rows : rows + 1, :] + steps[3:4, :]
    alpha = steps[2:3, :] / curve
    alpha_first = steps[0:1, :]
    chunks = damping.shape[1] // LANES
    copies = []

    def send(here, there, first, last):
        cols = pl.ds(first * LANES, (last - first) * LANES)
        copy = pltpu.make_async_copy(here.at[:, cols], there.at[:, cols], sem.at[len(copies)])
        copy.start()
        copies.append(copy)

    for h in range(chunks):
        cols = slice(h * LANES, (h + 1) * LANES)
        sol_out[:, cols] = alpha_first * first_dir[:, cols] + alpha * dirn[:, cols]
    for h in range(chunks):
        cols = slice(h * LANES, (h + 1) * LANES)
        image = lifted(proj, weights, h) + damping[:, cols] * dirn[:, cols]
        res_out[:, cols] = res[:, cols] - alpha * image
        if h == 0:
            send(sol_out, sol_hbm, 0, chunks)
        elif h % 2 == 0:
            send(res_out, res_hbm, h - 2, h)
    send(res_out, res_hbm, chunks - 2, chunks)
    for copy in copies:
        copy.wait()


def local(jacobian, splat_ids, pix_residual, live_blocks, proj_jac, damping, precond):
    n_blk, n_pix, n_col = jacobian.shape
    n_par, g_dev = damping.shape
    n_scene, n_x = lax.axis_size("scene"), lax.axis_size("x")
    per = LANES // n_scene
    msg = f32(n_scene, per, LANES)
    wide = f32(n_scene, n_x, per, LANES)
    sums = f32(80, LANES)
    state = f32(n_par, g_dev)
    square = pltpu.VMEM((LANES, LANES), F32)
    whole = jax.ShapeDtypeStruct
    weights = pltpu.VMEM((80, LANES), F32)
    table = pltpu.VMEM((72, LANES), F32)

    def to_owners(message, right):
        flat = message.reshape(n_scene * n_x, per, LANES)
        got = lax.all_to_all(flat, ("scene", "x"), 0, 0, tiled=True)
        first = right is None
        wide_k = n_x * n_blk * LANES
        extra = (whole((n_blk, LANES), jnp.int32), whole((LANES, wide_k), BF16))
        own, *kept = call(
            functools.partial(sum_kernel, first),
            (sums,) + (extra if first else ()),
            [VMEM] * (1 if first else 2),
            [
                pltpu.VMEM((n_x, LANES, LANES), F32),
                pltpu.VMEM((n_x, LANES, LANES), F32),
                pltpu.VMEM((160, wide_k), BF16),
            ],
            1 << 31,
        )(got.reshape(n_scene, n_x, per, LANES), *(() if first else (right,)))
        partner = lax.ppermute(own, "core", [(0, 1), (1, 0)])
        return own, partner, *kept

    def to_blocks(message):
        return lax.all_to_all(message, "scene", 0, 0, tiled=True)

    message, jac, aux = call(
        rhs_kernel,
        (wide, whole(jacobian.shape, BF16), whole((2 * n_blk, LANES), jnp.int32)),
        [HBM] * 4,
        [
            pltpu.VMEM((n_blk, n_pix), BF16),
            pltpu.VMEM((1, live_blocks.shape[0]), jnp.int32),
            pltpu.VMEM((n_blk, LANES), jnp.int32),
            square,
            pltpu.SemaphoreType.DMA((n_blk,)),
            pltpu.SemaphoreType.DMA((3,)),
        ],
    )(*map(in_hbm, (live_blocks.reshape(1, -1), jacobian, pix_residual, splat_ids)))
    own, partner, index, right = to_owners(message, None)
    matrix = call(form_kernel, (f32(45 * 8, LANES),), [VMEM] * 3, (), 1 << 31)(
        own, proj_jac, precond
    )[0]
    message = call(start_kernel, (msg,), [VMEM] * 4, [weights, table, square])(
        own, partner, matrix, index
    )[0]
    first_own, first_partner = own, partner
    arrived = to_blocks(message)
    message, picks = call(
        first_kernel,
        (wide, f32(n_blk, n_col)),
        [VMEM] * 3,
        [square, square],
    )(jac, aux, arrived)
    own, partner = to_owners(message, right)
    res, first_dir, cross, rz, wide_proj = call(
        state_kernel,
        (state, state, f32(72, LANES), f32(8, LANES), f32(*proj_jac.shape)),
        [VMEM] * 6,
        [weights],
        1 << 31,
    )(own, first_own, first_partner, proj_jac, precond, damping)
    message, image = call(step_kernel, (msg, state), [VMEM] * 10, [weights, table, square])(
        own, partner, wide_proj, precond, damping, matrix, cross, rz, index, first_dir
    )
    arrived = to_blocks(message)
    message, steps = call(
        second_kernel, (wide, f32(8, LANES)), [VMEM] * 4, [square, square]
    )(jac, aux, arrived, picks)
    own, partner = to_owners(message, right)
    res, second_dir = call(update_kernel, (state, state), [VMEM] * 6, (), 1 << 31)(
        own, steps, res, first_dir, image, precond
    )
    held = pltpu.VMEM((n_par, g_dev), F32)
    return call(
        last_kernel,
        (state, state),
        [VMEM] * 8,
        [weights, held, held, pltpu.SemaphoreType.DMA((1 + g_dev // (2 * LANES),))],
        out_space=HBM,
    )(
        own, partner, wide_proj, damping, steps, first_dir, res, second_dir
    )


def solution(mesh):
    scene = mesh.shape["scene"]
    finer = Mesh(mesh.devices.reshape(scene, -1, 2), ("scene", "x", "core"))
    everywhere = ("scene", "x", "core")
    in_specs = (
        P(everywhere, None, None),
        P(everywhere, None),
        P(everywhere, None),
        P(),
        P(None, None, "scene"),
        P(None, "scene"),
        P(None, "scene"),
    )
    out_specs = (P(None, "scene"), P(None, "scene"))
    return jax.shard_map(local, mesh=finer, in_specs=in_specs, out_specs=out_specs, check_vma=False)
```

```python
import functools

import jax
import jax.numpy as jnp
from jax import lax
from jax.experimental import pallas as pl
from jax.experimental.pallas import tpu as pltpu
from jax.sharding import Mesh
from jax.sharding import PartitionSpec as P

F32 = jnp.float32
BF16 = jnp.bfloat16
LANES = 128
ROWS = 16
VMEM = pl.BlockSpec(memory_space=pltpu.VMEM)
HBM = pl.BlockSpec(memory_space=pltpu.HBM)
NT = (((1,), (1,)), ((), ()))


def call(kernel, out, in_specs, scratch=(), flops=1 << 20, out_space=VMEM):
    return pl.pallas_call(
        kernel,
        out_shape=out,
        in_specs=in_specs,
        out_specs=jax.tree.map(lambda _: out_space, out),
        scratch_shapes=scratch,
        compiler_params=pltpu.CompilerParams(vmem_limit_bytes=24 << 20),
        cost_estimate=pl.CostEstimate(flops=flops, bytes_accessed=1 << 20, transcendentals=0),
    )


def in_hbm(array):
    return pltpu.with_memory_space_constraint(array, pltpu.HBM)


def f32(*shape):
    return jax.ShapeDtypeStruct(shape, F32)


def clear_stage(ids, stage, n_proj):
    stage[...] = jnp.zeros_like(stage)
    stage[pl.ds(n_proj, ids.shape[0], stride=ROWS), :] = ids.astype(F32)


def pack_return(acc, scalars, stage, out):
    n_blk = acc.shape[0]
    n_proj = acc.shape[1] // LANES
    for k in range(n_proj):
        stage[pl.ds(k, n_blk, stride=ROWS), :] = acc[:, k * LANES : (k + 1) * LANES]
    for i, value in enumerate(scalars):
        stage[n_proj + 1 + i : n_proj + 2 + i, :] = value
    turned = stage[...].T.reshape(out.shape[0], *out.shape[2:])
    for x in range(out.shape[1]):
        out[:, x] = turned


def rhs_kernel(live, jac, pix, ids, out, jbuf, aux, pixels, lives, index, stage, sem, small):
    n_blk = jac.shape[0]
    minor = [
        pltpu.make_async_copy(pix, pixels, small.at[0]),
        pltpu.make_async_copy(live, lives, small.at[1]),
        pltpu.make_async_copy(ids, index, small.at[2]),
    ]
    copies = [pltpu.make_async_copy(jac.at[b], jbuf.at[b], sem.at[b]) for b in range(n_blk)]
    for copy in minor + copies:
        copy.start()
    for copy in minor:
        copy.wait()
    n_x, n_core = lax.axis_size("x"), lax.axis_size("core")
    position = (lax.axis_index("scene") * n_x + lax.axis_index("x")) * n_core
    position = position + lax.axis_index("core")
    lane = lax.broadcasted_iota(jnp.int32, lives.shape, 1)
    own = jnp.sum(jnp.where(lane == position, lives[...], 0), axis=1, keepdims=True)
    local_ids = index[...] & (LANES * 8 - 1)
    aux[0:n_blk, :] = local_ids
    aux[n_blk : 2 * n_blk, :] = jnp.broadcast_to(own, (n_blk, LANES))
    clear_stage(local_ids, stage, jac.shape[2] // LANES)
    row = lax.broadcasted_iota(jnp.int32, pix.shape, 0)
    keep = row < jnp.broadcast_to(own, pix.shape)
    values = jnp.where(keep, pixels[...].astype(F32), 0.0)
    n_pix, n_col = jac.shape[1:]
    acc = jnp.zeros((n_blk, n_col), F32)
    cut = n_blk * 3 // 4
    for first, last in ((0, cut), (cut, n_blk)):
        signals = [jnp.where(row == b, values, 0.0).astype(BF16) for b in range(first, last)]
        for copy in copies[first:last]:
            copy.wait()
        stacked = jbuf[first:last].reshape((last - first) * n_pix, n_col)
        acc += jnp.dot(jnp.concatenate(signals, axis=1), stacked, preferred_element_type=F32)
    pack_return(acc, (), stage, out)


def lane_image(jac, b, line, ones):
    pieces = []
    for top in range(0, jac.shape[1], 64):
        folded = jnp.zeros((64, LANES), F32)
        for at in range(0, jac.shape[2], LANES):
            tile = jac[b, top : top + 64, at : at + LANES].astype(F32)
            folded += tile * line[:, at : at + LANES]
        high = folded.astype(BF16)
        pieces.append(jnp.concatenate([high, (folded - high.astype(F32)).astype(BF16)], axis=1))
    return lax.dot_general(
        ones, jnp.concatenate(pieces, axis=0), NT, preferred_element_type=F32
    )


def block_pass(picks, aux, jac, by_lanes):
    n_blk, n_pix = jac.shape[:2]
    row = lax.broadcasted_iota(jnp.int32, (n_blk, n_pix), 0)
    live = row < aux[n_blk : n_blk + 1, 0:1]
    chosen = picks.astype(BF16)
    rounded = chosen.astype(F32)
    ones = jnp.ones((n_blk, 2 * LANES), BF16)
    signals = []
    for b in range(n_blk):
        if (b * by_lanes) // n_blk != ((b + 1) * by_lanes) // n_blk:
            image = lane_image(jac, b, rounded[b : b + 1, :], ones)
        else:
            image = lax.dot_general(chosen, jac[b], NT, preferred_element_type=F32)
        signals.append(jnp.where((row == b) & live, image, 0.0).astype(BF16))
    stacked = jac[...].reshape(n_blk * n_pix, jac.shape[2])
    return jnp.dot(jnp.concatenate(signals, axis=1), stacked, preferred_element_type=F32)


def unpack_picks(recv, turned, n_blk, n_proj):
    turned[...] = recv[...].reshape(LANES, LANES).T
    return jnp.concatenate(
        [turned[pl.ds(k, n_blk, stride=ROWS), :] for k in range(n_proj)], axis=1
    )


def over_lanes(rows):
    return jnp.broadcast_to(jnp.sum(rows, axis=1, keepdims=True), rows.shape)


def first_kernel(jac, aux, recv, out, picks_out, turned, stage):
    n_blk = jac.shape[0]
    n_proj = jac.shape[2] // LANES
    picks = unpack_picks(recv, turned, n_blk, n_proj)
    picks_out[...] = picks
    acc = block_pass(picks, aux, jac, 5)
    clear_stage(aux[0:n_blk, :], stage, n_proj)
    pack_return(acc, (), stage, out)


def second_kernel(jac, aux, recv, picks_in, out, steps_out, turned, stage):
    n_blk = jac.shape[0]
    n_proj = jac.shape[2] // LANES
    fresh = unpack_picks(recv, turned, n_blk, n_proj)
    per = recv.shape[1]
    totals = over_lanes(turned[8:16, :]) * (1.0 / per)
    rz, curve, square, damped, mixed, scaled = (totals[i : i + 1, :] for i in range(2, 8))
    alpha = rz / curve
    after = rz - 2.0 * alpha * curve + alpha * alpha * square
    beta = after / rz
    grown = 1.0 + beta
    steps_out[0:1, :] = alpha
    steps_out[1:2, :] = beta
    steps_out[2:3, :] = after
    steps_out[3:4, :] = (
        grown * grown * damped - 2.0 * grown * alpha * mixed + alpha * alpha * scaled
    )
    steps_out[4:8, :] = jnp.zeros((4, LANES), F32)
    pieces = []
    for k in range(n_proj):
        cols = slice(k * LANES, (k + 1) * LANES)
        pieces.append(grown * picks_in[:, cols] - alpha * fresh[:, cols])
    picks = jnp.concatenate(pieces, axis=1)
    acc = block_pass(picks, aux, jac, 5)
    weighed = picks * acc
    line = jnp.zeros((n_blk, LANES), F32)
    for k in range(n_proj):
        line += weighed[:, k * LANES : (k + 1) * LANES]
    line = over_lanes(jnp.sum(line, axis=0, keepdims=True))
    clear_stage(aux[0:n_blk, :], stage, n_proj)
    pack_return(acc, (line,), stage, out)


def update_kernel(after, steps, res, dirn, image, precond, res_out, dir_out):
    del after
    alpha, beta = steps[0:1, :], steps[1:2, :]
    for h in range(res.shape[1] // LANES):
        cols = slice(h * LANES, (h + 1) * LANES)
        new_res = res[:, cols] - alpha * image[:, cols]
        res_out[:, cols] = new_res
        dir_out[:, cols] = precond[:, cols] * new_res + beta * dirn[:, cols]


def sum_kernel(first, recv, *rest):
    if first:
        out, ids_out, right, turned, fine, left = rest
    else:
        right, out, turned, fine, left = rest
    n_x = recv.shape[1]
    n_blk = LANES // ROWS
    n_proj = 9
    sub = lax.broadcasted_iota(jnp.int32, (n_blk, LANES), 0)
    deep = lax.broadcasted_iota(jnp.int32, (LANES, LANES), 0).astype(BF16)
    half = n_proj * 8

    def spread(table, x, base, high):
        lines = [
            jnp.broadcast_to(table[x, base + k : base + k + 1, :], (8, LANES))
            for k in range(n_proj)
        ]
        return jnp.concatenate([jnp.where(high, line, 0.0) for line in lines], axis=0)

    for x in range(n_x):
        values = recv[:, x].reshape(LANES, LANES).T
        turned[x] = values
        fine[x] = values - values.astype(BF16).astype(F32)
        for b in range(n_blk):
            at = (x * n_blk + b) * LANES
            cols = slice(at, at + LANES)
            base = b * ROWS
            ids = turned[x, base + n_proj : base + n_proj + 1, :].astype(jnp.int32)
            high = jnp.broadcast_to(ids >> 7, (8, LANES)) == sub
            left[0:half, cols] = spread(turned, x, base, high).astype(BF16)
            left[80 : 80 + half, cols] = spread(fine, x, base, high).astype(BF16)
            if first:
                low = jnp.broadcast_to((ids & 127).astype(BF16), (LANES, LANES)) == deep
                right[:, cols] = jnp.where(low, jnp.ones_like(deep), jnp.zeros_like(deep))
    summed = lax.dot_general(left[...], right[...], NT, preferred_element_type=F32)
    out[0:half, :] = summed[0:half] + summed[80 : 80 + half]
    per = recv.shape[2]
    mixed = jnp.zeros((1, LANES), F32)
    for x in range(n_x):
        mixed += turned[x, n_proj + 1 : n_proj + 2, :]
    out[half : half + 1, :] = over_lanes(mixed) * (1.0 / per)
    out[half + 1 : half + 8, :] = jnp.zeros((7, LANES), F32)
    if first:
        ids_out[...] = turned[lax.axis_index("x"), pl.ds(n_proj, n_blk, stride=ROWS), :].astype(jnp.int32)


def lifted(proj, weights, h):
    cols = slice(h * LANES, (h + 1) * LANES)
    n_proj, n_par, _ = proj.shape
    acc = jnp.zeros((n_par, LANES), F32)
    for k in range(n_proj):
        line = weights[k * 8 + h : k * 8 + h + 1, :]
        acc += proj[k, :, cols].astype(F32) * jnp.broadcast_to(line, (n_par, LANES))
    return acc


def projected(proj, field, h, table):
    cols = slice(h * LANES, (h + 1) * LANES)
    for k in range(proj.shape[0]):
        table[k * 8 + h : k * 8 + h + 1, :] = jnp.sum(
            proj[k, :, cols].astype(F32) * field, axis=0, keepdims=True
        )


def pairs(n_proj):
    return [(k, m) for k in range(n_proj) for m in range(k, n_proj)]


def form_kernel(after, proj, precond, out):
    del after
    n_proj = proj.shape[0]
    for h in range(precond.shape[1] // LANES):
        cols = slice(h * LANES, (h + 1) * LANES)
        tiles = [proj[k, :, cols].astype(F32) for k in range(n_proj)]
        scaled = [tile * precond[:, cols] for tile in tiles]
        for i, (k, m) in enumerate(pairs(n_proj)):
            out[i * 8 + h : i * 8 + h + 1, :] = jnp.sum(
                scaled[k] * tiles[m], axis=0, keepdims=True
            )


def blended(matrix, weights):
    n_proj = 9
    sums = [None] * n_proj

    def add(k, tile, m):
        term = tile * weights[m * 8 : m * 8 + 8, :]
        sums[k] = term if sums[k] is None else sums[k] + term

    for i, (k, m) in enumerate(pairs(n_proj)):
        tile = matrix[i * 8 : i * 8 + 8, :]
        add(k, tile, m)
        if k != m:
            add(m, tile, k)
    return sums


def lane_pick(table, low):
    return jnp.take_along_axis(table, low, axis=1, mode="promise_in_bounds")


def send_picks(table, ids, scalars, stage, out):
    n_blk = ids.shape[0]
    n_chunk = 8
    stage[...] = jnp.zeros_like(stage)
    index = ids[...]
    low = index & 127
    high = index >> 7
    for b in range(n_blk):
        low_b = jnp.broadcast_to(low[b : b + 1, :], (8, LANES))
        high_b = jnp.broadcast_to(high[b : b + 1, :], (8, LANES))
        got = jnp.zeros((8, LANES), F32)
        for h in range(n_chunk):
            piece = lane_pick(table[pl.ds(h, 8, stride=8), :], low_b)
            got = jnp.where(high_b == h, piece, got)
        stage[b * ROWS : b * ROWS + 8, :] = got
    got = jnp.zeros((n_blk, LANES), F32)
    for h in range(n_chunk):
        line = jnp.broadcast_to(table[64 + h : 65 + h, :], (n_blk, LANES))
        got = jnp.where(high == h, lane_pick(line, low), got)
    stage[pl.ds(8, n_blk, stride=ROWS), :] = got
    at = 10
    for rows in scalars:
        stage[at : at + rows.shape[0], :] = rows
        at += rows.shape[0]
    out[...] = stage[...].T.reshape(out.shape)


def start_kernel(own, partner, matrix, ids, out, weights, table, stage):
    weights[...] = own[...] + partner[...]
    for k, tile in enumerate(blended(matrix, weights)):
        table[k * 8 : k * 8 + 8, :] = -tile
    send_picks(table, ids, (), stage, out)


def state_kernel(
    after, own, partner, proj, precond, damping, res_out, dir_out, cross, rz_out, weights
):
    del after
    weights[...] = own[...] + partner[...]
    n_par, width = precond.shape
    rz = jnp.zeros((n_par, LANES), F32)
    for h in range(width // LANES):
        cols = slice(h * LANES, (h + 1) * LANES)
        res = -lifted(proj, weights, h)
        dirn = precond[:, cols] * res
        res_out[:, cols] = res
        dir_out[:, cols] = dirn
        rz += res * dirn
        projected(proj, precond[:, cols] * damping[:, cols] * dirn, h, cross)
    rz_out[...] = jnp.full(rz_out.shape, jnp.sum(rz), F32)


def step_kernel(
    own, partner, proj, precond, damping, matrix, cross, rz_in, ids, dirn,
    out, image_out, weights, table, stage,
):
    weights[...] = own[...] + partner[...]
    n_par, width = precond.shape
    for k, tile in enumerate(blended(matrix, weights)):
        table[k * 8 : k * 8 + 8, :] = tile + cross[k * 8 : k * 8 + 8, :]
    curve, square, damped, mixed, scaled = [jnp.zeros((n_par, LANES), F32)] * 5
    for h in range(width // LANES):
        cols = slice(h * LANES, (h + 1) * LANES)
        pull = damping[:, cols] * dirn[:, cols]
        image = lifted(proj, weights, h) + pull
        image_out[:, cols] = image
        change = precond[:, cols] * image
        curve += dirn[:, cols] * image
        square += change * image
        damped += pull * dirn[:, cols]
        mixed += pull * change
        scaled += damping[:, cols] * change * change
    lines = [jnp.sum(each, axis=0, keepdims=True) for each in (curve, square, damped, mixed, scaled)]
    send_picks(table, ids, (rz_in[0:1, :], over_lanes(jnp.concatenate(lines, axis=0))), stage, out)


def last_kernel(
    own, partner, proj, damping, steps, first_dir, res, dirn,
    sol_hbm, res_hbm, weights, sol_out, res_out, sem,
):
    weights[...] = own[...] + partner[...]
    rows = proj.shape[0] * 8
    curve = weights[rows : rows + 1, :] + steps[3:4, :]
    alpha = steps[2:3, :] / curve
    alpha_first = steps[0:1, :]
    chunks = damping.shape[1] // LANES
    copies = []

    def send(here, there, first, last):
        cols = pl.ds(first * LANES, (last - first) * LANES)
        copy = pltpu.make_async_copy(here.at[:, cols], there.at[:, cols], sem.at[len(copies)])
        copy.start()
        copies.append(copy)

    for h in range(chunks):
        cols = slice(h * LANES, (h + 1) * LANES)
        sol_out[:, cols] = alpha_first * first_dir[:, cols] + alpha * dirn[:, cols]
    for h in range(chunks):
        cols = slice(h * LANES, (h + 1) * LANES)
        image = lifted(proj, weights, h) + damping[:, cols] * dirn[:, cols]
        res_out[:, cols] = res[:, cols] - alpha * image
        if h == 0:
            send(sol_out, sol_hbm, 0, chunks)
        elif h == chunks // 2 + 1:
            send(res_out, res_hbm, 0, chunks // 2)
    send(res_out, res_hbm, chunks // 2, chunks)
    for copy in copies:
        copy.wait()


def local(jacobian, splat_ids, pix_residual, live_blocks, proj_jac, damping, precond):
    n_blk, n_pix, n_col = jacobian.shape
    n_par, g_dev = damping.shape
    n_scene, n_x = lax.axis_size("scene"), lax.axis_size("x")
    per = LANES // n_scene
    msg = f32(n_scene, per, LANES)
    wide = f32(n_scene, n_x, per, LANES)
    sums = f32(80, LANES)
    state = f32(n_par, g_dev)
    square = pltpu.VMEM((LANES, LANES), F32)
    whole = jax.ShapeDtypeStruct
    weights = pltpu.VMEM((80, LANES), F32)
    table = pltpu.VMEM((72, LANES), F32)

    def to_owners(message, right):
        flat = message.reshape(n_scene * n_x, per, LANES)
        got = lax.all_to_all(flat, ("scene", "x"), 0, 0, tiled=True)
        first = right is None
        wide_k = n_x * n_blk * LANES
        extra = (whole((n_blk, LANES), jnp.int32), whole((LANES, wide_k), BF16))
        own, *kept = call(
            functools.partial(sum_kernel, first),
            (sums,) + (extra if first else ()),
            [VMEM] * (1 if first else 2),
            [
                pltpu.VMEM((n_x, LANES, LANES), F32),
                pltpu.VMEM((n_x, LANES, LANES), F32),
                pltpu.VMEM((160, wide_k), BF16),
            ],
            1 << 31,
        )(got.reshape(n_scene, n_x, per, LANES), *(() if first else (right,)))
        partner = lax.ppermute(own, "core", [(0, 1), (1, 0)])
        return own, partner, *kept

    def to_blocks(message):
        return lax.all_to_all(message, "scene", 0, 0, tiled=True)

    message, jac, aux = call(
        rhs_kernel,
        (wide, whole(jacobian.shape, BF16), whole((2 * n_blk, LANES), jnp.int32)),
        [HBM] * 4,
        [
            pltpu.VMEM((n_blk, n_pix), BF16),
            pltpu.VMEM((1, live_blocks.shape[0]), jnp.int32),
            pltpu.VMEM((n_blk, LANES), jnp.int32),
            square,
            pltpu.SemaphoreType.DMA((n_blk,)),
            pltpu.SemaphoreType.DMA((3,)),
        ],
    )(*map(in_hbm, (live_blocks.reshape(1, -1), jacobian, pix_residual, splat_ids)))
    own, partner, index, right = to_owners(message, None)
    matrix = call(form_kernel, (f32(45 * 8, LANES),), [VMEM] * 3, (), 1 << 31)(
        own, proj_jac, precond
    )[0]
    message = call(start_kernel, (msg,), [VMEM] * 4, [weights, table, square])(
        own, partner, matrix, index
    )[0]
    first_own, first_partner = own, partner
    arrived = to_blocks(message)
    message, picks = call(
        first_kernel,
        (wide, f32(n_blk, n_col)),
        [VMEM] * 3,
        [square, square],
    )(jac, aux, arrived)
    own, partner = to_owners(message, right)
    res, first_dir, cross, rz = call(
        state_kernel, (state, state, f32(72, LANES), f32(8, LANES)), [VMEM] * 6, [weights], 1 << 31
    )(own, first_own, first_partner, proj_jac, precond, damping)
    message, image = call(step_kernel, (msg, state), [VMEM] * 10, [weights, table, square])(
        own, partner, proj_jac, precond, damping, matrix, cross, rz, index, first_dir
    )
    arrived = to_blocks(message)
    message, steps = call(
        second_kernel, (wide, f32(8, LANES)), [VMEM] * 4, [square, square]
    )(jac, aux, arrived, picks)
    own, partner = to_owners(message, right)
    res, second_dir = call(update_kernel, (state, state), [VMEM] * 6, (), 1 << 31)(
        own, steps, res, first_dir, image, precond
    )
    held = pltpu.VMEM((n_par, g_dev), F32)
    return call(
        last_kernel,
        (state, state),
        [VMEM] * 8,
        [weights, held, held, pltpu.SemaphoreType.DMA((3,))],
        out_space=HBM,
    )(
        own, partner, proj_jac, damping, steps, first_dir, res, second_dir
    )


def solution(mesh):
    scene = mesh.shape["scene"]
    finer = Mesh(mesh.devices.reshape(scene, -1, 2), ("scene", "x", "core"))
    everywhere = ("scene", "x", "core")
    in_specs = (
        P(everywhere, None, None),
        P(everywhere, None),
        P(everywhere, None),
        P(),
        P(None, None, "scene"),
        P(None, "scene"),
        P(None, "scene"),
    )
    out_specs = (P(None, "scene"), P(None, "scene"))
    return jax.shard_map(local, mesh=finer, in_specs=in_specs, out_specs=out_specs, check_vma=False)
```

```python
import functools

import jax
import jax.numpy as jnp
from jax import lax
from jax.experimental import pallas as pl
from jax.experimental.pallas import tpu as pltpu
from jax.sharding import Mesh
from jax.sharding import PartitionSpec as P

F32 = jnp.float32
BF16 = jnp.bfloat16
LANES = 128
ROWS = 16
VMEM = pl.BlockSpec(memory_space=pltpu.VMEM)
HBM = pl.BlockSpec(memory_space=pltpu.HBM)
NT = (((1,), (1,)), ((), ()))


def call(kernel, out, in_specs, scratch=(), flops=1 << 20, out_space=VMEM):
    return pl.pallas_call(
        kernel,
        out_shape=out,
        in_specs=in_specs,
        out_specs=jax.tree.map(lambda _: out_space, out),
        scratch_shapes=scratch,
        compiler_params=pltpu.CompilerParams(vmem_limit_bytes=24 << 20),
        cost_estimate=pl.CostEstimate(flops=flops, bytes_accessed=1 << 20, transcendentals=0),
    )


def in_hbm(array):
    return pltpu.with_memory_space_constraint(array, pltpu.HBM)


def f32(*shape):
    return jax.ShapeDtypeStruct(shape, F32)


def clear_stage(ids, stage, n_proj):
    stage[...] = jnp.zeros_like(stage)
    stage[pl.ds(n_proj, ids.shape[0], stride=ROWS), :] = ids.astype(F32)


def pack_return(acc, scalars, stage, out):
    n_blk = acc.shape[0]
    n_proj = acc.shape[1] // LANES
    for k in range(n_proj):
        stage[pl.ds(k, n_blk, stride=ROWS), :] = acc[:, k * LANES : (k + 1) * LANES]
    for i, value in enumerate(scalars):
        stage[n_proj + 1 + i : n_proj + 2 + i, :] = value
    turned = stage[...].T.reshape(out.shape[0], *out.shape[2:])
    for x in range(out.shape[1]):
        out[:, x] = turned


def rhs_kernel(live, jac, pix, ids, out, jbuf, aux, pixels, lives, index, stage, sem, small):
    n_blk = jac.shape[0]
    minor = [
        pltpu.make_async_copy(pix, pixels, small.at[0]),
        pltpu.make_async_copy(live, lives, small.at[1]),
        pltpu.make_async_copy(ids, index, small.at[2]),
    ]
    copies = [pltpu.make_async_copy(jac.at[b], jbuf.at[b], sem.at[b]) for b in range(n_blk)]
    for copy in minor:
        copy.start()
    for b, copy in enumerate(copies):
        copy.start(priority=b % 2)
    for copy in minor:
        copy.wait()
    n_x, n_core = lax.axis_size("x"), lax.axis_size("core")
    position = (lax.axis_index("scene") * n_x + lax.axis_index("x")) * n_core
    position = position + lax.axis_index("core")
    lane = lax.broadcasted_iota(jnp.int32, lives.shape, 1)
    own = jnp.sum(jnp.where(lane == position, lives[...], 0), axis=1, keepdims=True)
    local_ids = index[...] & (LANES * 8 - 1)
    aux[0:n_blk, :] = local_ids
    aux[n_blk : 2 * n_blk, :] = jnp.broadcast_to(own, (n_blk, LANES))
    clear_stage(local_ids, stage, jac.shape[2] // LANES)
    row = lax.broadcasted_iota(jnp.int32, pix.shape, 0)
    keep = row < jnp.broadcast_to(own, pix.shape)
    values = jnp.where(keep, pixels[...].astype(F32), 0.0)
    n_pix, n_col = jac.shape[1:]
    acc = jnp.zeros((n_blk, n_col), F32)
    cut = n_blk * 3 // 4
    for first, last in ((0, cut), (cut, n_blk)):
        signals = [jnp.where(row == b, values, 0.0).astype(BF16) for b in range(first, last)]
        for copy in copies[first:last]:
            copy.wait()
        stacked = jbuf[first:last].reshape((last - first) * n_pix, n_col)
        acc += jnp.dot(jnp.concatenate(signals, axis=1), stacked, preferred_element_type=F32)
    pack_return(acc, (), stage, out)


def lane_image(jac, b, line, ones):
    pieces = []
    for top in range(0, jac.shape[1], 64):
        folded = jnp.zeros((64, LANES), F32)
        for at in range(0, jac.shape[2], LANES):
            tile = jac[b, top : top + 64, at : at + LANES].astype(F32)
            folded += tile * line[:, at : at + LANES]
        high = folded.astype(BF16)
        pieces.append(jnp.concatenate([high, (folded - high.astype(F32)).astype(BF16)], axis=1))
    return lax.dot_general(
        ones, jnp.concatenate(pieces, axis=0), NT, preferred_element_type=F32
    )


def block_pass(picks, aux, jac, by_lanes):
    n_blk, n_pix = jac.shape[:2]
    row = lax.broadcasted_iota(jnp.int32, (n_blk, n_pix), 0)
    live = row < aux[n_blk : n_blk + 1, 0:1]
    chosen = picks.astype(BF16)
    rounded = chosen.astype(F32)
    ones = jnp.ones((n_blk, 2 * LANES), BF16)
    signals = []
    for b in range(n_blk):
        if (b * by_lanes) // n_blk != ((b + 1) * by_lanes) // n_blk:
            image = lane_image(jac, b, rounded[b : b + 1, :], ones)
        else:
            image = lax.dot_general(chosen, jac[b], NT, preferred_element_type=F32)
        signals.append(jnp.where((row == b) & live, image, 0.0).astype(BF16))
    stacked = jac[...].reshape(n_blk * n_pix, jac.shape[2])
    return jnp.dot(jnp.concatenate(signals, axis=1), stacked, preferred_element_type=F32)


def unpack_picks(recv, turned, n_blk, n_proj):
    turned[...] = recv[...].reshape(LANES, LANES).T
    return jnp.concatenate(
        [turned[pl.ds(k, n_blk, stride=ROWS), :] for k in range(n_proj)], axis=1
    )


def over_lanes(rows):
    return jnp.broadcast_to(jnp.sum(rows, axis=1, keepdims=True), rows.shape)


def first_kernel(jac, aux, recv, out, picks_out, turned, stage):
    n_blk = jac.shape[0]
    n_proj = jac.shape[2] // LANES
    picks = unpack_picks(recv, turned, n_blk, n_proj)
    picks_out[...] = picks
    acc = block_pass(picks, aux, jac, 5)
    clear_stage(aux[0:n_blk, :], stage, n_proj)
    pack_return(acc, (), stage, out)


def second_kernel(jac, aux, recv, picks_in, out, steps_out, turned, stage):
    n_blk = jac.shape[0]
    n_proj = jac.shape[2] // LANES
    fresh = unpack_picks(recv, turned, n_blk, n_proj)
    per = recv.shape[1]
    totals = over_lanes(turned[8:16, :]) * (1.0 / per)
    rz, curve, square, damped, mixed, scaled = (totals[i : i + 1, :] for i in range(2, 8))
    alpha = rz / curve
    after = rz - 2.0 * alpha * curve + alpha * alpha * square
    beta = after / rz
    grown = 1.0 + beta
    steps_out[0:1, :] = alpha
    steps_out[1:2, :] = beta
    steps_out[2:3, :] = after
    steps_out[3:4, :] = (
        grown * grown * damped - 2.0 * grown * alpha * mixed + alpha * alpha * scaled
    )
    steps_out[4:8, :] = jnp.zeros((4, LANES), F32)
    pieces = []
    for k in range(n_proj):
        cols = slice(k * LANES, (k + 1) * LANES)
        pieces.append(grown * picks_in[:, cols] - alpha * fresh[:, cols])
    picks = jnp.concatenate(pieces, axis=1)
    acc = block_pass(picks, aux, jac, 5)
    weighed = picks * acc
    line = jnp.zeros((n_blk, LANES), F32)
    for k in range(n_proj):
        line += weighed[:, k * LANES : (k + 1) * LANES]
    line = over_lanes(jnp.sum(line, axis=0, keepdims=True))
    clear_stage(aux[0:n_blk, :], stage, n_proj)
    pack_return(acc, (line,), stage, out)


def update_kernel(after, steps, res, dirn, image, precond, res_out, dir_out):
    del after
    alpha, beta = steps[0:1, :], steps[1:2, :]
    for h in range(res.shape[1] // LANES):
        cols = slice(h * LANES, (h + 1) * LANES)
        new_res = res[:, cols] - alpha * image[:, cols]
        res_out[:, cols] = new_res
        dir_out[:, cols] = precond[:, cols] * new_res + beta * dirn[:, cols]


def sum_kernel(first, recv, *rest):
    if first:
        out, ids_out, right, turned, fine, left = rest
    else:
        right, out, turned, fine, left = rest
    n_x = recv.shape[1]
    n_blk = LANES // ROWS
    n_proj = 9
    sub = lax.broadcasted_iota(jnp.int32, (n_blk, LANES), 0)
    deep = lax.broadcasted_iota(jnp.int32, (LANES, LANES), 0).astype(BF16)
    half = n_proj * 8

    def spread(table, x, base, high):
        lines = [
            jnp.broadcast_to(table[x, base + k : base + k + 1, :], (8, LANES))
            for k in range(n_proj)
        ]
        return jnp.concatenate([jnp.where(high, line, 0.0) for line in lines], axis=0)

    for x in range(n_x):
        values = recv[:, x].reshape(LANES, LANES).T
        turned[x] = values
        fine[x] = values - values.astype(BF16).astype(F32)
        for b in range(n_blk):
            at = (x * n_blk + b) * LANES
            cols = slice(at, at + LANES)
            base = b * ROWS
            ids = turned[x, base + n_proj : base + n_proj + 1, :].astype(jnp.int32)
            high = jnp.broadcast_to(ids >> 7, (8, LANES)) == sub
            left[0:half, cols] = spread(turned, x, base, high).astype(BF16)
            left[80 : 80 + half, cols] = spread(fine, x, base, high).astype(BF16)
            if first:
                low = jnp.broadcast_to((ids & 127).astype(BF16), (LANES, LANES)) == deep
                right[:, cols] = jnp.where(low, jnp.ones_like(deep), jnp.zeros_like(deep))
    summed = lax.dot_general(left[...], right[...], NT, preferred_element_type=F32)
    out[0:half, :] = summed[0:half] + summed[80 : 80 + half]
    per = recv.shape[2]
    mixed = jnp.zeros((1, LANES), F32)
    for x in range(n_x):
        mixed += turned[x, n_proj + 1 : n_proj + 2, :]
    out[half : half + 1, :] = over_lanes(mixed) * (1.0 / per)
    out[half + 1 : half + 8, :] = jnp.zeros((7, LANES), F32)
    if first:
        ids_out[...] = turned[lax.axis_index("x"), pl.ds(n_proj, n_blk, stride=ROWS), :].astype(jnp.int32)


def lifted(proj, weights, h):
    cols = slice(h * LANES, (h + 1) * LANES)
    n_proj, n_par, _ = proj.shape
    acc = jnp.zeros((n_par, LANES), F32)
    for k in range(n_proj):
        line = weights[k * 8 + h : k * 8 + h + 1, :]
        acc += proj[k, :, cols].astype(F32) * jnp.broadcast_to(line, (n_par, LANES))
    return acc


def projected(proj, field, h, table):
    cols = slice(h * LANES, (h + 1) * LANES)
    for k in range(proj.shape[0]):
        table[k * 8 + h : k * 8 + h + 1, :] = jnp.sum(
            proj[k, :, cols].astype(F32) * field, axis=0, keepdims=True
        )


def pairs(n_proj):
    return [(k, m) for k in range(n_proj) for m in range(k, n_proj)]


def form_kernel(after, proj, precond, out):
    del after
    n_proj = proj.shape[0]
    for h in range(precond.shape[1] // LANES):
        cols = slice(h * LANES, (h + 1) * LANES)
        tiles = [proj[k, :, cols].astype(F32) for k in range(n_proj)]
        scaled = [tile * precond[:, cols] for tile in tiles]
        for i, (k, m) in enumerate(pairs(n_proj)):
            out[i * 8 + h : i * 8 + h + 1, :] = jnp.sum(
                scaled[k] * tiles[m], axis=0, keepdims=True
            )


def blended(matrix, weights):
    n_proj = 9
    sums = [None] * n_proj

    def add(k, tile, m):
        term = tile * weights[m * 8 : m * 8 + 8, :]
        sums[k] = term if sums[k] is None else sums[k] + term

    for i, (k, m) in enumerate(pairs(n_proj)):
        tile = matrix[i * 8 : i * 8 + 8, :]
        add(k, tile, m)
        if k != m:
            add(m, tile, k)
    return sums


def lane_pick(table, low):
    return jnp.take_along_axis(table, low, axis=1, mode="promise_in_bounds")


def send_picks(table, ids, scalars, stage, out):
    n_blk = ids.shape[0]
    n_chunk = 8
    stage[...] = jnp.zeros_like(stage)
    index = ids[...]
    low = index & 127
    high = index >> 7
    for b in range(n_blk):
        low_b = jnp.broadcast_to(low[b : b + 1, :], (8, LANES))
        high_b = jnp.broadcast_to(high[b : b + 1, :], (8, LANES))
        got = jnp.zeros((8, LANES), F32)
        for h in range(n_chunk):
            piece = lane_pick(table[pl.ds(h, 8, stride=8), :], low_b)
            got = jnp.where(high_b == h, piece, got)
        stage[b * ROWS : b * ROWS + 8, :] = got
    got = jnp.zeros((n_blk, LANES), F32)
    for h in range(n_chunk):
        line = jnp.broadcast_to(table[64 + h : 65 + h, :], (n_blk, LANES))
        got = jnp.where(high == h, lane_pick(line, low), got)
    stage[pl.ds(8, n_blk, stride=ROWS), :] = got
    at = 10
    for rows in scalars:
        stage[at : at + rows.shape[0], :] = rows
        at += rows.shape[0]
    out[...] = stage[...].T.reshape(out.shape)


def start_kernel(own, partner, matrix, ids, out, weights, table, stage):
    weights[...] = own[...] + partner[...]
    for k, tile in enumerate(blended(matrix, weights)):
        table[k * 8 : k * 8 + 8, :] = -tile
    send_picks(table, ids, (), stage, out)


def state_kernel(
    after, own, partner, proj, precond, damping, res_out, dir_out, cross, rz_out, weights
):
    del after
    weights[...] = own[...] + partner[...]
    n_par, width = precond.shape
    rz = jnp.zeros((n_par, LANES), F32)
    for h in range(width // LANES):
        cols = slice(h * LANES, (h + 1) * LANES)
        res = -lifted(proj, weights, h)
        dirn = precond[:, cols] * res
        res_out[:, cols] = res
        dir_out[:, cols] = dirn
        rz += res * dirn
        projected(proj, precond[:, cols] * damping[:, cols] * dirn, h, cross)
    rz_out[...] = jnp.full(rz_out.shape, jnp.sum(rz), F32)


def step_kernel(
    own, partner, proj, precond, damping, matrix, cross, rz_in, ids, dirn,
    out, image_out, weights, table, stage,
):
    weights[...] = own[...] + partner[...]
    n_par, width = precond.shape
    for k, tile in enumerate(blended(matrix, weights)):
        table[k * 8 : k * 8 + 8, :] = tile + cross[k * 8 : k * 8 + 8, :]
    curve, square, damped, mixed, scaled = [jnp.zeros((n_par, LANES), F32)] * 5
    for h in range(width // LANES):
        cols = slice(h * LANES, (h + 1) * LANES)
        pull = damping[:, cols] * dirn[:, cols]
        image = lifted(proj, weights, h) + pull
        image_out[:, cols] = image
        change = precond[:, cols] * image
        curve += dirn[:, cols] * image
        square += change * image
        damped += pull * dirn[:, cols]
        mixed += pull * change
        scaled += damping[:, cols] * change * change
    lines = [jnp.sum(each, axis=0, keepdims=True) for each in (curve, square, damped, mixed, scaled)]
    send_picks(table, ids, (rz_in[0:1, :], over_lanes(jnp.concatenate(lines, axis=0))), stage, out)


def last_kernel(
    own, partner, proj, damping, steps, first_dir, res, dirn,
    sol_hbm, res_hbm, weights, sol_out, res_out, sem,
):
    weights[...] = own[...] + partner[...]
    rows = proj.shape[0] * 8
    curve = weights[rows : rows + 1, :] + steps[3:4, :]
    alpha = steps[2:3, :] / curve
    alpha_first = steps[0:1, :]
    chunks = damping.shape[1] // LANES
    copies = []

    def send(here, there, first, last):
        cols = pl.ds(first * LANES, (last - first) * LANES)
        copy = pltpu.make_async_copy(here.at[:, cols], there.at[:, cols], sem.at[len(copies)])
        copy.start()
        copies.append(copy)

    for h in range(chunks):
        cols = slice(h * LANES, (h + 1) * LANES)
        sol_out[:, cols] = alpha_first * first_dir[:, cols] + alpha * dirn[:, cols]
    for h in range(chunks):
        cols = slice(h * LANES, (h + 1) * LANES)
        image = lifted(proj, weights, h) + damping[:, cols] * dirn[:, cols]
        res_out[:, cols] = res[:, cols] - alpha * image
        if h == 0:
            send(sol_out, sol_hbm, 0, chunks)
        elif h % 2 == 0:
            send(res_out, res_hbm, h - 2, h)
    send(res_out, res_hbm, chunks - 2, chunks)
    for copy in copies:
        copy.wait()


def local(jacobian, splat_ids, pix_residual, live_blocks, proj_jac, damping, precond):
    n_blk, n_pix, n_col = jacobian.shape
    n_par, g_dev = damping.shape
    n_scene, n_x = lax.axis_size("scene"), lax.axis_size("x")
    per = LANES // n_scene
    msg = f32(n_scene, per, LANES)
    wide = f32(n_scene, n_x, per, LANES)
    sums = f32(80, LANES)
    state = f32(n_par, g_dev)
    square = pltpu.VMEM((LANES, LANES), F32)
    whole = jax.ShapeDtypeStruct
    weights = pltpu.VMEM((80, LANES), F32)
    table = pltpu.VMEM((72, LANES), F32)

    def to_owners(message, right):
        flat = message.reshape(n_scene * n_x, per, LANES)
        got = lax.all_to_all(flat, ("scene", "x"), 0, 0, tiled=True)
        first = right is None
        wide_k = n_x * n_blk * LANES
        extra = (whole((n_blk, LANES), jnp.int32), whole((LANES, wide_k), BF16))
        own, *kept = call(
            functools.partial(sum_kernel, first),
            (sums,) + (extra if first else ()),
            [VMEM] * (1 if first else 2),
            [
                pltpu.VMEM((n_x, LANES, LANES), F32),
                pltpu.VMEM((n_x, LANES, LANES), F32),
                pltpu.VMEM((160, wide_k), BF16),
            ],
            1 << 31,
        )(got.reshape(n_scene, n_x, per, LANES), *(() if first else (right,)))
        partner = lax.ppermute(own, "core", [(0, 1), (1, 0)])
        return own, partner, *kept

    def to_blocks(message):
        return lax.all_to_all(message, "scene", 0, 0, tiled=True)

    message, jac, aux = call(
        rhs_kernel,
        (wide, whole(jacobian.shape, BF16), whole((2 * n_blk, LANES), jnp.int32)),
        [HBM] * 4,
        [
            pltpu.VMEM((n_blk, n_pix), BF16),
            pltpu.VMEM((1, live_blocks.shape[0]), jnp.int32),
            pltpu.VMEM((n_blk, LANES), jnp.int32),
            square,
            pltpu.SemaphoreType.DMA((n_blk,)),
            pltpu.SemaphoreType.DMA((3,)),
        ],
    )(*map(in_hbm, (live_blocks.reshape(1, -1), jacobian, pix_residual, splat_ids)))
    own, partner, index, right = to_owners(message, None)
    matrix = call(form_kernel, (f32(45 * 8, LANES),), [VMEM] * 3, (), 1 << 31)(
        own, proj_jac, precond
    )[0]
    message = call(start_kernel, (msg,), [VMEM] * 4, [weights, table, square])(
        own, partner, matrix, index
    )[0]
    first_own, first_partner = own, partner
    arrived = to_blocks(message)
    message, picks = call(
        first_kernel,
        (wide, f32(n_blk, n_col)),
        [VMEM] * 3,
        [square, square],
    )(jac, aux, arrived)
    own, partner = to_owners(message, right)
    res, first_dir, cross, rz = call(
        state_kernel, (state, state, f32(72, LANES), f32(8, LANES)), [VMEM] * 6, [weights], 1 << 31
    )(own, first_own, first_partner, proj_jac, precond, damping)
    message, image = call(step_kernel, (msg, state), [VMEM] * 10, [weights, table, square])(
        own, partner, proj_jac, precond, damping, matrix, cross, rz, index, first_dir
    )
    arrived = to_blocks(message)
    message, steps = call(
        second_kernel, (wide, f32(8, LANES)), [VMEM] * 4, [square, square]
    )(jac, aux, arrived, picks)
    own, partner = to_owners(message, right)
    res, second_dir = call(update_kernel, (state, state), [VMEM] * 6, (), 1 << 31)(
        own, steps, res, first_dir, image, precond
    )
    held = pltpu.VMEM((n_par, g_dev), F32)
    return call(
        last_kernel,
        (state, state),
        [VMEM] * 8,
        [weights, held, held, pltpu.SemaphoreType.DMA((1 + g_dev // (2 * LANES),))],
        out_space=HBM,
    )(
        own, partner, proj_jac, damping, steps, first_dir, res, second_dir
    )


def solution(mesh):
    scene = mesh.shape["scene"]
    finer = Mesh(mesh.devices.reshape(scene, -1, 2), ("scene", "x", "core"))
    everywhere = ("scene", "x", "core")
    in_specs = (
        P(everywhere, None, None),
        P(everywhere, None),
        P(everywhere, None),
        P(),
        P(None, None, "scene"),
        P(None, "scene"),
        P(None, "scene"),
    )
    out_specs = (P(None, "scene"), P(None, "scene"))
    return jax.shard_map(local, mesh=finer, in_specs=in_specs, out_specs=out_specs, check_vma=False)
```
